256 devices in a mesh: beam: 4 (over y), row: 4 (over x), col: 16 (over z, core).
Axes of the slice: x: 4, y: 4, z: 8, core: 2. Of those that a mesh axis runs over, the one named last changes fastest.
Arguments:
- phase_volume: bfloat16 [64, 1024, 2048], P('beam', 'row', 'col'), may hold values from -0.75 to 0.75
- absorb_volume: bfloat16 [64, 1024, 2048], P('beam', 'row', 'col'), may hold values from -0.375 to 0.375
- probe: float32 [2, 256, 256], replicated, may hold values from -6 to 6
- amplitudes: bfloat16 [4, 16, 32, 256, 256], P('row', 'col', 'beam'), may hold values from 0.19921875 to 2.5
- scan_rows: int32 [4, 16, 32], P('row', 'col', 'beam'), may hold values from 0 to 255
- scan_cols: int32 [4, 16, 32], P('row', 'col', 'beam'), may hold values from 0 to 127
Outputs:
- object_step: float32 [2, 1024, 2048], P(None, 'row', 'col')
- probe_gradient: float32 [2, 256, 256], replicated
- loss: float32 [], replicated
The draws below stay inside these ranges and needn't reach their ends.
All inputs are finite; a program needn't handle non-finite values.
Results may differ from the reference program's by a relative error of at most 0.00055.
The reference program's roundings to bfloat16 on the way count: a program that leaves them out, or rounds other values in their place, can miss the bound.
Values sent between devices are 32-bit elements; how exact they have to be, the bound alone decides.
A program may use at most 64 MiB of HBM per device.

```python
import math
import jax
import jax.numpy as jnp
from jax import lax

ROW_DEV = 256
COL_DEV = 128
PROBE = 256
DEPTH = 64
NROWS = 1024
NCOLS = 2048
SCANS = 32
N_ROW = 4
N_COL = 16


def touch_ends(result, stream_key, least, largest):
    longest = result.shape.index(max(result.shape))
    spots = []
    for shift in (0, 1):
        where = [jax.random.randint(jax.random.fold_in(stream_key, axis), (), 0, length) for axis, length in enumerate(result.shape)]
        where[longest] = (where[longest] + shift) % result.shape[longest]
        spots.append(tuple(where))
    return result.at[spots[0]].set(least).at[spots[1]].set(largest)


def block_levels(rng, extent, split, least, largest):
    def one(dim, blocks):
        steps = jax.random.uniform(jax.random.fold_in(jax.random.fold_in(rng, 6), dim), (blocks,), jnp.float32, least / len(split), largest / len(split))
        return jnp.repeat(jnp.exp(steps), extent[dim] // blocks).reshape((-1,) + (1,) * (len(extent) - dim - 1))

    loudness = one(*split[0])
    for cut in split[1:]:
        loudness = loudness * one(*cut)
    return loudness


def normal_values(own_key, shape, scale, most, cuts=(), kind=jnp.bfloat16):
    loudness = block_levels(own_key, shape, cuts, -0.22, 0.18) if cuts else 1.0
    values = jax.random.normal(own_key, shape, jnp.float32) * scale * loudness
    return jnp.minimum(jnp.maximum(values, -most), most).astype(kind)


def setup_inputs(seed: int = 0) -> dict:
    seeds = jax.random.split(jax.random.key(seed), 7)
    return {
        "phase_volume": normal_values(seeds[0], (DEPTH, NROWS, NCOLS), DEPTH ** -0.5, 0.75, ((0, 4), (1, 4), (2, 16))),
        "absorb_volume": normal_values(seeds[1], (DEPTH, NROWS, NCOLS), (4 * DEPTH) ** -0.5, 0.375, ((0, 4), (1, 4), (2, 16))),
        "probe": normal_values(seeds[2], (2, PROBE, PROBE), 1.0, 6.0, (), jnp.float32),
        "amplitudes": jnp.clip(0.19921875 + 2.3007812 * jax.random.uniform(seeds[3], (N_ROW, N_COL, SCANS, PROBE, PROBE), jnp.float32) ** block_levels(seeds[3], (N_ROW, N_COL, SCANS, PROBE, PROBE), ((0, 4), (1, 16), (2, 4)), -0.2, 0.2), 0.19921875, 2.5).astype(jnp.bfloat16),
        "scan_rows": touch_ends(jax.random.randint(seeds[4], (N_ROW, N_COL, SCANS), 0, ROW_DEV), jax.random.fold_in(seeds[4], 1), 0, ROW_DEV - 1).astype(jnp.int32),
        "scan_cols": touch_ends(jax.random.randint(seeds[5], (N_ROW, N_COL, SCANS), 0, COL_DEV), jax.random.fold_in(seeds[5], 1), 0, COL_DEV - 1).astype(jnp.int32),
    }


def dft_tables(length):
    indices = jnp.arange(length, dtype=jnp.int32)
    product = indices[:, None] * indices[None, :] % length
    angles = product.astype(jnp.float32) * (2.0 * math.pi / length)
    factor = 1.0 / math.sqrt(length)
    return ((jnp.cos(angles) * factor).astype(jnp.bfloat16), (-jnp.sin(angles) * factor).astype(jnp.bfloat16))

def left_apply(matrix, batch):
    return jnp.einsum('ab,sbc->sac', matrix.astype(jnp.float32), batch.astype(jnp.float32))

def right_apply(batch, matrix):
    return jnp.einsum('sab,bc->sac', batch.astype(jnp.float32), matrix.astype(jnp.float32))

def window_terms(windows, probe, amplitude, table_real, table_imag):
    phase = windows[:, 0]
    absorb = windows[:, 1]
    damping = jnp.exp(-absorb)
    trans_real = damping * jnp.cos(phase)
    trans_imag = damping * jnp.sin(phase)
    wave_real = probe[0] * trans_real - probe[1] * trans_imag
    wave_imag = probe[0] * trans_imag + probe[1] * trans_real
    send_real = wave_real.astype(jnp.bfloat16)
    send_imag = wave_imag.astype(jnp.bfloat16)
    half_real = (left_apply(table_real, send_real) - left_apply(table_imag, send_imag)).astype(jnp.bfloat16)
    half_imag = (left_apply(table_real, send_imag) + left_apply(table_imag, send_real)).astype(jnp.bfloat16)
    far_real = right_apply(half_real, table_real) - right_apply(half_imag, table_imag)
    far_imag = right_apply(half_real, table_imag) + right_apply(half_imag, table_real)
    modulus = jnp.sqrt(far_real * far_real + far_imag * far_imag)
    misfit = jnp.sum((modulus - amplitude) * (modulus - amplitude))
    ratio = 1.0 - amplitude / jnp.maximum(modulus, 0.5)
    resid_real = (far_real * ratio).astype(jnp.bfloat16)
    resid_imag = (far_imag * ratio).astype(jnp.bfloat16)
    back_real = (left_apply(table_real, resid_real) + left_apply(table_imag, resid_imag)).astype(jnp.bfloat16)
    back_imag = (left_apply(table_real, resid_imag) - left_apply(table_imag, resid_real)).astype(jnp.bfloat16)
    grad_real = right_apply(back_real, table_real) + right_apply(back_imag, table_imag)
    grad_imag = right_apply(back_imag, table_real) - right_apply(back_real, table_imag)
    object_real = wave_real * grad_real + wave_imag * grad_imag
    object_imag = wave_real * grad_imag - wave_imag * grad_real
    cells = jnp.stack([object_imag, -object_real], axis=1)
    probe_real = lax.optimization_barrier(jnp.sum(trans_real * grad_real + trans_imag * grad_imag, axis=0))
    probe_imag = lax.optimization_barrier(jnp.sum(trans_real * grad_imag - trans_imag * grad_real, axis=0))
    return (cells, jnp.stack([probe_real, probe_imag]), misfit)

def reference(phase_volume, absorb_volume, probe, amplitudes, scan_rows, scan_cols):
    half = PROBE // 2
    projection = jnp.stack([lax.optimization_barrier(jnp.sum(phase_volume.astype(jnp.float32), axis=0)), lax.optimization_barrier(jnp.sum(absorb_volume.astype(jnp.float32), axis=0))])
    padded = jnp.pad(projection, ((0, 0), (half, half), (half, half)))
    table_real, table_imag = dft_tables(PROBE)
    tiles = N_ROW * N_COL
    row_list = scan_rows.reshape(tiles, SCANS).astype(jnp.int32)
    col_list = scan_cols.reshape(tiles, SCANS).astype(jnp.int32)
    amp_list = amplitudes.reshape(tiles, SCANS, PROBE, PROBE)
    zero_index = jnp.zeros((), jnp.int32)

    def per_tile(carry, inputs):
        canvas, probe_sum, misfit_sum = carry
        tile, rows_here, cols_here, amp_here = inputs
        row_start = (tile // N_COL * ROW_DEV + rows_here).astype(jnp.int32)
        col_start = (tile % N_COL * COL_DEV + cols_here).astype(jnp.int32)
        windows = jax.vmap(lambda row_at, col_at: lax.dynamic_slice(padded, (zero_index, row_at, col_at), (2, PROBE, PROBE)))(row_start, col_start)
        cells, probe_term, misfit = window_terms(windows, probe, amp_here.astype(jnp.float32), table_real, table_imag)

        def add_window(index, canvas_now):
            where = (zero_index, row_start[index], col_start[index])
            piece = lax.dynamic_slice(canvas_now, where, (2, PROBE, PROBE))
            return lax.dynamic_update_slice(canvas_now, piece + cells[index], where)
        canvas = lax.fori_loop(0, SCANS, add_window, canvas)
        return ((canvas, probe_sum + probe_term, misfit_sum + misfit), None)
    start = (jnp.zeros((2, NROWS + PROBE, NCOLS + PROBE), jnp.float32), jnp.zeros((2, PROBE, PROBE), jnp.float32), jnp.zeros((), jnp.float32))
    inputs = (jnp.arange(tiles, dtype=jnp.int32), row_list, col_list, amp_list)
    (canvas, probe_sum, misfit_sum), _ = lax.scan(per_tile, start, inputs)
    gradient = canvas[:, half:half + NROWS, half:half + NCOLS]
    mean_square = jnp.sum(gradient * gradient) / (2 * NROWS * NCOLS)
    factor = jnp.minimum(1.0, 0.5 / jnp.sqrt(mean_square + 1e-06))
    total = N_ROW * N_COL * SCANS
    return (gradient * factor, probe_sum / total, misfit_sum / (total * PROBE * PROBE))
```

```python
import math

import jax
import jax.numpy as jnp
import numpy as np
from jax import lax
from jax.experimental import pallas as pl
from jax.experimental.pallas import tpu as pltpu
from jax.sharding import Mesh
from jax.sharding import PartitionSpec as P

COL = ("col_0", "col_1")
ROW_COL = ("row", "col_0", "col_1")
LANES = 128
CHUNK = 128


def dft_tables(length):
    indices = np.arange(length, dtype=np.int32)
    product = indices[:, None] * indices[None, :] % length
    angles = product.astype(np.float32) * np.float32(2.0 * math.pi / length)
    factor = np.float32(1.0 / math.sqrt(length))
    return (
        jnp.asarray(np.cos(angles) * factor).astype(jnp.bfloat16),
        jnp.asarray(-np.sin(angles) * factor).astype(jnp.bfloat16),
    )


def window_kernel(
    rows_ref, cols_ref, t_ref, probe_ref, amp_ref, table_ref,
    canvas_ref, probe_sum_ref, misfit_ref,
    fwd, bwd, cut, psi, half, chi, back,
):
    step = pl.program_id(0)
    n = probe_ref.shape[1]

    @pl.when(step == 0)
    def _():
        real, imag = table_ref[0], table_ref[1]
        minus = -imag
        fwd[:n, :n] = real
        fwd[:n, n:] = minus
        fwd[n:, :n] = imag
        fwd[n:, n:] = real
        bwd[:n, :n] = real
        bwd[:n, n:] = imag
        bwd[n:, :n] = minus
        bwd[n:, n:] = real
        canvas_ref[...] = jnp.zeros_like(canvas_ref)
        probe_sum_ref[...] = jnp.zeros_like(probe_sum_ref)
        misfit_ref[...] = jnp.zeros_like(misfit_ref)

    row = rows_ref[step]
    col = cols_ref[step]
    turn = lax.rem(LANES - col, LANES)
    lane = lax.broadcasted_iota(jnp.int32, (32, LANES), 1)
    near = lane < LANES - col
    for at in range(0, n, 32):
        here = pl.ds(at, 32)
        pieces = []
        for part in range(2):
            turned = [
                pltpu.roll(t_ref[part, k, pl.ds(row + at, 32), :], turn, 1) for k in range(3)
            ]
            pieces.append([jnp.where(near, turned[k], turned[k + 1]) for k in range(2)])
        for k in range(2):
            lanes = pl.ds(k * LANES, LANES)
            tr, ti = pieces[0][k], pieces[1][k]
            cut[0, here, lanes] = tr
            cut[1, here, lanes] = ti
            pr = probe_ref[0, here, lanes]
            pi = probe_ref[1, here, lanes]
            psi[here, lanes] = (pr * tr - pi * ti).astype(jnp.bfloat16)
            psi[pl.ds(n + at, 32), lanes] = (pr * ti + pi * tr).astype(jnp.bfloat16)
    for part in range(2):
        half[:, part * n : (part + 1) * n] = jnp.dot(
            fwd[part * n : (part + 1) * n, :], psi[...], preferred_element_type=jnp.float32
        ).astype(jnp.bfloat16)
    total = jnp.zeros((8, LANES), jnp.float32)
    for at in range(0, n, CHUNK):
        here = pl.ds(at, CHUNK)
        far = jnp.dot(half[here, :], bwd[...], preferred_element_type=jnp.float32)
        fr, fi = far[:, :n], far[:, n:]
        amp = amp_ref[0, here, :].astype(jnp.float32)
        power = fr * fr + fi * fi
        inverse = lax.rsqrt(power)
        modulus = jnp.where(power > 0.0, power * inverse, 0.0)
        off = modulus - amp
        square = off * off
        total = total + jnp.sum(
            (square[:, :LANES] + square[:, LANES:]).reshape(CHUNK // 8, 8, LANES), axis=0
        )
        ratio = 1.0 - amp * jnp.minimum(inverse, 2.0)
        chi[here, :] = (fr * ratio).astype(jnp.bfloat16)
        chi[pl.ds(n + at, CHUNK), :] = (fi * ratio).astype(jnp.bfloat16)
    misfit_ref[...] += total
    for part in range(2):
        back[:, part * n : (part + 1) * n] = jnp.dot(
            bwd[part * n : (part + 1) * n, :], chi[...], preferred_element_type=jnp.float32
        ).astype(jnp.bfloat16)
    far_side = lax.broadcasted_iota(jnp.int32, (CHUNK, LANES), 1) >= col
    for at in range(0, n, CHUNK):
        here = pl.ds(at, CHUNK)
        grad = jnp.dot(back[here, :], fwd[...], preferred_element_type=jnp.float32)
        gr, gi = grad[:, :n], grad[:, n:]
        tr, ti = cut[0, here, :], cut[1, here, :]
        probe_sum_ref[0, here, :] += tr * gr + ti * gi
        probe_sum_ref[1, here, :] += tr * gi - ti * gr
        pr, pi = probe_ref[0, here, :], probe_ref[1, here, :]
        for part, value in enumerate((pr * gr + pi * gi, pr * gi - pi * gr)):
            first = pltpu.roll(value[:, :LANES], col, 1)
            second = pltpu.roll(value[:, LANES:], col, 1)
            there = pl.ds(row + at, CHUNK)
            canvas_ref[part, 0, there, :] += jnp.where(far_side, first, 0.0)
            canvas_ref[part, 1, there, :] += jnp.where(far_side, second, first)
            canvas_ref[part, 2, there, :] += jnp.where(far_side, 0.0, second)


def window_terms(t, probe, amplitudes, rows, cols):
    count, n, _ = amplitudes.shape
    grid_spec = pltpu.PrefetchScalarGridSpec(
        num_scalar_prefetch=2,
        grid=(count,),
        in_specs=[
            pl.BlockSpec(t.shape, lambda s, *_: (0, 0, 0, 0)),
            pl.BlockSpec(probe.shape, lambda s, *_: (0, 0, 0)),
            pl.BlockSpec((1, n, n), lambda s, *_: (s, 0, 0)),
            pl.BlockSpec((2, n, n), lambda s, *_: (0, 0, 0)),
        ],
        out_specs=[
            pl.BlockSpec(t.shape, lambda s, *_: (0, 0, 0, 0)),
            pl.BlockSpec(probe.shape, lambda s, *_: (0, 0, 0)),
            pl.BlockSpec((8, LANES), lambda s, *_: (0, 0)),
        ],
        scratch_shapes=[
            pltpu.VMEM((2 * n, 2 * n), jnp.bfloat16),
            pltpu.VMEM((2 * n, 2 * n), jnp.bfloat16),
            pltpu.VMEM((2, n, n), jnp.float32),
            pltpu.VMEM((2 * n, n), jnp.bfloat16),
            pltpu.VMEM((n, 2 * n), jnp.bfloat16),
            pltpu.VMEM((2 * n, n), jnp.bfloat16),
            pltpu.VMEM((n, 2 * n), jnp.bfloat16),
        ],
    )
    return pl.pallas_call(
        window_kernel,
        grid_spec=grid_spec,
        out_shape=[
            jax.ShapeDtypeStruct(t.shape, jnp.float32),
            jax.ShapeDtypeStruct(probe.shape, jnp.float32),
            jax.ShapeDtypeStruct((8, LANES), jnp.float32),
        ],
        compiler_params=pltpu.CompilerParams(dimension_semantics=("arbitrary",)),
        name="windows",
    )(rows, cols, t, probe, amplitudes, jnp.stack(dft_tables(n)))


def from_behind(value, axis, steps):
    count = lax.axis_size(axis)
    first, last = (max(0, -steps), min(count, count - steps))
    return lax.ppermute(value, axis, [(source, source + steps) for source in range(first, last)])


def sent_to_all(x, axis):
    copies = jnp.broadcast_to(x, (lax.axis_size(axis), *x.shape))
    return lax.all_to_all(copies, axis, split_axis=0, concat_axis=0, tiled=True)


def over_copies(x, axis):
    return sent_to_all(x, axis).sum(axis=0)


def extended(cells, sides, width):
    for axis, dim in sides:
        head = lax.slice_in_dim(cells, 0, width, axis=dim)
        tail = lax.slice_in_dim(cells, cells.shape[dim] - width, cells.shape[dim], axis=dim)
        cells = jnp.concatenate(
            [from_behind(tail, axis, 1), cells, from_behind(head, axis, -1)], axis=dim
        )
    return cells


def rows_for(lines, length):
    spare = -lines.shape[0] % length
    if not spare:
        return lines
    return jnp.concatenate([lines, jnp.zeros((spare, *lines.shape[1:]), lines.dtype)])


def joined_along(parts, dim):
    parts = jnp.moveaxis(parts, 0, dim)
    dims = parts.shape
    return parts.reshape(*dims[:dim], dims[dim] * dims[dim + 1], *dims[dim + 2 :])


def gather_axes(x, axes, dim):
    far, near = axes
    parts = sent_to_all(sent_to_all(x, far), near)
    return joined_along(parts.swapaxes(0, 1).reshape(-1, *x.shape), dim)


def cut_along(x, dim, length):
    before, after = (x.shape[:dim], x.shape[dim + 1 :])
    return jnp.moveaxis(x.reshape(*before, length, -1, *after), dim, 0)


def summed_on_arrival(x, axis, dim):
    length = lax.axis_size(axis)
    parts = lax.all_to_all(cut_along(x, dim, length), axis, 0, 0, tiled=True)
    return jnp.sum(parts, axis=0)


def summed_rows(x, axes, dim):
    far, near = axes
    own = summed_on_arrival(cut_along(x, dim, lax.axis_size(far)), near, dim + 1)
    return jnp.sum(lax.all_to_all(own, far, 0, 0, tiled=True), axis=0)


def sum_by_parts(x, axes):
    padded = rows_for(x, lax.axis_size(axes[0]) * lax.axis_size(axes[1]))
    whole = gather_axes(summed_rows(padded, axes, 0), axes, 0)
    return lax.slice_in_dim(whole, 0, len(x)).reshape(x.shape)


def packed_total(arrays, axis):
    ends = [0]
    for a in arrays:
        ends.append(ends[-1] + a.size)
    so_far = sum_by_parts(jnp.concatenate([a.ravel() for a in arrays]), axis)
    return tuple((so_far[b:e].reshape(a.shape) for a, b, e in zip(arrays, ends, ends[1:])))


def local(phase_volume, absorb_volume, probe, amplitudes, scan_rows, scan_cols):
    length = probe.shape[1]
    half = length // 2
    count = scan_rows.shape[2]
    rows_local = phase_volume.shape[1]
    cols_local = phase_volume.shape[2]
    part = jnp.stack(
        [
            jnp.sum(phase_volume, axis=0, dtype=jnp.float32),
            jnp.sum(absorb_volume, axis=0, dtype=jnp.float32),
        ]
    )
    summed = over_copies(part, "beam")
    tall = extended(summed, (("row", 1),), half)
    wide = jnp.stack([from_behind(tall, COL, 1), tall, from_behind(tall, COL, -1)], axis=1)
    damping = jnp.exp(-wide[1])
    t = jnp.stack([damping * jnp.cos(wide[0]), damping * jnp.sin(wide[0])])
    canvas, probe_term, misfit = window_terms(
        t,
        probe,
        amplitudes.reshape(count, length, length),
        scan_rows.reshape(count),
        scan_cols.reshape(count),
    )
    middle = canvas[:, 1] + from_behind(canvas[:, 0], COL, -1) + from_behind(canvas[:, 2], COL, 1)
    center = middle[:, half : half + rows_local]
    below = from_behind(middle[:, :half], "row", -1)
    above = from_behind(middle[:, half + rows_local :], "row", 1)
    center = center + jnp.pad(below, ((0, 0), (rows_local - half, 0), (0, 0)))
    center = center + jnp.pad(above, ((0, 0), (0, rows_local - half), (0, 0)))
    center = over_copies(center, "beam")
    tr = t[0, 1, half : half + rows_local]
    ti = t[1, 1, half : half + rows_local]
    gradient = jnp.stack(
        [tr * center[1] - ti * center[0], -(tr * center[0] + ti * center[1])]
    )
    probe_total, misfit_total = packed_total(
        (probe_term, jnp.sum(misfit)), ("beam", ("row", "col_0", "col_1"))
    )
    square_sum = over_copies(jnp.sum(gradient * gradient), ROW_COL)
    plane_devices = lax.axis_size("row") * lax.axis_size(COL)
    mean_square = square_sum / (2 * rows_local * cols_local * plane_devices)
    factor = jnp.minimum(1.0, 0.5 / jnp.sqrt(mean_square + 1e-06))
    total = plane_devices * lax.axis_size("beam") * count
    return (gradient * factor, probe_total / total, misfit_total / (total * length * length))


def solution(mesh):
    split = Mesh(
        mesh.devices.reshape(mesh.shape["beam"], mesh.shape["row"], 8, 2),
        ("beam", "row", "col_0", "col_1"),
    )
    in_specs = (
        P("beam", "row", COL),
        P("beam", "row", COL),
        P(),
        P("row", COL, "beam", None, None),
        P("row", COL, "beam"),
        P("row", COL, "beam"),
    )
    out_specs = (P(None, "row", COL), P(), P())
    return jax.shard_map(local, mesh=split, in_specs=in_specs, out_specs=out_specs, check_vma=False)
```

```python
import functools
import math

import jax
import jax.numpy as jnp
import numpy as np
from jax import lax
from jax.experimental import pallas as pl
from jax.experimental.pallas import tpu as pltpu
from jax.sharding import Mesh
from jax.sharding import PartitionSpec as P

COL = ("col_0", "col_1")
MESH = pl.DeviceIdType.MESH
LANES = 128
CHUNK = 128


def dft_tables(length):
    indices = np.arange(length, dtype=np.int32)
    product = indices[:, None] * indices[None, :] % length
    angles = product.astype(np.float32) * np.float32(2.0 * math.pi / length)
    factor = np.float32(1.0 / math.sqrt(length))
    return (
        jnp.asarray(np.cos(angles) * factor).astype(jnp.bfloat16),
        jnp.asarray(-np.sin(angles) * factor).astype(jnp.bfloat16),
    )


def window_kernel(
    rows_ref, cols_ref, t_ref, probe_ref, amp_ref, table_ref,
    canvas_ref, probe_sum_ref, misfit_ref,
    fwd, bwd, cut, psi, half, chi, back,
):
    step = pl.program_id(0)
    n = probe_ref.shape[1]

    @pl.when(step == 0)
    def _():
        real, imag = table_ref[0], table_ref[1]
        minus = -imag
        fwd[:n, :n] = real
        fwd[:n, n:] = minus
        fwd[n:, :n] = imag
        fwd[n:, n:] = real
        bwd[:n, :n] = real
        bwd[:n, n:] = imag
        bwd[n:, :n] = minus
        bwd[n:, n:] = real
        canvas_ref[...] = jnp.zeros_like(canvas_ref)
        probe_sum_ref[...] = jnp.zeros_like(probe_sum_ref)
        misfit_ref[...] = jnp.zeros_like(misfit_ref)

    row = rows_ref[step]
    col = cols_ref[step]
    turn = lax.rem(LANES - col, LANES)
    lane = lax.broadcasted_iota(jnp.int32, (32, LANES), 1)
    near = lane < LANES - col
    for at in range(0, n, 32):
        here = pl.ds(at, 32)
        pieces = []
        for part in range(2):
            turned = [
                pltpu.roll(t_ref[part, k, pl.ds(row + at, 32), :], turn, 1) for k in range(3)
            ]
            pieces.append([jnp.where(near, turned[k], turned[k + 1]) for k in range(2)])
        for k in range(2):
            lanes = pl.ds(k * LANES, LANES)
            tr, ti = pieces[0][k], pieces[1][k]
            cut[0, here, lanes] = tr
            cut[1, here, lanes] = ti
            pr = probe_ref[0, here, lanes]
            pi = probe_ref[1, here, lanes]
            psi[here, lanes] = (pr * tr - pi * ti).astype(jnp.bfloat16)
            psi[pl.ds(n + at, 32), lanes] = (pr * ti + pi * tr).astype(jnp.bfloat16)
    for part in range(2):
        half[:, part * n : (part + 1) * n] = jnp.dot(
            fwd[part * n : (part + 1) * n, :], psi[...], preferred_element_type=jnp.float32
        ).astype(jnp.bfloat16)
    total = jnp.zeros((8, LANES), jnp.float32)
    for at in range(0, n, CHUNK):
        here = pl.ds(at, CHUNK)
        far = jnp.dot(half[here, :], bwd[...], preferred_element_type=jnp.float32)
        fr, fi = far[:, :n], far[:, n:]
        amp = amp_ref[0, here, :].astype(jnp.float32)
        power = fr * fr + fi * fi
        inverse = lax.rsqrt(power)
        modulus = jnp.where(power > 0.0, power * inverse, 0.0)
        off = modulus - amp
        square = off * off
        total = total + jnp.sum(
            (square[:, :LANES] + square[:, LANES:]).reshape(CHUNK // 8, 8, LANES), axis=0
        )
        ratio = 1.0 - amp * jnp.minimum(inverse, 2.0)
        chi[here, :] = (fr * ratio).astype(jnp.bfloat16)
        chi[pl.ds(n + at, CHUNK), :] = (fi * ratio).astype(jnp.bfloat16)
    misfit_ref[...] += total
    for part in range(2):
        back[:, part * n : (part + 1) * n] = jnp.dot(
            bwd[part * n : (part + 1) * n, :], chi[...], preferred_element_type=jnp.float32
        ).astype(jnp.bfloat16)
    far_side = lax.broadcasted_iota(jnp.int32, (CHUNK, LANES), 1) >= col
    for at in range(0, n, CHUNK):
        here = pl.ds(at, CHUNK)
        grad = jnp.dot(back[here, :], fwd[...], preferred_element_type=jnp.float32)
        gr, gi = grad[:, :n], grad[:, n:]
        tr, ti = cut[0, here, :], cut[1, here, :]
        probe_sum_ref[0, here, :] += tr * gr + ti * gi
        probe_sum_ref[1, here, :] += tr * gi - ti * gr
        pr, pi = probe_ref[0, here, :], probe_ref[1, here, :]
        for part, value in enumerate((pr * gr + pi * gi, pr * gi - pi * gr)):
            first = pltpu.roll(value[:, :LANES], col, 1)
            second = pltpu.roll(value[:, LANES:], col, 1)
            there = pl.ds(row + at, CHUNK)
            canvas_ref[part, 0, there, :] += jnp.where(far_side, first, 0.0)
            canvas_ref[part, 1, there, :] += jnp.where(far_side, second, first)
            canvas_ref[part, 2, there, :] += jnp.where(far_side, 0.0, second)


def window_terms(t, probe, amplitudes, rows, cols):
    count, n, _ = amplitudes.shape
    grid_spec = pltpu.PrefetchScalarGridSpec(
        num_scalar_prefetch=2,
        grid=(count,),
        in_specs=[
            pl.BlockSpec(t.shape, lambda s, *_: (0, 0, 0, 0)),
            pl.BlockSpec(probe.shape, lambda s, *_: (0, 0, 0)),
            pl.BlockSpec((1, n, n), lambda s, *_: (s, 0, 0)),
            pl.BlockSpec((2, n, n), lambda s, *_: (0, 0, 0)),
        ],
        out_specs=[
            pl.BlockSpec(t.shape, lambda s, *_: (0, 0, 0, 0)),
            pl.BlockSpec(probe.shape, lambda s, *_: (0, 0, 0)),
            pl.BlockSpec((8, LANES), lambda s, *_: (0, 0)),
        ],
        scratch_shapes=[
            pltpu.VMEM((2 * n, 2 * n), jnp.bfloat16),
            pltpu.VMEM((2 * n, 2 * n), jnp.bfloat16),
            pltpu.VMEM((2, n, n), jnp.float32),
            pltpu.VMEM((2 * n, n), jnp.bfloat16),
            pltpu.VMEM((n, 2 * n), jnp.bfloat16),
            pltpu.VMEM((2 * n, n), jnp.bfloat16),
            pltpu.VMEM((n, 2 * n), jnp.bfloat16),
        ],
    )
    return pl.pallas_call(
        window_kernel,
        grid_spec=grid_spec,
        out_shape=[
            jax.ShapeDtypeStruct(t.shape, jnp.float32),
            jax.ShapeDtypeStruct(probe.shape, jnp.float32),
            jax.ShapeDtypeStruct((8, LANES), jnp.float32),
        ],
        compiler_params=pltpu.CompilerParams(dimension_semantics=("arbitrary",)),
        name="windows",
    )(rows, cols, t, probe, amplitudes, jnp.stack(dft_tables(n)))


def places():
    return tuple(lax.axis_index(axis) for axis in ("beam", "row", "col_0", "col_1"))


def sizes():
    return tuple(lax.axis_size(axis) for axis in ("beam", "row", "col_0", "col_1"))


def remote(src, dst, send_sem, recv_sem, **where):
    return pltpu.make_async_remote_copy(
        src_ref=src,
        dst_ref=dst,
        send_sem=send_sem,
        recv_sem=recv_sem,
        device_id=where,
        device_id_type=MESH,
    )


def greet(barrier, **where):
    pl.semaphore_signal(barrier, inc=1, device_id=where, device_id_type=MESH)


def spread_kernel(
    phase_ref, absorb_ref, t_ref, own_ref,
    vol, part, inbox,
    vol_sem, sum_send, sum_recv, beam_send, near_send, out_send, row_send, t_recv,
):
    beams, rows_n, deep_n, _ = sizes()
    b, i, z, c = places()
    h = phase_ref.shape[1] // beams
    top = beams // 2
    blocks = 2 * beams
    half = top * h
    out_z = z - 1 + 2 * c
    has_out = (out_z >= 0) & (out_z < deep_n)
    above, below = i > 0, i < rows_n - 1
    order = [*range(1, beams), 0]
    loads = {}
    for o in order:
        q = lax.rem(b + o, beams)
        for p, ref in enumerate((phase_ref, absorb_ref)):
            loads[o, p] = pltpu.make_async_copy(
                ref.at[:, pl.ds(pl.multiple_of(q * h, h), h), :], vol.at[o, p], vol_sem.at[o, p]
            )
            loads[o, p].start()

    barrier = pltpu.get_barrier_semaphore()
    for o in range(1, beams):
        greet(barrier, beam=lax.rem(b + o, beams))
    greet(barrier, col_1=1 - c)

    @pl.when(has_out)
    def _():
        greet(barrier, col_0=out_z, col_1=1 - c)

    @pl.when(above)
    def _():
        greet(barrier, row=i - 1)

    @pl.when(below)
    def _():
        greet(barrier, row=i + 1)

    pl.semaphore_wait(
        barrier,
        beams + has_out.astype(jnp.int32) + above.astype(jnp.int32) + below.astype(jnp.int32),
    )

    sums = []
    for o in order:
        for p in range(2):
            loads[o, p].wait()
            total = vol[o, p, 0].astype(jnp.float32)
            for d in range(1, phase_ref.shape[0]):
                total = total + vol[o, p, d].astype(jnp.float32)
            part[o, p] = total
        if o:
            copy = remote(
                part.at[o], inbox.at[o], sum_send.at[o], sum_recv.at[o],
                beam=lax.rem(b + o, beams),
            )
            copy.start()
            sums.append(copy)
    for copy in sums:
        copy.wait_recv()
    phase, absorb = part[0, 0], part[0, 1]
    for o in range(1, beams):
        phase = phase + inbox[o, 0]
        absorb = absorb + inbox[o, 1]
    damping = jnp.exp(-absorb)
    tr, ti = damping * jnp.cos(phase), damping * jnp.sin(phase)
    own_ref[0] = tr
    own_ref[1] = ti

    def cell(k, m):
        return t_ref.at[:, k, pl.ds(pl.multiple_of(m * h, h), h), :]

    mine = pl.ds(pl.multiple_of(half + b * h, h), h)
    t_ref[0, 1, mine, :] = tr
    t_ref[1, 1, mine, :] = ti
    m0 = top + b
    waits = []
    ring = []
    for o in [1, *range(3, beams), *range(2, min(3, beams))]:
        copy = remote(
            cell(1, m0), cell(1, m0), beam_send.at[o], t_recv.at[1, m0],
            beam=lax.rem(b + o, beams),
        )
        copy.start()
        waits.append((None, copy))
        ring.append(o)

    def sideways(m, slot, alive):
        near = remote(
            cell(1, m), cell(2 * c, m), near_send.at[slot], t_recv.at[2 * c, m], col_1=1 - c
        )
        far = remote(
            cell(1, m), cell(2 - 2 * c, m), out_send.at[slot], t_recv.at[2 - 2 * c, m],
            col_0=out_z, col_1=1 - c,
        )
        for copy, check in ((near, alive), (far, has_out if alive is None else has_out & alive)):
            if check is None:
                copy.start()
            else:
                pl.when(check)(copy.start)
            waits.append((check, copy))

    def arrived(k, m):
        remote(cell(1, m), cell(k, m), near_send.at[0], t_recv.at[k, m], col_1=1 - c).wait_recv()

    for slot, o in enumerate([0, *ring]):
        q = lax.rem(b + o, beams)
        m = top + q
        if o:
            arrived(1, m)
        upper = q // top
        goal = i - 1 + 2 * upper
        copy = remote(
            cell(1, m),
            cell(1, q - top + (1 - upper) * blocks),
            row_send.at[slot],
            t_recv.at[1, q - top + (1 - upper) * blocks],
            row=goal,
        )
        alive = (goal >= 0) & (goal < rows_n)
        pl.when(alive)(copy.start)
        waits.append((alive, copy))
        sideways(m, slot, None)
    for at in range(top):
        for m, alive in ((at, above), (top + beams + at, below)):
            pl.when(alive)(functools.partial(arrived, 1, m))
            sideways(m, beams + (m if m < top else m - beams), alive)
    for m in range(blocks):
        alive = above if m < top else below if m >= top + beams else None
        if alive is None:
            arrived(2 - 2 * c, m)
            pl.when(has_out)(functools.partial(arrived, 2 * c, m))
        else:
            pl.when(alive)(functools.partial(arrived, 2 - 2 * c, m))
            pl.when(alive & has_out)(functools.partial(arrived, 2 * c, m))
    for copy in sums:
        copy.wait_send()
    for alive, copy in waits:
        if alive is None:
            copy.wait_send()
        else:
            pl.when(alive)(copy.wait_send)
    tall = blocks * h

    def blank(tiles, start, size):
        for k in tiles:
            t_ref[0, k, pl.ds(start, size), :] = jnp.ones((size, LANES), jnp.float32)
            t_ref[1, k, pl.ds(start, size), :] = jnp.zeros((size, LANES), jnp.float32)

    pl.when(i == 0)(lambda: blank(range(3), 0, half))
    pl.when(i == rows_n - 1)(lambda: blank(range(3), tall - half, half))
    pl.when((z == 0) & (c == 0))(lambda: blank((0,), 0, tall))
    pl.when((z == deep_n - 1) & (c == 1))(lambda: blank((2,), 0, tall))


def transmission(phase_volume, absorb_volume):
    deep, rows, lanes = phase_volume.shape
    beams = lax.axis_size("beam")
    h = rows // beams
    return pl.pallas_call(
        spread_kernel,
        out_shape=[
            jax.ShapeDtypeStruct((2, 3, 2 * rows, lanes), jnp.float32),
            jax.ShapeDtypeStruct((2, h, lanes), jnp.float32),
        ],
        in_specs=[pl.BlockSpec(memory_space=pl.ANY)] * 2,
        out_specs=[pl.BlockSpec(memory_space=pltpu.VMEM)] * 2,
        scratch_shapes=[
            pltpu.VMEM((beams, 2, deep, h, lanes), jnp.bfloat16),
            pltpu.VMEM((beams, 2, h, lanes), jnp.float32),
            pltpu.VMEM((beams, 2, h, lanes), jnp.float32),
            pltpu.SemaphoreType.DMA((beams, 2)),
            pltpu.SemaphoreType.DMA((beams,)),
            pltpu.SemaphoreType.DMA((beams,)),
            pltpu.SemaphoreType.DMA((beams,)),
            pltpu.SemaphoreType.DMA((2 * beams,)),
            pltpu.SemaphoreType.DMA((2 * beams,)),
            pltpu.SemaphoreType.DMA((beams,)),
            pltpu.SemaphoreType.DMA((3, 2 * beams)),
        ],
        compiler_params=pltpu.CompilerParams(collective_id=0, has_side_effects=True),
        name="spread",
    )(phase_volume, absorb_volume)


def fold_kernel(
    scale, pixels, canvas_ref, own_ref, probe_ref, misfit_ref,
    step_ref, probe_out, loss_ref,
    sib_in, out_in, acc, row_in, q_in, grad, p_in, p_sum, x_in, z_in, n_xy, n_zc,
    sib_send, sib_recv, out_send, out_recv, row_send, row_recv, q_send, q_recv,
    g_send, g_recv, p_send, p_recv, x_send, x_recv, z_send, z_recv, y_send, y_recv,
    n_send, n_recv, m_send, m_recv,
):
    beams, rows_n, deep_n, cores = sizes()
    b, i, z, c = places()
    rows = grad.shape[1]
    h = rows // beams
    half = rows // 2
    tall = 2 * rows
    plane = beams * rows_n
    across = deep_n * cores
    share = p_sum.shape[0] // plane
    me_xy = b * rows_n + i
    me_zc = z * cores + c
    out_z = z - 1 + 2 * c
    has_out = (out_z >= 0) & (out_z < deep_n)
    above, below = i > 0, i < rows_n - 1
    finish = []

    def go(copy, check=None):
        if check is None:
            copy.start()
        else:
            pl.when(check)(copy.start)
        finish.append((check, copy))
        return copy

    def peer_xy(o):
        return dict(beam=lax.rem(b + o // rows_n, beams), row=lax.rem(i + o % rows_n, rows_n))

    def peer_zc(o):
        return dict(col_0=lax.rem(z + o // cores, deep_n), col_1=lax.rem(c + o % cores, cores))

    barrier = pltpu.get_barrier_semaphore()
    for o in range(1, plane):
        greet(barrier, **peer_xy(o))
    for o in range(1, across):
        greet(barrier, **peer_zc(o))
    pl.semaphore_wait(barrier, plane + across - 2)

    half_copy = go(remote(probe_ref.at[1 - c], p_in, p_send.at[0], p_recv.at[0], col_1=1 - c))
    spans = [(0, half, above), (tall - half, half, below), (half, rows, None)]
    near, far = [], []
    for e, (start, size, alive) in enumerate(spans):
        where = pl.ds(start, size)
        far.append(
            go(
                remote(
                    canvas_ref.at[:, 2 * c, where, :], out_in.at[:, where, :],
                    out_send.at[e], out_recv.at[e], col_0=out_z, col_1=1 - c,
                ),
                has_out if alive is None else has_out & alive,
            )
        )
        near.append(
            go(
                remote(
                    canvas_ref.at[:, 2 - 2 * c, where, :], sib_in.at[:, where, :],
                    sib_send.at[e], sib_recv.at[e], col_1=1 - c,
                ),
                alive,
            )
        )
    half_copy.wait_recv()
    p_sum[...] = probe_ref[c] + p_in[...]
    parts = []
    for o in range(1, plane):
        peer = peer_xy(o)
        there = pl.multiple_of((peer["beam"] * rows_n + peer["row"]) * share, share)
        parts.append(
            go(
                remote(
                    p_sum.at[pl.ds(there, share), :], x_in.at[o], x_send.at[o], x_recv.at[o], **peer
                )
            )
        )

    def merge(e):
        start, size, _ = spans[e]
        where = pl.ds(start, size)
        near[e].wait_recv()
        acc[:, where, :] = canvas_ref[:, 1, where, :] + sib_in[:, where, :]

        @pl.when(has_out)
        def _():
            far[e].wait_recv()
            acc[:, where, :] += out_in[:, where, :]

    rims = []
    for e, goal in ((0, i - 1), (1, i + 1)):
        start, size, alive = spans[e]
        pl.when(alive)(functools.partial(merge, e))
        rims.append(
            go(
                remote(
                    acc.at[:, pl.ds(start, size), :], row_in.at[e],
                    row_send.at[e], row_recv.at[e], row=goal,
                ),
                alive,
            )
        )
    merge(2)

    @pl.when(below)
    def _():
        rims[0].wait_recv()
        acc[:, pl.ds(rows, half), :] += row_in[0]

    @pl.when(above)
    def _():
        rims[1].wait_recv()
        acc[:, pl.ds(half, half), :] += row_in[1]

    quarters = []
    for o in range(1, beams):
        q = lax.rem(b + o, beams)
        there = pl.multiple_of(half + q * h, h)
        quarters.append(
            go(
                remote(
                    acc.at[:, pl.ds(there, h), :], q_in.at[o], q_send.at[o], q_recv.at[o], beam=q
                )
            )
        )
    total = p_sum[pl.ds(pl.multiple_of(me_xy * share, share), share), :]
    for o in range(1, plane):
        parts[o - 1].wait_recv()
        total = total + x_in[o]
    z_in[z] = total
    levels = []
    for o in range(1, deep_n):
        levels.append(
            go(
                remote(
                    z_in.at[z], z_in.at[z], z_send.at[o], z_recv.at[o],
                    col_0=lax.rem(z + o, deep_n),
                )
            )
        )

    mine = pl.ds(pl.multiple_of(half + b * h, h), h)
    cr, ci = acc[0, mine, :], acc[1, mine, :]
    for o in range(1, beams):
        quarters[o - 1].wait_recv()
        cr = cr + q_in[o, 0]
        ci = ci + q_in[o, 1]
    tr, ti = own_ref[0], own_ref[1]
    phase = tr * ci - ti * cr
    absorb = -(tr * cr + ti * ci)
    home = pl.ds(pl.multiple_of(b * h, h), h)
    grad[0, home, :] = phase
    grad[1, home, :] = absorb
    squares = phase * phase + absorb * absorb
    n_xy[me_xy, 0] = jnp.sum(squares.reshape(h // 8, 8, LANES), axis=0)
    n_xy[me_xy, 1] = misfit_ref[...]
    norms = []
    for o in range(1, plane):
        norms.append(
            go(
                remote(
                    n_xy.at[me_xy], n_xy.at[me_xy], n_send.at[o], n_recv.at[o], **peer_xy(o)
                )
            )
        )
    grads = []
    for o in range(1, beams):
        grads.append(
            go(
                remote(
                    grad.at[:, home, :], grad.at[:, home, :], g_send.at[o], g_recv.at[o],
                    beam=lax.rem(b + o, beams),
                )
            )
        )

    for copy in levels:
        copy.wait_recv()
    total = z_in[0]
    for k in range(1, deep_n):
        total = total + z_in[k]
    piece = pl.ds(pl.multiple_of(me_xy * share, share), share)
    probe_out[c, piece, :] = total * scale
    spreads = []
    for o in range(1, plane):
        spreads.append(
            go(
                remote(
                    probe_out.at[c, piece, :], probe_out.at[c, piece, :],
                    y_send.at[o], y_recv.at[o], **peer_xy(o),
                )
            )
        )

    for copy in norms:
        copy.wait_recv()
    pair = n_xy[0]
    for k in range(1, plane):
        pair = pair + n_xy[k]
    n_zc[me_zc] = pair
    norms = []
    for o in range(1, across):
        norms.append(
            go(
                remote(
                    n_zc.at[me_zc], n_zc.at[me_zc], m_send.at[o], m_recv.at[o], **peer_zc(o)
                )
            )
        )
    for copy in spreads:
        copy.wait_recv()
    last = go(remote(probe_out.at[c], probe_out.at[c], p_send.at[1], p_recv.at[1], col_1=1 - c))
    for copy in norms:
        copy.wait_recv()
    pair = n_zc[0]
    for k in range(1, across):
        pair = pair + n_zc[k]
    sums = jnp.sum(jnp.sum(pair, axis=1, keepdims=True), axis=2, keepdims=True)
    mean_square = sums[0] / (2 * rows * LANES * rows_n * across)
    factor = jnp.minimum(1.0, 0.5 / jnp.sqrt(mean_square + 1e-06))
    loss_ref[...] = jnp.broadcast_to(sums[1] * (scale / pixels), loss_ref.shape)
    for copy in grads:
        copy.wait_recv()
    for p in range(2):
        step_ref[p] = grad[p] * factor
    last.wait_recv()
    for check, copy in finish:
        if check is None:
            copy.wait_send()
        else:
            pl.when(check)(copy.wait_send)


def folded(canvas, own, probe_sum, misfit, positions):
    beams, rows_n, deep_n, cores = sizes()
    _, _, tall, lanes = canvas.shape
    rows = tall // 2
    h = rows // beams
    n = probe_sum.shape[1]
    plane, across = beams * rows_n, deep_n * cores
    f32 = functools.partial(pltpu.VMEM, dtype=jnp.float32)
    sems = [3, 3, 3, 3, 2, 2, beams, beams, beams, beams, 2, 2, plane, plane, deep_n, deep_n]
    sems += [plane, plane, plane, plane, across, across]
    return pl.pallas_call(
        functools.partial(fold_kernel, 1.0 / positions, n * n),
        out_shape=[
            jax.ShapeDtypeStruct((2, rows, lanes), jnp.float32),
            jax.ShapeDtypeStruct(probe_sum.shape, jnp.float32),
            jax.ShapeDtypeStruct((8, LANES), jnp.float32),
        ],
        in_specs=[pl.BlockSpec(memory_space=pltpu.VMEM)] * 4,
        out_specs=[pl.BlockSpec(memory_space=pltpu.VMEM)] * 3,
        scratch_shapes=[
            f32((2, tall, lanes)),
            f32((2, tall, lanes)),
            f32((2, tall, lanes)),
            f32((2, 2, rows // 2, lanes)),
            f32((beams, 2, h, lanes)),
            f32((2, rows, lanes)),
            f32((n, n)),
            f32((n, n)),
            f32((plane, n // plane, n)),
            f32((deep_n, n // plane, n)),
            f32((plane, 2, 8, LANES)),
            f32((across, 2, 8, LANES)),
            *[pltpu.SemaphoreType.DMA((count,)) for count in sems],
        ],
        compiler_params=pltpu.CompilerParams(collective_id=1, has_side_effects=True),
        name="fold",
    )(canvas, own, probe_sum, misfit)


def local(phase_volume, absorb_volume, probe, amplitudes, scan_rows, scan_cols):
    length = probe.shape[1]
    count = scan_rows.shape[2]
    beams, rows_n, deep_n, cores = sizes()
    t, own = transmission(phase_volume, absorb_volume)
    canvas, probe_term, misfit = window_terms(
        t,
        probe,
        amplitudes.reshape(count, length, length),
        scan_rows.reshape(count),
        scan_cols.reshape(count),
    )
    step, probe_total, loss = folded(
        canvas, own, probe_term, misfit, beams * rows_n * deep_n * cores * count
    )
    return (step, probe_total, loss[0, 0])


def solution(mesh):
    split = Mesh(
        mesh.devices.reshape(mesh.shape["beam"], mesh.shape["row"], -1, 2),
        ("beam", "row", "col_0", "col_1"),
    )
    in_specs = (
        P("beam", "row", COL),
        P("beam", "row", COL),
        P(),
        P("row", COL, "beam", None, None),
        P("row", COL, "beam"),
        P("row", COL, "beam"),
    )
    out_specs = (P(None, "row", COL), P(), P())
    return jax.shard_map(local, mesh=split, in_specs=in_specs, out_specs=out_specs, check_vma=False)
```

```python
import functools
import math

import jax
import jax.numpy as jnp
import numpy as np
from jax import lax
from jax.experimental import pallas as pl
from jax.experimental.pallas import tpu as pltpu
from jax.sharding import Mesh
from jax.sharding import PartitionSpec as P

COL = ("col_0", "col_1")
MESH = pl.DeviceIdType.MESH
LANES = 128
CHUNK = 128
VMEM_LIMIT = 20 << 20


def dft_tables(length):
    indices = np.arange(length, dtype=np.int32)
    product = indices[:, None] * indices[None, :] % length
    angles = product.astype(np.float32) * np.float32(2.0 * math.pi / length)
    factor = np.float32(1.0 / math.sqrt(length))
    return (
        jnp.asarray(np.cos(angles) * factor).astype(jnp.bfloat16),
        jnp.asarray(-np.sin(angles) * factor).astype(jnp.bfloat16),
    )


def window_kernel(
    rows_ref, cols_ref, t_ref, probe_ref, amp_ref, table_ref,
    canvas_ref, probe_sum_ref, misfit_ref,
    fwd, bwd, cut, psi, half, chi, back,
):
    step = pl.program_id(0)
    n = probe_ref.shape[1]

    @pl.when(step == 0)
    def _():
        real, imag = table_ref[0], table_ref[1]
        minus = -imag
        fwd[:n, :n] = real
        fwd[:n, n:] = minus
        fwd[n:, :n] = imag
        fwd[n:, n:] = real
        bwd[:n, :n] = real
        bwd[:n, n:] = imag
        bwd[n:, :n] = minus
        bwd[n:, n:] = real
        canvas_ref[...] = jnp.zeros_like(canvas_ref)
        probe_sum_ref[...] = jnp.zeros_like(probe_sum_ref)
        misfit_ref[...] = jnp.zeros_like(misfit_ref)

    row = rows_ref[step]
    col = cols_ref[step]
    turn = lax.rem(LANES - col, LANES)
    lane = lax.broadcasted_iota(jnp.int32, (32, LANES), 1)
    near = lane < LANES - col
    for at in range(0, n, 32):
        here = pl.ds(at, 32)
        pieces = []
        for part in range(2):
            turned = [
                pltpu.roll(t_ref[part, k, pl.ds(row + at, 32), :], turn, 1) for k in range(3)
            ]
            pieces.append([jnp.where(near, turned[k], turned[k + 1]) for k in range(2)])
        for k in range(2):
            lanes = pl.ds(k * LANES, LANES)
            tr, ti = pieces[0][k], pieces[1][k]
            cut[0, here, lanes] = tr
            cut[1, here, lanes] = ti
            pr = probe_ref[0, here, lanes]
            pi = probe_ref[1, here, lanes]
            psi[here, lanes] = (pr * tr - pi * ti).astype(jnp.bfloat16)
            psi[pl.ds(n + at, 32), lanes] = (pr * ti + pi * tr).astype(jnp.bfloat16)
    for part in range(2):
        half[:, part * n : (part + 1) * n] = jnp.dot(
            fwd[part * n : (part + 1) * n, :], psi[...], preferred_element_type=jnp.float32
        ).astype(jnp.bfloat16)
    total = jnp.zeros((8, LANES), jnp.float32)
    for at in range(0, n, CHUNK):
        here = pl.ds(at, CHUNK)
        far = jnp.dot(half[here, :], bwd[...], preferred_element_type=jnp.float32)
        fr, fi = far[:, :n], far[:, n:]
        amp = amp_ref[0, here, :].astype(jnp.float32)
        power = fr * fr + fi * fi
        inverse = lax.rsqrt(power)
        modulus = jnp.where(power > 0.0, power * inverse, 0.0)
        off = modulus - amp
        square = off * off
        total = total + jnp.sum(
            (square[:, :LANES] + square[:, LANES:]).reshape(CHUNK // 8, 8, LANES), axis=0
        )
        ratio = 1.0 - amp * jnp.minimum(inverse, 2.0)
        chi[here, :] = (fr * ratio).astype(jnp.bfloat16)
        chi[pl.ds(n + at, CHUNK), :] = (fi * ratio).astype(jnp.bfloat16)
    misfit_ref[...] += total
    for part in range(2):
        back[:, part * n : (part + 1) * n] = jnp.dot(
            bwd[part * n : (part + 1) * n, :], chi[...], preferred_element_type=jnp.float32
        ).astype(jnp.bfloat16)
    far_side = lax.broadcasted_iota(jnp.int32, (CHUNK, LANES), 1) >= col
    for at in range(0, n, CHUNK):
        here = pl.ds(at, CHUNK)
        grad = jnp.dot(back[here, :], fwd[...], preferred_element_type=jnp.float32)
        gr, gi = grad[:, :n], grad[:, n:]
        tr, ti = cut[0, here, :], cut[1, here, :]
        probe_sum_ref[0, here, :] += tr * gr + ti * gi
        probe_sum_ref[1, here, :] += tr * gi - ti * gr
        pr, pi = probe_ref[0, here, :], probe_ref[1, here, :]
        for part, value in enumerate((pr * gr + pi * gi, pr * gi - pi * gr)):
            first = pltpu.roll(value[:, :LANES], col, 1)
            second = pltpu.roll(value[:, LANES:], col, 1)
            there = pl.ds(row + at, CHUNK)
            canvas_ref[part, 0, there, :] += jnp.where(far_side, first, 0.0)
            canvas_ref[part, 1, there, :] += jnp.where(far_side, second, first)
            canvas_ref[part, 2, there, :] += jnp.where(far_side, 0.0, second)


def window_terms(t, probe, amplitudes, rows, cols):
    count, n, _ = amplitudes.shape
    grid_spec = pltpu.PrefetchScalarGridSpec(
        num_scalar_prefetch=2,
        grid=(count,),
        in_specs=[
            pl.BlockSpec(t.shape, lambda s, *_: (0, 0, 0, 0)),
            pl.BlockSpec(probe.shape, lambda s, *_: (0, 0, 0)),
            pl.BlockSpec((1, n, n), lambda s, *_: (s, 0, 0)),
            pl.BlockSpec((2, n, n), lambda s, *_: (0, 0, 0)),
        ],
        out_specs=[
            pl.BlockSpec(t.shape, lambda s, *_: (0, 0, 0, 0)),
            pl.BlockSpec(probe.shape, lambda s, *_: (0, 0, 0)),
            pl.BlockSpec((8, LANES), lambda s, *_: (0, 0)),
        ],
        scratch_shapes=[
            pltpu.VMEM((2 * n, 2 * n), jnp.bfloat16),
            pltpu.VMEM((2 * n, 2 * n), jnp.bfloat16),
            pltpu.VMEM((2, n, n), jnp.float32),
            pltpu.VMEM((2 * n, n), jnp.bfloat16),
            pltpu.VMEM((n, 2 * n), jnp.bfloat16),
            pltpu.VMEM((2 * n, n), jnp.bfloat16),
            pltpu.VMEM((n, 2 * n), jnp.bfloat16),
        ],
    )
    return pl.pallas_call(
        window_kernel,
        grid_spec=grid_spec,
        out_shape=[
            jax.ShapeDtypeStruct(t.shape, jnp.float32),
            jax.ShapeDtypeStruct(probe.shape, jnp.float32),
            jax.ShapeDtypeStruct((8, LANES), jnp.float32),
        ],
        compiler_params=pltpu.CompilerParams(dimension_semantics=("arbitrary",), vmem_limit_bytes=VMEM_LIMIT),
        name="windows",
    )(rows, cols, t, probe, amplitudes, jnp.stack(dft_tables(n)))


def places():
    return tuple(lax.axis_index(axis) for axis in ("beam", "row", "col_0", "col_1"))


def sizes():
    return tuple(lax.axis_size(axis) for axis in ("beam", "row", "col_0", "col_1"))


def remote(src, dst, send_sem, recv_sem, **where):
    return pltpu.make_async_remote_copy(
        src_ref=src,
        dst_ref=dst,
        send_sem=send_sem,
        recv_sem=recv_sem,
        device_id=where,
        device_id_type=MESH,
    )


def greet(barrier, **where):
    pl.semaphore_signal(barrier, inc=1, device_id=where, device_id_type=MESH)


def spread_kernel(
    phase_ref, absorb_ref, t_ref, own_ref,
    vol, part, inbox,
    vol_sem, sum_send, sum_recv, beam_send, near_send, out_send, row_send, t_recv,
):
    beams, rows_n, deep_n, _ = sizes()
    b, i, z, c = places()
    h = phase_ref.shape[1] // beams
    top = beams // 2
    blocks = 2 * beams
    half = top * h
    out_z = z - 1 + 2 * c
    has_out = (out_z >= 0) & (out_z < deep_n)
    above, below = i > 0, i < rows_n - 1
    order = [*range(1, beams), 0]
    loads = {}
    for o in order:
        q = lax.rem(b + o, beams)
        for p, ref in enumerate((phase_ref, absorb_ref)):
            loads[o, p] = pltpu.make_async_copy(
                ref.at[:, pl.ds(pl.multiple_of(q * h, h), h), :], vol.at[o, p], vol_sem.at[o, p]
            )
            loads[o, p].start()

    barrier = pltpu.get_barrier_semaphore()
    for o in range(1, beams):
        greet(barrier, beam=lax.rem(b + o, beams))
    greet(barrier, col_1=1 - c)

    @pl.when(has_out)
    def _():
        greet(barrier, col_0=out_z, col_1=1 - c)

    @pl.when(above)
    def _():
        greet(barrier, row=i - 1)

    @pl.when(below)
    def _():
        greet(barrier, row=i + 1)

    pl.semaphore_wait(
        barrier,
        beams + has_out.astype(jnp.int32) + above.astype(jnp.int32) + below.astype(jnp.int32),
    )

    sums = []
    for o in order:
        for p in range(2):
            loads[o, p].wait()
            total = vol[o, p, 0].astype(jnp.float32)
            for d in range(1, phase_ref.shape[0]):
                total = total + vol[o, p, d].astype(jnp.float32)
            part[o, p] = total
        if o:
            copy = remote(
                part.at[o], inbox.at[o], sum_send.at[o], sum_recv.at[o],
                beam=lax.rem(b + o, beams),
            )
            copy.start()
            sums.append(copy)
    for copy in sums:
        copy.wait_recv()
    phase, absorb = part[0, 0], part[0, 1]
    for o in range(1, beams):
        phase = phase + inbox[o, 0]
        absorb = absorb + inbox[o, 1]
    damping = jnp.exp(-absorb)
    tr, ti = damping * jnp.cos(phase), damping * jnp.sin(phase)
    own_ref[0] = tr
    own_ref[1] = ti

    def cell(k, m):
        return t_ref.at[:, k, pl.ds(pl.multiple_of(m * h, h), h), :]

    mine = pl.ds(pl.multiple_of(half + b * h, h), h)
    t_ref[0, 1, mine, :] = tr
    t_ref[1, 1, mine, :] = ti
    m0 = top + b
    waits = []
    ring = []
    for o in [1, *range(3, beams), *range(2, min(3, beams))]:
        copy = remote(
            cell(1, m0), cell(1, m0), beam_send.at[o], t_recv.at[1, m0],
            beam=lax.rem(b + o, beams),
        )
        copy.start()
        waits.append((None, copy))
        ring.append(o)

    def sideways(m, slot, alive):
        near = remote(
            cell(1, m), cell(2 * c, m), near_send.at[slot], t_recv.at[2 * c, m], col_1=1 - c
        )
        far = remote(
            cell(1, m), cell(2 - 2 * c, m), out_send.at[slot], t_recv.at[2 - 2 * c, m],
            col_0=out_z, col_1=1 - c,
        )
        for copy, check in ((near, alive), (far, has_out if alive is None else has_out & alive)):
            if check is None:
                copy.start()
            else:
                pl.when(check)(copy.start)
            waits.append((check, copy))

    def arrived(k, m):
        remote(cell(1, m), cell(k, m), near_send.at[0], t_recv.at[k, m], col_1=1 - c).wait_recv()

    for slot, o in enumerate([0, *ring]):
        q = lax.rem(b + o, beams)
        m = top + q
        if o:
            arrived(1, m)
        upper = q // top
        goal = i - 1 + 2 * upper
        copy = remote(
            cell(1, m),
            cell(1, q - top + (1 - upper) * blocks),
            row_send.at[slot],
            t_recv.at[1, q - top + (1 - upper) * blocks],
            row=goal,
        )
        alive = (goal >= 0) & (goal < rows_n)
        pl.when(alive)(copy.start)
        waits.append((alive, copy))
        sideways(m, slot, None)
    for at in range(top):
        for m, alive in ((at, above), (top + beams + at, below)):
            pl.when(alive)(functools.partial(arrived, 1, m))
            sideways(m, beams + (m if m < top else m - beams), alive)
    for m in range(blocks):
        alive = above if m < top else below if m >= top + beams else None
        if alive is None:
            arrived(2 - 2 * c, m)
            pl.when(has_out)(functools.partial(arrived, 2 * c, m))
        else:
            pl.when(alive)(functools.partial(arrived, 2 - 2 * c, m))
            pl.when(alive & has_out)(functools.partial(arrived, 2 * c, m))
    for copy in sums:
        copy.wait_send()
    for alive, copy in waits:
        if alive is None:
            copy.wait_send()
        else:
            pl.when(alive)(copy.wait_send)
    tall = blocks * h

    def blank(tiles, start, size):
        for k in tiles:
            t_ref[0, k, pl.ds(start, size), :] = jnp.ones((size, LANES), jnp.float32)
            t_ref[1, k, pl.ds(start, size), :] = jnp.zeros((size, LANES), jnp.float32)

    pl.when(i == 0)(lambda: blank(range(3), 0, half))
    pl.when(i == rows_n - 1)(lambda: blank(range(3), tall - half, half))
    pl.when((z == 0) & (c == 0))(lambda: blank((0,), 0, tall))
    pl.when((z == deep_n - 1) & (c == 1))(lambda: blank((2,), 0, tall))


def transmission(phase_volume, absorb_volume):
    deep, rows, lanes = phase_volume.shape
    beams = lax.axis_size("beam")
    h = rows // beams
    return pl.pallas_call(
        spread_kernel,
        out_shape=[
            jax.ShapeDtypeStruct((2, 3, 2 * rows, lanes), jnp.float32),
            jax.ShapeDtypeStruct((2, h, lanes), jnp.float32),
        ],
        in_specs=[pl.BlockSpec(memory_space=pltpu.HBM)] * 2,
        out_specs=[pl.BlockSpec(memory_space=pltpu.VMEM)] * 2,
        scratch_shapes=[
            pltpu.VMEM((beams, 2, deep, h, lanes), jnp.bfloat16),
            pltpu.VMEM((beams, 2, h, lanes), jnp.float32),
            pltpu.VMEM((beams, 2, h, lanes), jnp.float32),
            pltpu.SemaphoreType.DMA((beams, 2)),
            pltpu.SemaphoreType.DMA((beams,)),
            pltpu.SemaphoreType.DMA((beams,)),
            pltpu.SemaphoreType.DMA((beams,)),
            pltpu.SemaphoreType.DMA((2 * beams,)),
            pltpu.SemaphoreType.DMA((2 * beams,)),
            pltpu.SemaphoreType.DMA((beams,)),
            pltpu.SemaphoreType.DMA((3, 2 * beams)),
        ],
        compiler_params=pltpu.CompilerParams(
            collective_id=0, has_side_effects=True, vmem_limit_bytes=VMEM_LIMIT
        ),
        name="spread",
    )(phase_volume, absorb_volume)


def fold_kernel(
    scale, canvas_ref, own_ref, probe_ref, misfit_ref,
    grad, probe_out, sums_ref,
    sib_in, out_in, acc, row_in, q_in, p_in, p_sum, x_in, z_in, n_xy, n_zc,
    sib_send, sib_recv, out_send, out_recv, row_send, row_recv, q_send, q_recv,
    g_send, g_recv, p_send, p_recv, x_send, x_recv, z_send, z_recv, y_send, y_recv,
    n_send, n_recv, m_send, m_recv,
):
    beams, rows_n, deep_n, cores = sizes()
    b, i, z, c = places()
    rows = grad.shape[1]
    h = rows // beams
    half = rows // 2
    tall = 2 * rows
    plane = beams * rows_n
    across = deep_n * cores
    share = p_sum.shape[0] // plane
    me_xy = b * rows_n + i
    me_zc = z * cores + c
    out_z = z - 1 + 2 * c
    has_out = (out_z >= 0) & (out_z < deep_n)
    above, below = i > 0, i < rows_n - 1
    finish = []

    def go(copy, check=None):
        if check is None:
            copy.start()
        else:
            pl.when(check)(copy.start)
        finish.append((check, copy))
        return copy

    def peer_xy(o):
        return dict(beam=lax.rem(b + o // rows_n, beams), row=lax.rem(i + o % rows_n, rows_n))

    def peer_zc(o):
        return dict(col_0=lax.rem(z + o // cores, deep_n), col_1=lax.rem(c + o % cores, cores))

    barrier = pltpu.get_barrier_semaphore()
    for o in range(1, plane):
        greet(barrier, **peer_xy(o))
    for o in range(1, across):
        greet(barrier, **peer_zc(o))
    pl.semaphore_wait(barrier, plane + across - 2)

    half_copy = go(remote(probe_ref.at[1 - c], p_in, p_send.at[0], p_recv.at[0], col_1=1 - c))
    spans = [(0, half, above), (tall - half, half, below), (half, rows, None)]
    near, far = [], []
    for e, (start, size, alive) in enumerate(spans):
        where = pl.ds(start, size)
        far.append(
            go(
                remote(
                    canvas_ref.at[:, 2 * c, where, :], out_in.at[:, where, :],
                    out_send.at[e], out_recv.at[e], col_0=out_z, col_1=1 - c,
                ),
                has_out if alive is None else has_out & alive,
            )
        )
        near.append(
            go(
                remote(
                    canvas_ref.at[:, 2 - 2 * c, where, :], sib_in.at[:, where, :],
                    sib_send.at[e], sib_recv.at[e], col_1=1 - c,
                ),
                alive,
            )
        )
    half_copy.wait_recv()
    p_sum[...] = probe_ref[c] + p_in[...]
    parts = []
    for o in range(1, plane):
        peer = peer_xy(o)
        there = pl.multiple_of((peer["beam"] * rows_n + peer["row"]) * share, share)
        parts.append(
            go(
                remote(
                    p_sum.at[pl.ds(there, share), :], x_in.at[o], x_send.at[o], x_recv.at[o], **peer
                )
            )
        )

    def merge(e):
        start, size, _ = spans[e]
        where = pl.ds(start, size)
        near[e].wait_recv()
        acc[:, where, :] = canvas_ref[:, 1, where, :] + sib_in[:, where, :]

        @pl.when(has_out)
        def _():
            far[e].wait_recv()
            acc[:, where, :] += out_in[:, where, :]

    rims = []
    for e, goal in ((0, i - 1), (1, i + 1)):
        start, size, alive = spans[e]
        pl.when(alive)(functools.partial(merge, e))
        rims.append(
            go(
                remote(
                    acc.at[:, pl.ds(start, size), :], row_in.at[e],
                    row_send.at[e], row_recv.at[e], row=goal,
                ),
                alive,
            )
        )
    merge(2)

    @pl.when(below)
    def _():
        rims[0].wait_recv()
        acc[:, pl.ds(rows, half), :] += row_in[0]

    @pl.when(above)
    def _():
        rims[1].wait_recv()
        acc[:, pl.ds(half, half), :] += row_in[1]

    quarters = []
    for o in range(1, beams):
        q = lax.rem(b + o, beams)
        there = pl.multiple_of(half + q * h, h)
        quarters.append(
            go(
                remote(
                    acc.at[:, pl.ds(there, h), :], q_in.at[o], q_send.at[o], q_recv.at[o], beam=q
                )
            )
        )
    total = p_sum[pl.ds(pl.multiple_of(me_xy * share, share), share), :]
    for o in range(1, plane):
        parts[o - 1].wait_recv()
        total = total + x_in[o]
    z_in[z] = total
    levels = []
    for o in range(1, deep_n):
        levels.append(
            go(
                remote(
                    z_in.at[z], z_in.at[z], z_send.at[o], z_recv.at[o],
                    col_0=lax.rem(z + o, deep_n),
                )
            )
        )

    mine = pl.ds(pl.multiple_of(half + b * h, h), h)
    cr, ci = acc[0, mine, :], acc[1, mine, :]
    for o in range(1, beams):
        quarters[o - 1].wait_recv()
        cr = cr + q_in[o, 0]
        ci = ci + q_in[o, 1]
    tr, ti = own_ref[0], own_ref[1]
    phase = tr * ci - ti * cr
    absorb = -(tr * cr + ti * ci)
    home = pl.ds(pl.multiple_of(b * h, h), h)
    grad[0, home, :] = phase
    grad[1, home, :] = absorb
    squares = jnp.sum(phase * phase + absorb * absorb, axis=0, keepdims=True)
    misfits = jnp.sum(misfit_ref[...], axis=0, keepdims=True)
    left = lax.broadcasted_iota(jnp.int32, (1, LANES), 1) < LANES // 2
    n_xy[me_xy] = jnp.where(
        left,
        squares + pltpu.roll(squares, LANES // 2, 1),
        misfits + pltpu.roll(misfits, LANES // 2, 1),
    )
    norms = []
    for o in range(1, plane):
        norms.append(
            go(
                remote(
                    n_xy.at[me_xy], n_xy.at[me_xy], n_send.at[o], n_recv.at[o], **peer_xy(o)
                )
            )
        )
    grads = []
    for o in range(1, beams):
        grads.append(
            go(
                remote(
                    grad.at[:, home, :], grad.at[:, home, :], g_send.at[o], g_recv.at[o],
                    beam=lax.rem(b + o, beams),
                )
            )
        )

    for copy in levels:
        copy.wait_recv()
    total = z_in[0]
    for k in range(1, deep_n):
        total = total + z_in[k]
    piece = pl.ds(pl.multiple_of(me_xy * share, share), share)
    probe_out[c, piece, :] = total * scale
    spreads = []
    for o in range(1, plane):
        spreads.append(
            go(
                remote(
                    probe_out.at[c, piece, :], probe_out.at[c, piece, :],
                    y_send.at[o], y_recv.at[o], **peer_xy(o),
                )
            )
        )

    for copy in norms:
        copy.wait_recv()
    pair = n_xy[0]
    for k in range(1, plane):
        pair = pair + n_xy[k]
    n_zc[me_zc] = pair
    norms = []
    for o in range(1, across):
        norms.append(
            go(
                remote(
                    n_zc.at[me_zc], n_zc.at[me_zc], m_send.at[o], m_recv.at[o], **peer_zc(o)
                )
            )
        )
    for copy in spreads:
        copy.wait_recv()
    last = go(remote(probe_out.at[c], probe_out.at[c], p_send.at[1], p_recv.at[1], col_1=1 - c))
    for copy in norms:
        copy.wait_recv()
    pair = n_zc[0]
    for k in range(1, across):
        pair = pair + n_zc[k]
    sums_ref[...] = pair
    for copy in grads:
        copy.wait_recv()
    last.wait_recv()
    for check, copy in finish:
        if check is None:
            copy.wait_send()
        else:
            pl.when(check)(copy.wait_send)


def folded(canvas, own, probe_sum, misfit, positions):
    beams, rows_n, deep_n, cores = sizes()
    _, _, tall, lanes = canvas.shape
    rows = tall // 2
    h = rows // beams
    n = probe_sum.shape[1]
    plane, across = beams * rows_n, deep_n * cores
    f32 = functools.partial(pltpu.VMEM, dtype=jnp.float32)
    sems = [3, 3, 3, 3, 2, 2, beams, beams, beams, beams, 2, 2, plane, plane, deep_n, deep_n]
    sems += [plane, plane, plane, plane, across, across]
    return pl.pallas_call(
        functools.partial(fold_kernel, 1.0 / positions),
        out_shape=[
            jax.ShapeDtypeStruct((2, rows, lanes), jnp.float32),
            jax.ShapeDtypeStruct(probe_sum.shape, jnp.float32),
            jax.ShapeDtypeStruct((1, LANES), jnp.float32),
        ],
        in_specs=[pl.BlockSpec(memory_space=pltpu.VMEM)] * 4,
        out_specs=[pl.BlockSpec(memory_space=pltpu.VMEM)] * 3,
        scratch_shapes=[
            f32((2, tall, lanes)),
            f32((2, tall, lanes)),
            f32((2, tall, lanes)),
            f32((2, 2, rows // 2, lanes)),
            f32((beams, 2, h, lanes)),
            f32((n, n)),
            f32((n, n)),
            f32((plane, n // plane, n)),
            f32((deep_n, n // plane, n)),
            f32((plane, 1, LANES)),
            f32((across, 1, LANES)),
            *[pltpu.SemaphoreType.DMA((count,)) for count in sems],
        ],
        compiler_params=pltpu.CompilerParams(
            collective_id=1, has_side_effects=True, vmem_limit_bytes=VMEM_LIMIT
        ),
        name="fold",
    )(canvas, own, probe_sum, misfit)


def finish_kernel(entries, terms, grad_ref, probe_ref, sums_ref, step_ref, probe_out, loss_ref):
    sums = sums_ref[...]
    left = lax.broadcasted_iota(jnp.int32, sums.shape, 1) < LANES // 2
    square = jnp.sum(jnp.where(left, sums, 0.0), axis=1, keepdims=True)
    factor = jnp.minimum(1.0, 0.5 / jnp.sqrt(square / entries + 1e-06))
    for p in range(2):
        step_ref[p] = grad_ref[p] * factor
    probe_out[...] = probe_ref[...]
    loss_ref[...] = jnp.sum(jnp.where(left, 0.0, sums), axis=1, keepdims=True) / terms


def finished(grad, probe_total, sums, entries, terms):
    vmem = pl.BlockSpec(memory_space=pltpu.VMEM)
    return pl.pallas_call(
        functools.partial(finish_kernel, entries, terms),
        out_shape=[
            jax.ShapeDtypeStruct(grad.shape, jnp.float32),
            jax.ShapeDtypeStruct(probe_total.shape, jnp.float32),
            jax.ShapeDtypeStruct((1, 1), jnp.float32),
        ],
        in_specs=[vmem] * 3,
        out_specs=[vmem] * 3,
        compiler_params=pltpu.CompilerParams(vmem_limit_bytes=VMEM_LIMIT),
        name="finish",
    )(grad, probe_total, sums)


def local(phase_volume, absorb_volume, probe, amplitudes, scan_rows, scan_cols):
    length = probe.shape[1]
    count = scan_rows.shape[2]
    beams, rows_n, deep_n, cores = sizes()
    t, own = transmission(phase_volume, absorb_volume)
    canvas, probe_term, misfit = window_terms(
        t,
        probe,
        amplitudes.reshape(count, length, length),
        scan_rows.reshape(count),
        scan_cols.reshape(count),
    )
    positions = beams * rows_n * deep_n * cores * count
    grad, probe_total, sums = folded(canvas, own, probe_term, misfit, positions)
    entries = grad.size * rows_n * deep_n * cores
    step, probe_total, loss = finished(
        grad, probe_total, sums, entries, positions * length * length
    )
    return (step, probe_total, loss[0, 0])


def solution(mesh):
    split = Mesh(
        mesh.devices.reshape(mesh.shape["beam"], mesh.shape["row"], -1, 2),
        ("beam", "row", "col_0", "col_1"),
    )
    in_specs = (
        P("beam", "row", COL),
        P("beam", "row", COL),
        P(),
        P("row", COL, "beam", None, None),
        P("row", COL, "beam"),
        P("row", COL, "beam"),
    )
    out_specs = (P(None, "row", COL), P(), P())
    return jax.shard_map(local, mesh=split, in_specs=in_specs, out_specs=out_specs, check_vma=False)
```

```python
import functools
import math

import jax
import jax.numpy as jnp
import numpy as np
from jax import lax
from jax.experimental import pallas as pl
from jax.experimental.pallas import tpu as pltpu
from jax.sharding import Mesh
from jax.sharding import PartitionSpec as P

COL = ("col_0", "col_1")
MESH = pl.DeviceIdType.MESH
LANES = 128
CHUNK = 128
VMEM_LIMIT = 20 << 20


def dft_tables(length):
    indices = np.arange(length, dtype=np.int32)
    product = indices[:, None] * indices[None, :] % length
    angles = product.astype(np.float32) * np.float32(2.0 * math.pi / length)
    factor = np.float32(1.0 / math.sqrt(length))
    return (
        jnp.asarray(np.cos(angles) * factor).astype(jnp.bfloat16),
        jnp.asarray(-np.sin(angles) * factor).astype(jnp.bfloat16),
    )


def window_kernel(
    rows_ref, cols_ref, t_ref, probe_ref, amp_ref, table_ref,
    canvas_ref, probe_sum_ref, misfit_ref,
    fwd, bwd, cut, psi, half, chi, back,
):
    step = pl.program_id(0)
    n = probe_ref.shape[1]

    @pl.when(step == 0)
    def _():
        real, imag = table_ref[0], table_ref[1]
        minus = -imag
        fwd[:n, :n] = real
        fwd[:n, n:] = minus
        fwd[n:, :n] = imag
        fwd[n:, n:] = real
        bwd[:n, :n] = real
        bwd[:n, n:] = imag
        bwd[n:, :n] = minus
        bwd[n:, n:] = real
        canvas_ref[...] = jnp.zeros_like(canvas_ref)
        probe_sum_ref[...] = jnp.zeros_like(probe_sum_ref)
        misfit_ref[...] = jnp.zeros_like(misfit_ref)

    row = rows_ref[step]
    col = cols_ref[step]
    turn = lax.rem(LANES - col, LANES)
    lane = lax.broadcasted_iota(jnp.int32, (32, LANES), 1)
    near = lane < LANES - col
    for at in range(0, n, 32):
        here = pl.ds(at, 32)
        pieces = []
        for part in range(2):
            turned = [
                pltpu.roll(t_ref[part, k, pl.ds(row + at, 32), :], turn, 1) for k in range(3)
            ]
            pieces.append([jnp.where(near, turned[k], turned[k + 1]) for k in range(2)])
        for k in range(2):
            lanes = pl.ds(k * LANES, LANES)
            tr, ti = pieces[0][k], pieces[1][k]
            cut[0, here, lanes] = tr
            cut[1, here, lanes] = ti
            pr = probe_ref[0, here, lanes]
            pi = probe_ref[1, here, lanes]
            psi[here, lanes] = (pr * tr - pi * ti).astype(jnp.bfloat16)
            psi[pl.ds(n + at, 32), lanes] = (pr * ti + pi * tr).astype(jnp.bfloat16)
    for part in range(2):
        half[:, part * n : (part + 1) * n] = jnp.dot(
            fwd[part * n : (part + 1) * n, :], psi[...], preferred_element_type=jnp.float32
        ).astype(jnp.bfloat16)
    total = jnp.zeros((8, LANES), jnp.float32)
    for at in range(0, n, CHUNK):
        here = pl.ds(at, CHUNK)
        far = jnp.dot(half[here, :], bwd[...], preferred_element_type=jnp.float32)
        fr, fi = far[:, :n], far[:, n:]
        amp = amp_ref[0, here, :].astype(jnp.float32)
        power = fr * fr + fi * fi
        inverse = lax.rsqrt(power)
        modulus = jnp.where(power > 0.0, power * inverse, 0.0)
        off = modulus - amp
        square = off * off
        total = total + jnp.sum(
            (square[:, :LANES] + square[:, LANES:]).reshape(CHUNK // 8, 8, LANES), axis=0
        )
        ratio = 1.0 - amp * jnp.minimum(inverse, 2.0)
        chi[here, :] = (fr * ratio).astype(jnp.bfloat16)
        chi[pl.ds(n + at, CHUNK), :] = (fi * ratio).astype(jnp.bfloat16)
    misfit_ref[...] += total
    for part in range(2):
        back[:, part * n : (part + 1) * n] = jnp.dot(
            bwd[part * n : (part + 1) * n, :], chi[...], preferred_element_type=jnp.float32
        ).astype(jnp.bfloat16)
    far_side = lax.broadcasted_iota(jnp.int32, (CHUNK, LANES), 1) >= col
    for at in range(0, n, CHUNK):
        here = pl.ds(at, CHUNK)
        grad = jnp.dot(back[here, :], fwd[...], preferred_element_type=jnp.float32)
        gr, gi = grad[:, :n], grad[:, n:]
        tr, ti = cut[0, here, :], cut[1, here, :]
        probe_sum_ref[0, here, :] += tr * gr + ti * gi
        probe_sum_ref[1, here, :] += tr * gi - ti * gr
        pr, pi = probe_ref[0, here, :], probe_ref[1, here, :]
        for part, value in enumerate((pr * gr + pi * gi, pr * gi - pi * gr)):
            first = pltpu.roll(value[:, :LANES], col, 1)
            second = pltpu.roll(value[:, LANES:], col, 1)
            there = pl.ds(row + at, CHUNK)
            canvas_ref[part, 0, there, :] += jnp.where(far_side, first, 0.0)
            canvas_ref[part, 1, there, :] += jnp.where(far_side, second, first)
            canvas_ref[part, 2, there, :] += jnp.where(far_side, 0.0, second)


def window_terms(t, probe, amplitudes, rows, cols):
    count, n, _ = amplitudes.shape
    grid_spec = pltpu.PrefetchScalarGridSpec(
        num_scalar_prefetch=2,
        grid=(count,),
        in_specs=[
            pl.BlockSpec(t.shape, lambda s, *_: (0, 0, 0, 0)),
            pl.BlockSpec(probe.shape, lambda s, *_: (0, 0, 0)),
            pl.BlockSpec((1, n, n), lambda s, *_: (s, 0, 0)),
            pl.BlockSpec((2, n, n), lambda s, *_: (0, 0, 0)),
        ],
        out_specs=[
            pl.BlockSpec(t.shape, lambda s, *_: (0, 0, 0, 0)),
            pl.BlockSpec(probe.shape, lambda s, *_: (0, 0, 0)),
            pl.BlockSpec((8, LANES), lambda s, *_: (0, 0)),
        ],
        scratch_shapes=[
            pltpu.VMEM((2 * n, 2 * n), jnp.bfloat16),
            pltpu.VMEM((2 * n, 2 * n), jnp.bfloat16),
            pltpu.VMEM((2, n, n), jnp.float32),
            pltpu.VMEM((2 * n, n), jnp.bfloat16),
            pltpu.VMEM((n, 2 * n), jnp.bfloat16),
            pltpu.VMEM((2 * n, n), jnp.bfloat16),
            pltpu.VMEM((n, 2 * n), jnp.bfloat16),
        ],
    )
    return pl.pallas_call(
        window_kernel,
        grid_spec=grid_spec,
        out_shape=[
            jax.ShapeDtypeStruct(t.shape, jnp.float32),
            jax.ShapeDtypeStruct(probe.shape, jnp.float32),
            jax.ShapeDtypeStruct((8, LANES), jnp.float32),
        ],
        compiler_params=pltpu.CompilerParams(dimension_semantics=("arbitrary",), vmem_limit_bytes=VMEM_LIMIT),
        name="windows",
    )(rows, cols, t, probe, amplitudes, jnp.stack(dft_tables(n)))


def places():
    return tuple(lax.axis_index(axis) for axis in ("beam", "row", "col_0", "col_1"))


def sizes():
    return tuple(lax.axis_size(axis) for axis in ("beam", "row", "col_0", "col_1"))


def remote(src, dst, send_sem, recv_sem, **where):
    return pltpu.make_async_remote_copy(
        src_ref=src,
        dst_ref=dst,
        send_sem=send_sem,
        recv_sem=recv_sem,
        device_id=where,
        device_id_type=MESH,
    )


def greet(barrier, **where):
    pl.semaphore_signal(barrier, inc=1, device_id=where, device_id_type=MESH)


def spread_kernel(
    phase_ref, absorb_ref, t_ref, own_ref,
    vol, part, inbox,
    vol_sem, sum_send, sum_recv, beam_send, near_send, out_send, row_send, t_recv,
):
    beams, rows_n, deep_n, _ = sizes()
    b, i, z, c = places()
    h = phase_ref.shape[1] // beams
    top = beams // 2
    blocks = 2 * beams
    half = top * h
    out_z = z - 1 + 2 * c
    has_out = (out_z >= 0) & (out_z < deep_n)
    above, below = i > 0, i < rows_n - 1
    order = [*range(1, beams), 0]
    loads = {}
    for o in order:
        q = lax.rem(b + o, beams)
        for p, ref in enumerate((phase_ref, absorb_ref)):
            loads[o, p] = pltpu.make_async_copy(
                ref.at[:, pl.ds(pl.multiple_of(q * h, h), h), :], vol.at[o, p], vol_sem.at[o, p]
            )
            loads[o, p].start()

    barrier = pltpu.get_barrier_semaphore()
    for o in range(1, beams):
        greet(barrier, beam=lax.rem(b + o, beams))
    greet(barrier, col_1=1 - c)

    @pl.when(has_out)
    def _():
        greet(barrier, col_0=out_z, col_1=1 - c)

    @pl.when(above)
    def _():
        greet(barrier, row=i - 1)

    @pl.when(below)
    def _():
        greet(barrier, row=i + 1)

    for o in order:
        for p in range(2):
            loads[o, p].wait()
            total = vol[o, p, 0].astype(jnp.float32)
            for d in range(1, phase_ref.shape[0]):
                total = total + vol[o, p, d].astype(jnp.float32)
            part[o, p] = total
    pl.semaphore_wait(
        barrier,
        beams + has_out.astype(jnp.int32) + above.astype(jnp.int32) + below.astype(jnp.int32),
    )
    sums = []
    for o in order[:-1]:
        copy = remote(
            part.at[o], inbox.at[o], sum_send.at[o], sum_recv.at[o], beam=lax.rem(b + o, beams)
        )
        copy.start()
        sums.append(copy)
    for copy in sums:
        copy.wait_recv()
    phase, absorb = part[0, 0], part[0, 1]
    for o in range(1, beams):
        phase = phase + inbox[o, 0]
        absorb = absorb + inbox[o, 1]
    damping = jnp.exp(-absorb)
    tr, ti = damping * jnp.cos(phase), damping * jnp.sin(phase)
    own_ref[0] = tr
    own_ref[1] = ti

    def cell(k, m):
        return t_ref.at[:, k, pl.ds(pl.multiple_of(m * h, h), h), :]

    mine = pl.ds(pl.multiple_of(half + b * h, h), h)
    t_ref[0, 1, mine, :] = tr
    t_ref[1, 1, mine, :] = ti
    m0 = top + b
    waits = []

    def send(copy, check=None):
        if check is None:
            copy.start()
        else:
            pl.when(check)(copy.start)
        waits.append((check, copy))

    def arrived(k, m, check=None):
        wait = remote(cell(1, m), cell(k, m), near_send.at[0], t_recv.at[k, m], col_1=1 - c).wait_recv
        if check is None:
            wait()
        else:
            pl.when(check)(wait)

    def both(first, second):
        return second if first is None else first & second

    def to_sibling(m, slot, check=None):
        send(
            remote(
                cell(1, m), cell(2 * c, m), near_send.at[slot], t_recv.at[2 * c, m], col_1=1 - c
            ),
            check,
        )

    def to_outer(m, slot, check=None):
        send(
            remote(
                cell(1, m), cell(2 - 2 * c, m), out_send.at[slot], t_recv.at[2 - 2 * c, m],
                col_0=out_z, col_1=1 - c,
            ),
            both(check, has_out),
        )

    def quarter(o):
        q = lax.rem(b + o, beams)
        upper = q // top
        rim = q - top + (1 - upper) * blocks
        goal, source = i - 1 + 2 * upper, i + 1 - 2 * upper
        return top + q, rim, goal, (goal >= 0) & (goal < rows_n), (source >= 0) & (source < rows_n)

    def to_row(o, k, slot, check=None):
        m, rim, goal, alive, _ = quarter(o)
        send(
            remote(cell(k, m), cell(k, rim), row_send.at[slot], t_recv.at[k, rim], row=goal),
            both(check, alive),
        )

    ring = [1, *range(3, beams), *range(2, min(3, beams))]
    by_row = {0, 2}
    for o in ring:
        send(
            remote(
                cell(1, m0), cell(1, m0), beam_send.at[o], t_recv.at[1, m0],
                beam=lax.rem(b + o, beams),
            )
        )

    def spread_tile(o):
        m = quarter(o)[0]
        if o:
            arrived(1, m)
        to_outer(m, o)
        to_row(o, 1, o)
        to_sibling(m, o)

    def spread_rim(o):
        _, rim, _, _, alive = quarter(o)
        arrived(1, rim, alive)
        if o not in by_row:
            to_outer(rim, beams + o, alive)
        to_sibling(rim, beams + o, alive)

    def spread_corner(o):
        m = quarter(o)[0]
        arrived(2 * c, m, has_out)
        if o in by_row:
            to_row(o, 2 * c, beams + o, has_out)

    events = [(spread_tile, 0), (spread_tile, ring[0]), (spread_corner, 0), (spread_rim, 0)]
    for now, later in zip(ring, ring[1:] + [None]):
        if later is not None:
            events.append((spread_tile, later))
        events.append((spread_corner, now))
        events.append((spread_rim, now))
    for event, o in events:
        event(o)
    for o in range(beams):
        m, rim, _, _, alive = quarter(o)
        arrived(2 - 2 * c, m)
        arrived(2 - 2 * c, rim, alive)
        arrived(2 * c, rim, alive & has_out)
    for copy in sums:
        copy.wait_send()
    for alive, copy in waits:
        if alive is None:
            copy.wait_send()
        else:
            pl.when(alive)(copy.wait_send)
    tall = blocks * h

    def blank(tiles, start, size):
        for k in tiles:
            t_ref[0, k, pl.ds(start, size), :] = jnp.ones((size, LANES), jnp.float32)
            t_ref[1, k, pl.ds(start, size), :] = jnp.zeros((size, LANES), jnp.float32)

    pl.when(i == 0)(lambda: blank(range(3), 0, half))
    pl.when(i == rows_n - 1)(lambda: blank(range(3), tall - half, half))
    pl.when((z == 0) & (c == 0))(lambda: blank((0,), 0, tall))
    pl.when((z == deep_n - 1) & (c == 1))(lambda: blank((2,), 0, tall))


def transmission(phase_volume, absorb_volume):
    deep, rows, lanes = phase_volume.shape
    beams = lax.axis_size("beam")
    h = rows // beams
    return pl.pallas_call(
        spread_kernel,
        out_shape=[
            jax.ShapeDtypeStruct((2, 3, 2 * rows, lanes), jnp.float32),
            jax.ShapeDtypeStruct((2, h, lanes), jnp.float32),
        ],
        in_specs=[pl.BlockSpec(memory_space=pltpu.HBM)] * 2,
        out_specs=[pl.BlockSpec(memory_space=pltpu.VMEM)] * 2,
        scratch_shapes=[
            pltpu.VMEM((beams, 2, deep, h, lanes), jnp.bfloat16),
            pltpu.VMEM((beams, 2, h, lanes), jnp.float32),
            pltpu.VMEM((beams, 2, h, lanes), jnp.float32),
            pltpu.SemaphoreType.DMA((beams, 2)),
            pltpu.SemaphoreType.DMA((beams,)),
            pltpu.SemaphoreType.DMA((beams,)),
            pltpu.SemaphoreType.DMA((beams,)),
            pltpu.SemaphoreType.DMA((2 * beams,)),
            pltpu.SemaphoreType.DMA((2 * beams,)),
            pltpu.SemaphoreType.DMA((2 * beams,)),
            pltpu.SemaphoreType.DMA((3, 2 * beams)),
        ],
        compiler_params=pltpu.CompilerParams(
            collective_id=0, has_side_effects=True, vmem_limit_bytes=VMEM_LIMIT
        ),
        name="spread",
    )(
        pltpu.with_memory_space_constraint(phase_volume, pltpu.HBM),
        pltpu.with_memory_space_constraint(absorb_volume, pltpu.HBM),
    )


def fold_kernel(
    scale, canvas_ref, own_ref, probe_ref, misfit_ref,
    grad, probe_out, sums_ref,
    sib_in, out_in, acc, corner_in, corner, row_in, q_in, p_in, p_sum, y_in, x_in, z_in, n_xy, n_zc,
    sib_send, sib_recv, out_send, out_recv, corner_send, corner_recv, row_send, row_recv,
    pair_send, pair_recv, group_send, group_recv,
):
    beams, rows_n, deep_n, cores = sizes()
    b, i, z, c = places()
    rows = grad.shape[1]
    h = rows // beams
    half = rows // 2
    tall = 2 * rows
    plane = beams * rows_n
    across = deep_n * cores
    out_z = z - 1 + 2 * c
    me_xy = b * rows_n + i
    me_zc = z * cores + c
    has_out = (out_z >= 0) & (out_z < deep_n)
    above, below = i > 0, i < rows_n - 1
    finish = []

    def go(copy, check=None):
        if check is None:
            copy.start()
        else:
            pl.when(check)(copy.start)
        finish.append((check, copy))
        return copy

    def peer_xy(o):
        return dict(beam=lax.rem(b + o // rows_n, beams), row=lax.rem(i + o % rows_n, rows_n))

    def peer_zc(o):
        return dict(col_0=lax.rem(z + o // cores, deep_n), col_1=lax.rem(c + o % cores, cores))

    def group(g, copies, like):
        for src, dst, where in copies:
            remote(src, dst, group_send.at[g], group_recv.at[g], **where).start()
        everything = remote(like, like, group_send.at[g], group_recv.at[g], col_1=1 - c)
        finish.append((None, everything))
        return everything

    barrier = pltpu.get_barrier_semaphore()
    for o in range(1, plane):
        greet(barrier, **peer_xy(o))
    for o in range(1, across):
        greet(barrier, **peer_zc(o))
    pl.semaphore_wait(barrier, plane + across - 2)

    middle = pl.ds(half, rows)
    rims = [(pl.ds(0, half), above, i - 1), (pl.ds(tall - half, half), below, i + 1)]
    outer = dict(col_0=out_z, col_1=1 - c)
    half_copy = go(remote(probe_ref.at[1 - c], p_in, pair_send.at[0], pair_recv.at[0], col_1=1 - c))
    far_rims, near_rims, corners = [], [], []
    for e, (where, alive, goal) in enumerate(rims):
        near_rims.append(
            go(
                remote(
                    canvas_ref.at[:, 2 - 2 * c, where, :], sib_in.at[:, where, :],
                    sib_send.at[e], sib_recv.at[e], col_1=1 - c,
                ),
                alive,
            )
        )
        far_rims.append(
            go(
                remote(
                    canvas_ref.at[0, 2 * c, where, :], out_in.at[0, where, :],
                    out_send.at[e], out_recv.at[e], **outer,
                ),
                has_out & alive,
            )
        )
        corners.append(
            go(
                remote(
                    canvas_ref.at[1, 2 * c, where, :], corner_in.at[e],
                    corner_send.at[e], corner_recv.at[e], row=goal,
                ),
                has_out & alive,
            )
        )
    far_first = go(
        remote(
            canvas_ref.at[0, 2 * c, middle, :], out_in.at[0, middle, :],
            out_send.at[2], out_recv.at[2], **outer,
        ),
        has_out,
    )
    near_middle = go(
        remote(
            canvas_ref.at[:, 2 - 2 * c, middle, :], sib_in.at[:, middle, :],
            sib_send.at[2], sib_recv.at[2], col_1=1 - c,
        )
    )
    half_copy.wait_recv()
    p_sum[...] = (probe_ref[c] + p_in[...]).reshape(p_sum.shape)
    parts = group(
        0,
        [
            (p_sum.at[:, lax.rem(b + o, beams)], y_in.at[o], dict(beam=lax.rem(b + o, beams)))
            for o in range(1, beams)
        ],
        y_in.at[pl.ds(1, beams - 1)],
    )

    edges = {}
    for p in (1, 0):
        for e, (where, alive, goal) in enumerate(rims):

            def rim(p=p, e=e, where=where):
                if p == 1:
                    near_rims[e].wait_recv()
                acc[p, where, :] = canvas_ref[p, 1, where, :] + sib_in[p, where, :]
                if p == 0:

                    @pl.when(has_out)
                    def _():
                        far_rims[e].wait_recv()
                        acc[0, where, :] += out_in[0, where, :]

            pl.when(alive)(rim)
            edges[p, e] = go(
                remote(
                    acc.at[p, where, :], row_in.at[p, e],
                    row_send.at[p, e], row_recv.at[p, e], row=goal,
                ),
                alive,
            )
    low, high = pl.ds(half, half), pl.ds(rows, half)

    @pl.when(has_out)
    def _():
        corner[...] = canvas_ref[1, 2 * c, middle, :]

        @pl.when(below)
        def _():
            corners[0].wait_recv()
            corner[pl.ds(half, half), :] += corner_in[0]

        @pl.when(above)
        def _():
            corners[1].wait_recv()
            corner[pl.ds(0, half), :] += corner_in[1]

    far_second = go(
        remote(
            corner, out_in.at[1, middle, :], out_send.at[3], out_recv.at[3], **outer
        ),
        has_out,
    )
    near_middle.wait_recv()
    acc[:, middle, :] = canvas_ref[:, 1, middle, :] + sib_in[:, middle, :]
    parts.wait_recv()
    block = p_sum[:, b]
    for o in range(1, beams):
        block = block + y_in[o]
    y_in[0] = block
    parts = group(
        1,
        [
            (y_in.at[0, lax.rem(i + o, rows_n)], x_in.at[o], dict(row=lax.rem(i + o, rows_n)))
            for o in range(1, rows_n)
        ],
        x_in.at[pl.ds(1, rows_n - 1)],
    )

    @pl.when(has_out)
    def _():
        far_first.wait_recv()
        acc[0, middle, :] += out_in[0, middle, :]

    for p in (1, 0):
        for e, (alive, where) in enumerate(((below, high), (above, low))):

            def settle(p=p, e=e, where=where):
                edges[p, e].wait_recv()
                acc[p, where, :] += row_in[p, e]

            pl.when(alive)(settle)

    @pl.when(has_out)
    def _():
        far_second.wait_recv()
        acc[1, middle, :] += out_in[1, middle, :]

    quarters = group(
        2,
        [
            (
                acc.at[:, pl.ds(pl.multiple_of(half + lax.rem(b + o, beams) * h, h), h), :],
                q_in.at[o],
                dict(beam=lax.rem(b + o, beams)),
            )
            for o in [*range(2, beams), 1]
        ],
        q_in.at[pl.ds(1, beams - 1)],
    )
    parts.wait_recv()
    total = y_in[0, i]
    for o in range(1, rows_n):
        total = total + x_in[o]
    z_in[z] = total
    levels = group(
        3,
        [
            (z_in.at[z], z_in.at[z], dict(col_0=lax.rem(z + o, deep_n)))
            for o in sorted(range(1, deep_n), key=lambda o: -min(o, deep_n - o))
        ],
        z_in.at[pl.ds(0, deep_n - 1)],
    )

    mine = pl.ds(pl.multiple_of(half + b * h, h), h)
    quarters.wait_recv()
    cr, ci = acc[0, mine, :], acc[1, mine, :]
    for o in range(1, beams):
        cr = cr + q_in[o, 0]
        ci = ci + q_in[o, 1]
    tr, ti = own_ref[0], own_ref[1]
    phase = tr * ci - ti * cr
    absorb = -(tr * cr + ti * ci)
    home = pl.ds(pl.multiple_of(b * h, h), h)
    grad[0, home, :] = phase
    grad[1, home, :] = absorb
    squares = jnp.sum(phase * phase + absorb * absorb, axis=0, keepdims=True)
    misfits = jnp.sum(misfit_ref[...], axis=0, keepdims=True)
    left = lax.broadcasted_iota(jnp.int32, (1, LANES), 1) < LANES // 2
    n_xy[me_xy] = jnp.where(
        left,
        squares + pltpu.roll(squares, LANES // 2, 1),
        misfits + pltpu.roll(misfits, LANES // 2, 1),
    )
    norms = group(
        4,
        [(n_xy.at[me_xy], n_xy.at[me_xy], peer_xy(o)) for o in range(1, plane)],
        n_xy.at[pl.ds(0, plane - 1)],
    )

    levels.wait_recv()
    total = z_in[0]
    for k in range(1, deep_n):
        total = total + z_in[k]
    probe_out[c, i, b] = total * scale
    spreads = group(
        5,
        [
            (probe_out.at[c, i, b], probe_out.at[c, i, b], dict(beam=lax.rem(b + o, beams)))
            for o in range(1, beams)
        ],
        z_in.at[pl.ds(0, beams - 1)] if beams <= deep_n else y_in.at[0, pl.ds(0, beams - 1)],
    )
    grads = group(
        6,
        [
            (grad.at[:, home, :], grad.at[:, home, :], dict(beam=lax.rem(b + o, beams)))
            for o in range(1, beams)
        ],
        q_in.at[pl.ds(1, beams - 1)],
    )

    norms.wait_recv()
    pair = n_xy[0]
    for k in range(1, plane):
        pair = pair + n_xy[k]
    n_zc[me_zc] = pair
    norms = group(
        7,
        [
            (n_zc.at[me_zc], n_zc.at[me_zc], peer_zc(o))
            for o in sorted(range(1, across), key=lambda o: -min(o // cores, deep_n - o // cores))
        ],
        n_zc.at[pl.ds(0, across - 1)],
    )
    spreads.wait_recv()
    spreads = group(
        8,
        [
            (probe_out.at[c, i], probe_out.at[c, i], dict(row=lax.rem(i + o, rows_n)))
            for o in range(1, rows_n)
        ],
        y_in.at[pl.ds(0, rows_n - 1)] if rows_n == beams else probe_out.at[0, pl.ds(0, rows_n - 1)],
    )
    spreads.wait_recv()
    last = go(
        remote(probe_out.at[c], probe_out.at[c], pair_send.at[1], pair_recv.at[1], col_1=1 - c)
    )
    norms.wait_recv()
    pair = n_zc[0]
    for k in range(1, across):
        pair = pair + n_zc[k]
    sums_ref[...] = pair
    grads.wait_recv()
    last.wait_recv()
    for check, copy in finish:
        if check is None:
            copy.wait_send()
        else:
            pl.when(check)(copy.wait_send)


def folded(canvas, own, probe_sum, misfit, positions):
    beams, rows_n, deep_n, cores = sizes()
    _, _, tall, lanes = canvas.shape
    rows = tall // 2
    h = rows // beams
    n = probe_sum.shape[1]
    plane, across = beams * rows_n, deep_n * cores
    share = n // plane
    f32 = functools.partial(pltpu.VMEM, dtype=jnp.float32)
    sems = [(3,), (3,), (4,), (4,), (2,), (2,), (2, 2), (2, 2), (2,), (2,), (9,), (9,)]
    grad, probe_total, sums = pl.pallas_call(
        functools.partial(fold_kernel, 1.0 / positions),
        out_shape=[
            jax.ShapeDtypeStruct((2, rows, lanes), jnp.float32),
            jax.ShapeDtypeStruct((2, rows_n, beams, share, n), jnp.float32),
            jax.ShapeDtypeStruct((1, LANES), jnp.float32),
        ],
        in_specs=[pl.BlockSpec(memory_space=pltpu.VMEM)] * 4,
        out_specs=[pl.BlockSpec(memory_space=pltpu.VMEM)] * 3,
        scratch_shapes=[
            f32((2, tall, lanes)),
            f32((2, tall, lanes)),
            f32((2, tall, lanes)),
            f32((2, rows // 2, lanes)),
            f32((rows, lanes)),
            f32((2, 2, rows // 2, lanes)),
            f32((beams, 2, h, lanes)),
            f32((n, n)),
            f32((rows_n, beams, share, n)),
            f32((beams, rows_n, share, n)),
            f32((rows_n, share, n)),
            f32((deep_n, share, n)),
            f32((plane, 1, LANES)),
            f32((across, 1, LANES)),
            *[pltpu.SemaphoreType.DMA(count) for count in sems],
        ],
        compiler_params=pltpu.CompilerParams(
            collective_id=1, has_side_effects=True, vmem_limit_bytes=VMEM_LIMIT
        ),
        name="fold",
    )(canvas, own, probe_sum, misfit)
    return grad, probe_total.reshape(probe_sum.shape), sums


def finish_kernel(entries, terms, grad_ref, probe_ref, sums_ref, step_ref, probe_out, loss_ref):
    sums = sums_ref[...]
    left = lax.broadcasted_iota(jnp.int32, sums.shape, 1) < LANES // 2
    square = jnp.sum(jnp.where(left, sums, 0.0), axis=1, keepdims=True)
    factor = jnp.minimum(1.0, 0.5 / jnp.sqrt(square / entries + 1e-06))
    for p in range(2):
        step_ref[p] = grad_ref[p] * factor
    probe_out[...] = probe_ref[...]
    loss_ref[...] = jnp.sum(jnp.where(left, 0.0, sums), axis=1, keepdims=True) / terms


def finished(grad, probe_total, sums, entries, terms):
    vmem = pl.BlockSpec(memory_space=pltpu.VMEM)
    return pl.pallas_call(
        functools.partial(finish_kernel, entries, terms),
        out_shape=[
            jax.ShapeDtypeStruct(grad.shape, jnp.float32),
            jax.ShapeDtypeStruct(probe_total.shape, jnp.float32),
            jax.ShapeDtypeStruct((1, 1), jnp.float32),
        ],
        in_specs=[vmem] * 3,
        out_specs=[vmem] * 3,
        compiler_params=pltpu.CompilerParams(vmem_limit_bytes=VMEM_LIMIT),
        name="finish",
    )(grad, probe_total, sums)


def local(phase_volume, absorb_volume, probe, amplitudes, scan_rows, scan_cols):
    length = probe.shape[1]
    count = scan_rows.shape[2]
    beams, rows_n, deep_n, cores = sizes()
    t, own = transmission(phase_volume, absorb_volume)
    canvas, probe_term, misfit = window_terms(
        t,
        probe,
        amplitudes.reshape(count, length, length),
        scan_rows.reshape(count),
        scan_cols.reshape(count),
    )
    positions = beams * rows_n * deep_n * cores * count
    grad, probe_total, sums = folded(canvas, own, probe_term, misfit, positions)
    entries = grad.size * rows_n * deep_n * cores
    step, probe_total, loss = finished(
        grad, probe_total, sums, entries, positions * length * length
    )
    return (step, probe_total, loss[0, 0])


def solution(mesh):
    split = Mesh(
        mesh.devices.reshape(mesh.shape["beam"], mesh.shape["row"], -1, 2),
        ("beam", "row", "col_0", "col_1"),
    )
    in_specs = (
        P("beam", "row", COL),
        P("beam", "row", COL),
        P(),
        P("row", COL, "beam", None, None),
        P("row", COL, "beam"),
        P("row", COL, "beam"),
    )
    out_specs = (P(None, "row", COL), P(), P())
    return jax.shard_map(local, mesh=split, in_specs=in_specs, out_specs=out_specs, check_vma=False)
```

```python
import functools
import math

import jax
import jax.numpy as jnp
import numpy as np
from jax import lax
from jax.experimental import pallas as pl
from jax.experimental.pallas import tpu as pltpu
from jax.sharding import Mesh
from jax.sharding import PartitionSpec as P

COL = ("col_0", "col_1")
MESH = pl.DeviceIdType.MESH
LANES = 128
CHUNK = 128
BATCH = 4
VMEM_LIMIT = 20 << 20


def dft_tables(length):
    indices = np.arange(length, dtype=np.int32)
    product = indices[:, None] * indices[None, :] % length
    angles = product.astype(np.float32) * np.float32(2.0 * math.pi / length)
    factor = np.float32(1.0 / math.sqrt(length))
    return (
        jnp.asarray(np.cos(angles) * factor).astype(jnp.bfloat16),
        jnp.asarray(-np.sin(angles) * factor).astype(jnp.bfloat16),
    )


def window_kernel(
    rows_ref, cols_ref, t_ref, probe_ref, amp_ref, table_ref,
    canvas_ref, probe_sum_ref, misfit_ref,
    fwd, bwd, cut, psi, half, chi, back,
):
    step = pl.program_id(0)
    n = probe_ref.shape[1]
    batch = amp_ref.shape[0]

    @pl.when(step == 0)
    def _():
        real, imag = table_ref[0], table_ref[1]
        minus = -imag
        fwd[:n, :n] = real
        fwd[:n, n:] = minus
        fwd[n:, :n] = imag
        fwd[n:, n:] = real
        bwd[:n, :n] = real
        bwd[:n, n:] = imag
        bwd[n:, :n] = minus
        bwd[n:, n:] = real
        canvas_ref[...] = jnp.zeros_like(canvas_ref)
        probe_sum_ref[...] = jnp.zeros_like(probe_sum_ref)
        misfit_ref[...] = jnp.zeros_like(misfit_ref)

    lane = lax.broadcasted_iota(jnp.int32, (32, LANES), 1)

    def cut_windows(j):
        row, col = rows_ref[step * batch + j], cols_ref[step * batch + j]
        turn = lax.rem(LANES - col, LANES)
        near = lane < LANES - col
        for at in range(0, n, 32):
            here = pl.ds(at, 32)
            pieces = []
            for part in range(2):
                turned = [
                    pltpu.roll(t_ref[part, k, pl.ds(row + at, 32), :], turn, 1)
                    for k in range(3)
                ]
                pieces.append([jnp.where(near, turned[k], turned[k + 1]) for k in range(2)])
            for k in range(2):
                lanes = pl.ds(k * LANES, LANES)
                tr, ti = pieces[0][k], pieces[1][k]
                cut[j, 0, here, lanes] = tr
                cut[j, 1, here, lanes] = ti
                pr = probe_ref[0, here, lanes]
                pi = probe_ref[1, here, lanes]
                psi[j, here, lanes] = (pr * tr - pi * ti).astype(jnp.bfloat16)
                psi[j, pl.ds(n + at, 32), lanes] = (pr * ti + pi * tr).astype(jnp.bfloat16)

    def to_half(j):
        for part in range(2):
            half[j, :, part * n : (part + 1) * n] = jnp.dot(
                fwd[part * n : (part + 1) * n, :], psi[j], preferred_element_type=jnp.float32
            ).astype(jnp.bfloat16)

    def to_far(j):
        total = jnp.zeros((8, LANES), jnp.float32)
        for at in range(0, n, CHUNK):
            here = pl.ds(at, CHUNK)
            far = jnp.dot(half[j, here, :], bwd[...], preferred_element_type=jnp.float32)
            fr, fi = far[:, :n], far[:, n:]
            amp = amp_ref[j, here, :].astype(jnp.float32)
            power = fr * fr + fi * fi
            inverse = lax.rsqrt(power)
            modulus = jnp.where(power > 0.0, power * inverse, 0.0)
            off = modulus - amp
            square = off * off
            total = total + jnp.sum(
                (square[:, :LANES] + square[:, LANES:]).reshape(CHUNK // 8, 8, LANES), axis=0
            )
            ratio = 1.0 - amp * jnp.minimum(inverse, 2.0)
            chi[j, here, :] = (fr * ratio).astype(jnp.bfloat16)
            chi[j, pl.ds(n + at, CHUNK), :] = (fi * ratio).astype(jnp.bfloat16)
        misfit_ref[...] += total

    def to_back(j):
        for part in range(2):
            back[j, :, part * n : (part + 1) * n] = jnp.dot(
                bwd[part * n : (part + 1) * n, :], chi[j], preferred_element_type=jnp.float32
            ).astype(jnp.bfloat16)

    def add_terms(j):
        row, col = rows_ref[step * batch + j], cols_ref[step * batch + j]
        far_side = lax.broadcasted_iota(jnp.int32, (CHUNK, LANES), 1) >= col
        for at in range(0, n, CHUNK):
            here = pl.ds(at, CHUNK)
            grad = jnp.dot(back[j, here, :], fwd[...], preferred_element_type=jnp.float32)
            gr, gi = grad[:, :n], grad[:, n:]
            tr, ti = cut[j, 0, here, :], cut[j, 1, here, :]
            probe_sum_ref[0, here, :] += tr * gr + ti * gi
            probe_sum_ref[1, here, :] += tr * gi - ti * gr
            pr, pi = probe_ref[0, here, :], probe_ref[1, here, :]
            for part, value in enumerate((pr * gr + pi * gi, pr * gi - pi * gr)):
                first = pltpu.roll(value[:, :LANES], col, 1)
                second = pltpu.roll(value[:, LANES:], col, 1)
                there = pl.ds(row + at, CHUNK)
                canvas_ref[part, 0, there, :] += jnp.where(far_side, first, 0.0)
                canvas_ref[part, 1, there, :] += jnp.where(far_side, second, first)
                canvas_ref[part, 2, there, :] += jnp.where(far_side, 0.0, second)

    steps = (cut_windows, to_half, to_far, to_back, add_terms)
    for tick in range(batch + len(steps) - 1):
        for at, stage in reversed(list(enumerate(steps))):
            if 0 <= tick - at < batch:
                stage(tick - at)


def window_terms(t, probe, amplitudes, rows, cols):
    count, n, _ = amplitudes.shape
    batch = max(size for size in (1, 2, BATCH) if count % size == 0)
    grid_spec = pltpu.PrefetchScalarGridSpec(
        num_scalar_prefetch=2,
        grid=(count // batch,),
        in_specs=[
            pl.BlockSpec(t.shape, lambda s, *_: (0, 0, 0, 0)),
            pl.BlockSpec(probe.shape, lambda s, *_: (0, 0, 0)),
            pl.BlockSpec((batch, n, n), lambda s, *_: (s, 0, 0)),
            pl.BlockSpec((2, n, n), lambda s, *_: (0, 0, 0)),
        ],
        out_specs=[
            pl.BlockSpec(t.shape, lambda s, *_: (0, 0, 0, 0)),
            pl.BlockSpec(probe.shape, lambda s, *_: (0, 0, 0)),
            pl.BlockSpec((8, LANES), lambda s, *_: (0, 0)),
        ],
        scratch_shapes=[
            pltpu.VMEM((2 * n, 2 * n), jnp.bfloat16),
            pltpu.VMEM((2 * n, 2 * n), jnp.bfloat16),
            pltpu.VMEM((batch, 2, n, n), jnp.float32),
            pltpu.VMEM((batch, 2 * n, n), jnp.bfloat16),
            pltpu.VMEM((batch, n, 2 * n), jnp.bfloat16),
            pltpu.VMEM((batch, 2 * n, n), jnp.bfloat16),
            pltpu.VMEM((batch, n, 2 * n), jnp.bfloat16),
        ],
    )
    return pl.pallas_call(
        window_kernel,
        grid_spec=grid_spec,
        out_shape=[
            jax.ShapeDtypeStruct(t.shape, jnp.float32),
            jax.ShapeDtypeStruct(probe.shape, jnp.float32),
            jax.ShapeDtypeStruct((8, LANES), jnp.float32),
        ],
        compiler_params=pltpu.CompilerParams(
            dimension_semantics=("arbitrary",), vmem_limit_bytes=VMEM_LIMIT
        ),
        name="windows",
    )(rows, cols, t, probe, amplitudes, jnp.stack(dft_tables(n)))


def places():
    return tuple(lax.axis_index(axis) for axis in ("beam", "row", "col_0", "col_1"))


def sizes():
    return tuple(lax.axis_size(axis) for axis in ("beam", "row", "col_0", "col_1"))


def remote(src, dst, send_sem, recv_sem, **where):
    return pltpu.make_async_remote_copy(
        src_ref=src,
        dst_ref=dst,
        send_sem=send_sem,
        recv_sem=recv_sem,
        device_id=where,
        device_id_type=MESH,
    )


def greet(barrier, **where):
    pl.semaphore_signal(barrier, inc=1, device_id=where, device_id_type=MESH)


def spread_kernel(
    phase_ref, absorb_ref, t_ref, own_ref,
    vol, part, inbox,
    vol_sem, sum_send, sum_recv, beam_send, near_send, out_send, row_send, t_recv,
):
    beams, rows_n, deep_n, _ = sizes()
    b, i, z, c = places()
    h = phase_ref.shape[1] // beams
    top = beams // 2
    blocks = 2 * beams
    half = top * h
    out_z = z - 1 + 2 * c
    has_out = (out_z >= 0) & (out_z < deep_n)
    above, below = i > 0, i < rows_n - 1
    order = [*range(1, beams), 0]
    loads = {}
    for o in order:
        q = lax.rem(b + o, beams)
        for p, ref in enumerate((phase_ref, absorb_ref)):
            loads[o, p] = pltpu.make_async_copy(
                ref.at[:, pl.ds(pl.multiple_of(q * h, h), h), :], vol.at[o, p], vol_sem.at[o, p]
            )
            loads[o, p].start()

    barrier = pltpu.get_barrier_semaphore()
    for o in range(1, beams):
        greet(barrier, beam=lax.rem(b + o, beams))
    greet(barrier, col_1=1 - c)

    @pl.when(has_out)
    def _():
        greet(barrier, col_0=out_z, col_1=1 - c)

    for alive, row in ((above, i - 1), (below, i + 1)):

        @pl.when(alive)
        def _(row=row):
            greet(barrier, row=row)

        @pl.when(alive & has_out)
        def _(row=row):
            greet(barrier, row=row, col_0=out_z, col_1=1 - c)

    for o in order:
        for p in range(2):
            loads[o, p].wait()
            total = vol[o, p, 0].astype(jnp.float32)
            for d in range(1, phase_ref.shape[0]):
                total = total + vol[o, p, d].astype(jnp.float32)
            part[o, p] = total
    ups, downs, outs = (flag.astype(jnp.int32) for flag in (above, below, has_out))
    pl.semaphore_wait(barrier, beams + outs + (1 + outs) * (ups + downs))
    sums = []
    for o in order[:-1]:
        copy = remote(
            part.at[o], inbox.at[o], sum_send.at[o], sum_recv.at[o], beam=lax.rem(b + o, beams)
        )
        copy.start()
        sums.append(copy)
    for copy in sums:
        copy.wait_recv()
    phase, absorb = part[0, 0], part[0, 1]
    for o in range(1, beams):
        phase = phase + inbox[o, 0]
        absorb = absorb + inbox[o, 1]
    damping = jnp.exp(-absorb)
    tr, ti = damping * jnp.cos(phase), damping * jnp.sin(phase)
    own_ref[0] = tr
    own_ref[1] = ti

    def cell(k, m):
        return t_ref.at[:, k, pl.ds(pl.multiple_of(m * h, h), h), :]

    mine = pl.ds(pl.multiple_of(half + b * h, h), h)
    t_ref[0, 1, mine, :] = tr
    t_ref[1, 1, mine, :] = ti
    m0 = top + b
    waits = []

    def send(copy, check=None):
        if check is None:
            copy.start()
        else:
            pl.when(check)(copy.start)
        waits.append((check, copy))

    def arrived(k, m, check=None):
        wait = remote(cell(1, m), cell(k, m), near_send.at[0], t_recv.at[k, m], col_1=1 - c).wait_recv
        if check is None:
            wait()
        else:
            pl.when(check)(wait)

    def both(first, second):
        return second if first is None else first & second

    def to_sibling(m, slot, check=None):
        send(
            remote(
                cell(1, m), cell(2 * c, m), near_send.at[slot], t_recv.at[2 * c, m], col_1=1 - c
            ),
            check,
        )

    def to_outer(m, slot, check=None):
        send(
            remote(
                cell(1, m), cell(2 - 2 * c, m), out_send.at[slot], t_recv.at[2 - 2 * c, m],
                col_0=out_z, col_1=1 - c,
            ),
            both(check, has_out),
        )

    def quarter(o):
        q = lax.rem(b + o, beams)
        upper = q // top
        rim = q - top + (1 - upper) * blocks
        goal, source = i - 1 + 2 * upper, i + 1 - 2 * upper
        return top + q, rim, goal, (goal >= 0) & (goal < rows_n), (source >= 0) & (source < rows_n)

    def to_row(o, k, slot, check=None):
        m, rim, goal, alive, _ = quarter(o)
        send(
            remote(cell(k, m), cell(k, rim), row_send.at[slot], t_recv.at[k, rim], row=goal),
            both(check, alive),
        )

    ring = [1, *range(3, beams), *range(2, min(3, beams))]
    by_row, direct = {0}, {2}
    for o in ring:
        send(
            remote(
                cell(1, m0), cell(1, m0), beam_send.at[o], t_recv.at[1, m0],
                beam=lax.rem(b + o, beams),
            )
        )

    def to_diagonal(o, slot):
        m, rim, goal, alive, _ = quarter(o)
        send(
            remote(
                cell(1, m), cell(2 - 2 * c, rim), out_send.at[slot], t_recv.at[2 - 2 * c, rim],
                row=goal, col_0=out_z, col_1=1 - c,
            ),
            alive & has_out,
        )

    def spread_tile(o):
        m = quarter(o)[0]
        if o:
            arrived(1, m)
        to_outer(m, o)
        to_row(o, 1, o)
        if o in direct:
            to_diagonal(o, beams + o)
        to_sibling(m, o)

    def spread_rim(o):
        _, rim, _, _, alive = quarter(o)
        arrived(1, rim, alive)
        if o not in by_row and o not in direct:
            to_outer(rim, beams + o, alive)
        to_sibling(rim, beams + o, alive)

    def spread_corner(o):
        m = quarter(o)[0]
        arrived(2 * c, m, has_out)
        if o in by_row:
            to_row(o, 2 * c, beams + o, has_out)

    events = [(spread_tile, 0), (spread_tile, ring[0]), (spread_corner, 0), (spread_rim, 0)]
    events += [(spread_tile, o) for o in ring[1:]]
    for o in ring:
        events += [(spread_corner, o), (spread_rim, o)]
    for event, o in events:
        event(o)
    for o in range(beams):
        m, rim, _, _, alive = quarter(o)
        arrived(2 - 2 * c, m)
        arrived(2 - 2 * c, rim, alive)
        arrived(2 * c, rim, alive & has_out)
    for copy in sums:
        copy.wait_send()
    for alive, copy in waits:
        if alive is None:
            copy.wait_send()
        else:
            pl.when(alive)(copy.wait_send)
    tall = blocks * h

    def blank(tiles, start, size):
        for k in tiles:
            t_ref[0, k, pl.ds(start, size), :] = jnp.ones((size, LANES), jnp.float32)
            t_ref[1, k, pl.ds(start, size), :] = jnp.zeros((size, LANES), jnp.float32)

    pl.when(i == 0)(lambda: blank(range(3), 0, half))
    pl.when(i == rows_n - 1)(lambda: blank(range(3), tall - half, half))
    pl.when((z == 0) & (c == 0))(lambda: blank((0,), 0, tall))
    pl.when((z == deep_n - 1) & (c == 1))(lambda: blank((2,), 0, tall))


def transmission(phase_volume, absorb_volume):
    deep, rows, lanes = phase_volume.shape
    beams = lax.axis_size("beam")
    h = rows // beams
    return pl.pallas_call(
        spread_kernel,
        out_shape=[
            jax.ShapeDtypeStruct((2, 3, 2 * rows, lanes), jnp.float32),
            jax.ShapeDtypeStruct((2, h, lanes), jnp.float32),
        ],
        in_specs=[pl.BlockSpec(memory_space=pltpu.HBM)] * 2,
        out_specs=[pl.BlockSpec(memory_space=pltpu.VMEM)] * 2,
        scratch_shapes=[
            pltpu.VMEM((beams, 2, deep, h, lanes), jnp.bfloat16),
            pltpu.VMEM((beams, 2, h, lanes), jnp.float32),
            pltpu.VMEM((beams, 2, h, lanes), jnp.float32),
            pltpu.SemaphoreType.DMA((beams, 2)),
            pltpu.SemaphoreType.DMA((beams,)),
            pltpu.SemaphoreType.DMA((beams,)),
            pltpu.SemaphoreType.DMA((beams,)),
            pltpu.SemaphoreType.DMA((2 * beams,)),
            pltpu.SemaphoreType.DMA((2 * beams,)),
            pltpu.SemaphoreType.DMA((2 * beams,)),
            pltpu.SemaphoreType.DMA((3, 2 * beams)),
        ],
        compiler_params=pltpu.CompilerParams(
            collective_id=0, has_side_effects=True, vmem_limit_bytes=VMEM_LIMIT
        ),
        name="spread",
    )(
        pltpu.with_memory_space_constraint(phase_volume, pltpu.HBM),
        pltpu.with_memory_space_constraint(absorb_volume, pltpu.HBM),
    )


def fold_kernel(
    scale, canvas_ref, own_ref, probe_ref, misfit_ref,
    grad, probe_out, sums_ref,
    sib_in, out_in, acc, corner_in, corner, row_in, q_in, p_in, p_sum, x_in, z_in, n_xy, n_zc,
    sib_send, sib_recv, out_send, out_recv, corner_send, corner_recv, row_send, row_recv,
    pair_send, pair_recv, group_send, group_recv,
):
    beams, rows_n, deep_n, cores = sizes()
    b, i, z, c = places()
    rows = grad.shape[1]
    h = rows // beams
    half = rows // 2
    tall = 2 * rows
    plane = beams * rows_n
    across = deep_n * cores
    out_z = z - 1 + 2 * c
    me_xy = b * rows_n + i
    me_zc = z * cores + c
    has_out = (out_z >= 0) & (out_z < deep_n)
    above, below = i > 0, i < rows_n - 1
    finish = []

    def go(copy, check=None):
        if check is None:
            copy.start()
        else:
            pl.when(check)(copy.start)
        finish.append((check, copy))
        return copy

    def peer_xy(o):
        return dict(beam=lax.rem(b + o // rows_n, beams), row=lax.rem(i + o % rows_n, rows_n))

    def peer_zc(o):
        return dict(col_0=lax.rem(z + o // cores, deep_n), col_1=lax.rem(c + o % cores, cores))

    def group(g, copies, like):
        for src, dst, where in copies:
            remote(src, dst, group_send.at[g], group_recv.at[g], **where).start()
        everything = remote(like, like, group_send.at[g], group_recv.at[g], col_1=1 - c)
        finish.append((None, everything))
        return everything

    barrier = pltpu.get_barrier_semaphore()
    for o in range(1, plane):
        greet(barrier, **peer_xy(o))
    for o in range(1, across):
        greet(barrier, **peer_zc(o))
    pl.semaphore_wait(barrier, plane + across - 2)

    middle = pl.ds(half, rows)
    rims = [(pl.ds(0, half), above, i - 1), (pl.ds(tall - half, half), below, i + 1)]
    outer = dict(col_0=out_z, col_1=1 - c)
    half_copy = go(remote(probe_ref.at[1 - c], p_in, pair_send.at[0], pair_recv.at[0], col_1=1 - c))
    far_rims, near_rims, corners = [], [], []
    for e, (where, alive, goal) in enumerate(rims):
        near_rims.append(
            go(
                remote(
                    canvas_ref.at[:, 2 - 2 * c, where, :], sib_in.at[:, where, :],
                    sib_send.at[e], sib_recv.at[e], col_1=1 - c,
                ),
                alive,
            )
        )
        far_rims.append(
            go(
                remote(
                    canvas_ref.at[0, 2 * c, where, :], out_in.at[0, where, :],
                    out_send.at[e], out_recv.at[e], **outer,
                ),
                has_out & alive,
            )
        )
        corners.append(
            go(
                remote(
                    canvas_ref.at[1, 2 * c, where, :], corner_in.at[e],
                    corner_send.at[e], corner_recv.at[e], row=goal,
                ),
                has_out & alive,
            )
        )
    far_first = go(
        remote(
            canvas_ref.at[0, 2 * c, middle, :], out_in.at[0, middle, :],
            out_send.at[2], out_recv.at[2], **outer,
        ),
        has_out,
    )
    near_middle = go(
        remote(
            canvas_ref.at[:, 2 - 2 * c, middle, :], sib_in.at[:, middle, :],
            sib_send.at[2], sib_recv.at[2], col_1=1 - c,
        )
    )
    half_copy.wait_recv()
    p_sum[...] = (probe_ref[c] + p_in[...]).reshape(p_sum.shape)

    edges = {}
    for p in (1, 0):
        for e, (where, alive, goal) in enumerate(rims):

            def rim(p=p, e=e, where=where):
                if p == 1:
                    near_rims[e].wait_recv()
                acc[p, where, :] = canvas_ref[p, 1, where, :] + sib_in[p, where, :]
                if p == 0:

                    @pl.when(has_out)
                    def _():
                        far_rims[e].wait_recv()
                        acc[0, where, :] += out_in[0, where, :]

            pl.when(alive)(rim)
            edges[p, e] = go(
                remote(
                    acc.at[p, where, :], row_in.at[p, e],
                    row_send.at[p, e], row_recv.at[p, e], row=goal,
                ),
                alive,
            )
    low, high = pl.ds(half, half), pl.ds(rows, half)

    def at_xy(o):
        peer = peer_xy(o)
        return peer["beam"] * rows_n + peer["row"]

    parts = group(
        0,
        [(p_sum.at[at_xy(o)], x_in.at[o], peer_xy(o)) for o in range(1, plane)],
        x_in.at[pl.ds(1, plane - 1)],
    )

    @pl.when(has_out)
    def _():
        corner[...] = canvas_ref[1, 2 * c, middle, :]

        @pl.when(below)
        def _():
            corners[0].wait_recv()
            corner[pl.ds(half, half), :] += corner_in[0]

        @pl.when(above)
        def _():
            corners[1].wait_recv()
            corner[pl.ds(0, half), :] += corner_in[1]

    far_second = go(
        remote(
            corner, out_in.at[1, middle, :], out_send.at[3], out_recv.at[3], **outer
        ),
        has_out,
    )
    near_middle.wait_recv()
    acc[:, middle, :] = canvas_ref[:, 1, middle, :] + sib_in[:, middle, :]
    @pl.when(has_out)
    def _():
        far_first.wait_recv()
        acc[0, middle, :] += out_in[0, middle, :]

    for p in (1, 0):
        for e, (alive, where) in enumerate(((below, high), (above, low))):

            def settle(p=p, e=e, where=where):
                edges[p, e].wait_recv()
                acc[p, where, :] += row_in[p, e]

            pl.when(alive)(settle)

    @pl.when(has_out)
    def _():
        far_second.wait_recv()
        acc[1, middle, :] += out_in[1, middle, :]

    quarters = group(
        2,
        [
            (
                acc.at[:, pl.ds(pl.multiple_of(half + lax.rem(b + o, beams) * h, h), h), :],
                q_in.at[o],
                dict(beam=lax.rem(b + o, beams)),
            )
            for o in [*range(2, beams), 1]
        ],
        q_in.at[pl.ds(1, beams - 1)],
    )
    parts.wait_recv()
    total = p_sum[me_xy]
    for o in range(1, plane):
        total = total + x_in[o]
    z_in[z] = total
    levels = group(
        3,
        [
            (z_in.at[z], z_in.at[z], dict(col_0=lax.rem(z + o, deep_n)))
            for o in sorted(range(1, deep_n), key=lambda o: -min(o, deep_n - o))
        ],
        z_in.at[pl.ds(0, deep_n - 1)],
    )

    mine = pl.ds(pl.multiple_of(half + b * h, h), h)
    quarters.wait_recv()
    cr, ci = acc[0, mine, :], acc[1, mine, :]
    for o in range(1, beams):
        cr = cr + q_in[o, 0]
        ci = ci + q_in[o, 1]
    tr, ti = own_ref[0], own_ref[1]
    phase = tr * ci - ti * cr
    absorb = -(tr * cr + ti * ci)
    home = pl.ds(pl.multiple_of(b * h, h), h)
    grad[0, home, :] = phase
    grad[1, home, :] = absorb
    squares = jnp.sum(phase * phase + absorb * absorb, axis=0, keepdims=True)
    misfits = jnp.sum(misfit_ref[...], axis=0, keepdims=True)
    left = lax.broadcasted_iota(jnp.int32, (1, LANES), 1) < LANES // 2
    n_xy[me_xy] = jnp.where(
        left,
        squares + pltpu.roll(squares, LANES // 2, 1),
        misfits + pltpu.roll(misfits, LANES // 2, 1),
    )
    norms = group(
        4,
        [(n_xy.at[me_xy], n_xy.at[me_xy], peer_xy(o)) for o in range(1, plane)],
        n_xy.at[pl.ds(0, plane - 1)],
    )

    levels.wait_recv()
    total = z_in[0]
    for k in range(1, deep_n):
        total = total + z_in[k]
    probe_out[c, me_xy] = total * scale
    spreads = group(
        5,
        [(probe_out.at[c, me_xy], probe_out.at[c, me_xy], peer_xy(o)) for o in range(1, plane)],
        x_in.at[pl.ds(1, plane - 1)],
    )
    grads = group(
        6,
        [
            (grad.at[:, home, :], grad.at[:, home, :], dict(beam=lax.rem(b + o, beams)))
            for o in range(1, beams)
        ],
        q_in.at[pl.ds(1, beams - 1)],
    )

    norms.wait_recv()
    pair = n_xy[0]
    for k in range(1, plane):
        pair = pair + n_xy[k]
    n_zc[me_zc] = pair
    norms = group(
        7,
        [
            (n_zc.at[me_zc], n_zc.at[me_zc], peer_zc(o))
            for o in sorted(range(1, across), key=lambda o: -min(o // cores, deep_n - o // cores))
        ],
        n_zc.at[pl.ds(0, across - 1)],
    )
    spreads.wait_recv()
    last = go(
        remote(probe_out.at[c], probe_out.at[c], pair_send.at[1], pair_recv.at[1], col_1=1 - c)
    )
    norms.wait_recv()
    pair = n_zc[0]
    for k in range(1, across):
        pair = pair + n_zc[k]
    sums_ref[...] = pair
    grads.wait_recv()
    last.wait_recv()
    for check, copy in finish:
        if check is None:
            copy.wait_send()
        else:
            pl.when(check)(copy.wait_send)


def folded(canvas, own, probe_sum, misfit, positions):
    beams, rows_n, deep_n, cores = sizes()
    _, _, tall, lanes = canvas.shape
    rows = tall // 2
    h = rows // beams
    n = probe_sum.shape[1]
    plane, across = beams * rows_n, deep_n * cores
    share = n // plane
    f32 = functools.partial(pltpu.VMEM, dtype=jnp.float32)
    sems = [(3,), (3,), (4,), (4,), (2,), (2,), (2, 2), (2, 2), (2,), (2,), (9,), (9,)]
    grad, probe_total, sums = pl.pallas_call(
        functools.partial(fold_kernel, 1.0 / positions),
        out_shape=[
            jax.ShapeDtypeStruct((2, rows, lanes), jnp.float32),
            jax.ShapeDtypeStruct((2, plane, share, n), jnp.float32),
            jax.ShapeDtypeStruct((1, LANES), jnp.float32),
        ],
        in_specs=[pl.BlockSpec(memory_space=pltpu.VMEM)] * 4,
        out_specs=[pl.BlockSpec(memory_space=pltpu.VMEM)] * 3,
        scratch_shapes=[
            f32((2, tall, lanes)),
            f32((2, tall, lanes)),
            f32((2, tall, lanes)),
            f32((2, rows // 2, lanes)),
            f32((rows, lanes)),
            f32((2, 2, rows // 2, lanes)),
            f32((beams, 2, h, lanes)),
            f32((n, n)),
            f32((plane, share, n)),
            f32((plane, share, n)),
            f32((deep_n, share, n)),
            f32((plane, 1, LANES)),
            f32((across, 1, LANES)),
            *[pltpu.SemaphoreType.DMA(count) for count in sems],
        ],
        compiler_params=pltpu.CompilerParams(
            collective_id=1, has_side_effects=True, vmem_limit_bytes=VMEM_LIMIT
        ),
        name="fold",
    )(canvas, own, probe_sum, misfit)
    return grad, probe_total.reshape(probe_sum.shape), sums


def finish_kernel(entries, terms, grad_ref, probe_ref, sums_ref, step_ref, probe_out, loss_ref):
    sums = sums_ref[...]
    left = lax.broadcasted_iota(jnp.int32, sums.shape, 1) < LANES // 2
    square = jnp.sum(jnp.where(left, sums, 0.0), axis=1, keepdims=True)
    factor = jnp.minimum(1.0, 0.5 / jnp.sqrt(square / entries + 1e-06))
    for p in range(2):
        step_ref[p] = grad_ref[p] * factor
    probe_out[...] = probe_ref[...]
    loss_ref[...] = jnp.sum(jnp.where(left, 0.0, sums), axis=1, keepdims=True) / terms


def finished(grad, probe_total, sums, entries, terms):
    vmem = pl.BlockSpec(memory_space=pltpu.VMEM)
    return pl.pallas_call(
        functools.partial(finish_kernel, entries, terms),
        out_shape=[
            jax.ShapeDtypeStruct(grad.shape, jnp.float32),
            jax.ShapeDtypeStruct(probe_total.shape, jnp.float32),
            jax.ShapeDtypeStruct((1, 1), jnp.float32),
        ],
        in_specs=[vmem] * 3,
        out_specs=[vmem] * 3,
        compiler_params=pltpu.CompilerParams(vmem_limit_bytes=VMEM_LIMIT),
        name="finish",
    )(grad, probe_total, sums)


def local(phase_volume, absorb_volume, probe, amplitudes, scan_rows, scan_cols):
    length = probe.shape[1]
    count = scan_rows.shape[2]
    beams, rows_n, deep_n, cores = sizes()
    t, own = transmission(phase_volume, absorb_volume)
    canvas, probe_term, misfit = window_terms(
        t,
        probe,
        amplitudes.reshape(count, length, length),
        scan_rows.reshape(count),
        scan_cols.reshape(count),
    )
    positions = beams * rows_n * deep_n * cores * count
    grad, probe_total, sums = folded(canvas, own, probe_term, misfit, positions)
    entries = grad.size * rows_n * deep_n * cores
    step, probe_total, loss = finished(
        grad, probe_total, sums, entries, positions * length * length
    )
    return (step, probe_total, loss[0, 0])


def solution(mesh):
    split = Mesh(
        mesh.devices.reshape(mesh.shape["beam"], mesh.shape["row"], -1, 2),
        ("beam", "row", "col_0", "col_1"),
    )
    in_specs = (
        P("beam", "row", COL),
        P("beam", "row", COL),
        P(),
        P("row", COL, "beam", None, None),
        P("row", COL, "beam"),
        P("row", COL, "beam"),
    )
    out_specs = (P(None, "row", COL), P(), P())
    return jax.shard_map(local, mesh=split, in_specs=in_specs, out_specs=out_specs, check_vma=False)
```

```python
import functools
import math

import jax
import jax.numpy as jnp
import numpy as np
from jax import lax
from jax.experimental import pallas as pl
from jax.experimental.pallas import tpu as pltpu
from jax.sharding import Mesh
from jax.sharding import PartitionSpec as P

COL = ("col_0", "col_1")
MESH = pl.DeviceIdType.MESH
LANES = 128
CHUNK = 128
BATCH = 4
SUBS = 2
VMEM_LIMIT = 20 << 20


def dft_tables(length):
    indices = np.arange(length, dtype=np.int32)
    product = indices[:, None] * indices[None, :] % length
    angles = product.astype(np.float32) * np.float32(2.0 * math.pi / length)
    factor = np.float32(1.0 / math.sqrt(length))
    return (
        jnp.asarray(np.cos(angles) * factor).astype(jnp.bfloat16),
        jnp.asarray(-np.sin(angles) * factor).astype(jnp.bfloat16),
    )


def window_kernel(
    rows_ref, cols_ref, t_ref, probe_ref, amp_ref, table_ref,
    canvas_ref, probe_sum_ref, misfit_ref,
    fwd, bwd, cut, psi, half, chi, back,
):
    step = pl.program_id(0)
    n = probe_ref.shape[1]
    batch = amp_ref.shape[0]

    @pl.when(step == 0)
    def _():
        real, imag = table_ref[0], table_ref[1]
        minus = -imag
        fwd[:n, :n] = real
        fwd[:n, n:] = minus
        fwd[n:, :n] = imag
        fwd[n:, n:] = real
        bwd[:n, :n] = real
        bwd[:n, n:] = imag
        bwd[n:, :n] = minus
        bwd[n:, n:] = real
        canvas_ref[...] = jnp.zeros_like(canvas_ref)
        probe_sum_ref[...] = jnp.zeros_like(probe_sum_ref)
        misfit_ref[...] = jnp.zeros_like(misfit_ref)

    lane = lax.broadcasted_iota(jnp.int32, (32, LANES), 1)

    def cut_windows(j):
        row, col = rows_ref[step * batch + j], cols_ref[step * batch + j]
        turn = lax.rem(LANES - col, LANES)
        near = lane < LANES - col
        for at in range(0, n, 32):
            here = pl.ds(at, 32)
            pieces = []
            for part in range(2):
                turned = [
                    pltpu.roll(t_ref[part, k, pl.ds(row + at, 32), :], turn, 1)
                    for k in range(3)
                ]
                pieces.append([jnp.where(near, turned[k], turned[k + 1]) for k in range(2)])
            for k in range(2):
                lanes = pl.ds(k * LANES, LANES)
                tr, ti = pieces[0][k], pieces[1][k]
                cut[j, 0, here, lanes] = tr
                cut[j, 1, here, lanes] = ti
                pr = probe_ref[0, here, lanes]
                pi = probe_ref[1, here, lanes]
                psi[j, here, lanes] = (pr * tr - pi * ti).astype(jnp.bfloat16)
                psi[j, pl.ds(n + at, 32), lanes] = (pr * ti + pi * tr).astype(jnp.bfloat16)

    def to_half(j):
        for part in range(2):
            half[j, :, part * n : (part + 1) * n] = jnp.dot(
                fwd[part * n : (part + 1) * n, :], psi[j], preferred_element_type=jnp.float32
            ).astype(jnp.bfloat16)

    def to_far(j):
        total = jnp.zeros((8, LANES), jnp.float32)
        for at in range(0, n, CHUNK):
            here = pl.ds(at, CHUNK)
            far = jnp.dot(half[j, here, :], bwd[...], preferred_element_type=jnp.float32)
            fr, fi = far[:, :n], far[:, n:]
            amp = amp_ref[j, here, :].astype(jnp.float32)
            power = fr * fr + fi * fi
            inverse = lax.rsqrt(power)
            modulus = jnp.where(power > 0.0, power * inverse, 0.0)
            off = modulus - amp
            square = off * off
            total = total + jnp.sum(
                (square[:, :LANES] + square[:, LANES:]).reshape(CHUNK // 8, 8, LANES), axis=0
            )
            ratio = 1.0 - amp * jnp.minimum(inverse, 2.0)
            chi[j, here, :] = (fr * ratio).astype(jnp.bfloat16)
            chi[j, pl.ds(n + at, CHUNK), :] = (fi * ratio).astype(jnp.bfloat16)
        misfit_ref[...] += total

    def to_back(j):
        for part in range(2):
            back[j, :, part * n : (part + 1) * n] = jnp.dot(
                bwd[part * n : (part + 1) * n, :], chi[j], preferred_element_type=jnp.float32
            ).astype(jnp.bfloat16)

    def add_terms(j):
        row, col = rows_ref[step * batch + j], cols_ref[step * batch + j]
        far_side = lax.broadcasted_iota(jnp.int32, (CHUNK, LANES), 1) >= col
        for at in range(0, n, CHUNK):
            here = pl.ds(at, CHUNK)
            grad = jnp.dot(back[j, here, :], fwd[...], preferred_element_type=jnp.float32)
            gr, gi = grad[:, :n], grad[:, n:]
            tr, ti = cut[j, 0, here, :], cut[j, 1, here, :]
            probe_sum_ref[0, here, :] += tr * gr + ti * gi
            probe_sum_ref[1, here, :] += tr * gi - ti * gr
            pr, pi = probe_ref[0, here, :], probe_ref[1, here, :]
            for part, value in enumerate((pr * gr + pi * gi, pr * gi - pi * gr)):
                first = pltpu.roll(value[:, :LANES], col, 1)
                second = pltpu.roll(value[:, LANES:], col, 1)
                there = pl.ds(row + at, CHUNK)
                canvas_ref[part, 0, there, :] += jnp.where(far_side, first, 0.0)
                canvas_ref[part, 1, there, :] += jnp.where(far_side, second, first)
                canvas_ref[part, 2, there, :] += jnp.where(far_side, 0.0, second)

    steps = (cut_windows, to_half, to_far, to_back, add_terms)
    for tick in range(batch + len(steps) - 1):
        for at, stage in enumerate(steps):
            if 0 <= tick - at < batch:
                stage(tick - at)


def window_terms(t, probe, amplitudes, rows, cols):
    count, n, _ = amplitudes.shape
    batch = max(size for size in (1, 2, BATCH) if count % size == 0)
    grid_spec = pltpu.PrefetchScalarGridSpec(
        num_scalar_prefetch=2,
        grid=(count // batch,),
        in_specs=[
            pl.BlockSpec(t.shape, lambda s, *_: (0, 0, 0, 0)),
            pl.BlockSpec(probe.shape, lambda s, *_: (0, 0, 0)),
            pl.BlockSpec((batch, n, n), lambda s, *_: (s, 0, 0)),
            pl.BlockSpec((2, n, n), lambda s, *_: (0, 0, 0)),
        ],
        out_specs=[
            pl.BlockSpec(t.shape, lambda s, *_: (0, 0, 0, 0)),
            pl.BlockSpec(probe.shape, lambda s, *_: (0, 0, 0)),
            pl.BlockSpec((8, LANES), lambda s, *_: (0, 0)),
        ],
        scratch_shapes=[
            pltpu.VMEM((2 * n, 2 * n), jnp.bfloat16),
            pltpu.VMEM((2 * n, 2 * n), jnp.bfloat16),
            pltpu.VMEM((batch, 2, n, n), jnp.float32),
            pltpu.VMEM((batch, 2 * n, n), jnp.bfloat16),
            pltpu.VMEM((batch, n, 2 * n), jnp.bfloat16),
            pltpu.VMEM((batch, 2 * n, n), jnp.bfloat16),
            pltpu.VMEM((batch, n, 2 * n), jnp.bfloat16),
        ],
    )
    return pl.pallas_call(
        window_kernel,
        grid_spec=grid_spec,
        out_shape=[
            jax.ShapeDtypeStruct(t.shape, jnp.float32),
            jax.ShapeDtypeStruct(probe.shape, jnp.float32),
            jax.ShapeDtypeStruct((8, LANES), jnp.float32),
        ],
        compiler_params=pltpu.CompilerParams(
            dimension_semantics=("arbitrary",), vmem_limit_bytes=VMEM_LIMIT
        ),
        name="windows",
    )(rows, cols, t, probe, amplitudes, jnp.stack(dft_tables(n)))


def places():
    return tuple(lax.axis_index(axis) for axis in ("beam", "row", "col_0", "col_1"))


def sizes():
    return tuple(lax.axis_size(axis) for axis in ("beam", "row", "col_0", "col_1"))


def remote(src, dst, send_sem, recv_sem, **where):
    return pltpu.make_async_remote_copy(
        src_ref=src,
        dst_ref=dst,
        send_sem=send_sem,
        recv_sem=recv_sem,
        device_id=where,
        device_id_type=MESH,
    )


def greet(barrier, **where):
    pl.semaphore_signal(barrier, inc=1, device_id=where, device_id_type=MESH)


def spread_kernel(
    phase_ref, absorb_ref, t_ref, own_ref,
    vol, part, inbox,
    vol_sem, sum_send, sum_recv, beam_send, near_send, rim_send, out_send, row_send, corner_send,
    t_recv,
):
    beams, rows_n, deep_n, _ = sizes()
    b, i, z, c = places()
    subs, h = part.shape[1], part.shape[3]
    quarter_rows = subs * h
    top = beams // 2
    half = top * quarter_rows
    blocks = 2 * beams * subs
    out_z = z - 1 + 2 * c
    has_out = (out_z >= 0) & (out_z < deep_n)
    above, below = i > 0, i < rows_n - 1
    outer = dict(col_0=out_z, col_1=1 - c)
    order = [*range(1, beams), 0]
    loads = {}
    for o in order:
        q = lax.rem(b + o, beams)
        rows_here = pl.ds(pl.multiple_of(q * quarter_rows, quarter_rows), quarter_rows)
        for p, ref in enumerate((phase_ref, absorb_ref)):
            loads[o, p] = pltpu.make_async_copy(
                ref.at[:, rows_here, :], vol.at[o, p], vol_sem.at[o, p]
            )
            loads[o, p].start()

    barrier = pltpu.get_barrier_semaphore()
    for o in range(1, beams):
        greet(barrier, beam=lax.rem(b + o, beams))
    greet(barrier, col_1=1 - c)

    @pl.when(has_out)
    def _():
        greet(barrier, **outer)

    for alive, row in ((above, i - 1), (below, i + 1)):

        @pl.when(alive)
        def _(row=row):
            greet(barrier, row=row)

        @pl.when(alive & has_out)
        def _(row=row):
            greet(barrier, row=row, **outer)

    for o in order:
        for p in range(2):
            loads[o, p].wait()
            total = vol[o, p, 0].astype(jnp.float32)
            for d in range(1, phase_ref.shape[0]):
                total = total + vol[o, p, d].astype(jnp.float32)
            for s in range(subs):
                part[o, s, p] = total[s * h : (s + 1) * h]
    ups, downs, outs = (flag.astype(jnp.int32) for flag in (above, below, has_out))
    pl.semaphore_wait(barrier, beams + outs + (1 + outs) * (ups + downs))
    for s in range(subs):
        for o in order[:-1]:
            remote(
                part.at[o, s], inbox.at[s, o], sum_send.at[s], sum_recv.at[s],
                beam=lax.rem(b + o, beams),
            ).start()

    def cell(k, m):
        return t_ref.at[:, k, pl.ds(pl.multiple_of(m * h, h), h), :]

    def arrived(k, m, check=None):
        wait = remote(cell(1, m), cell(k, m), near_send, t_recv.at[k, m], col_1=1 - c).wait_recv
        if check is None:
            wait()
        else:
            pl.when(check)(wait)

    def spot(o, s):
        q = lax.rem(b + o, beams)
        upper = q // top
        rim = q * subs + s - top * subs + (1 - upper) * blocks
        goal, source = i - 1 + 2 * upper, i + 1 - 2 * upper
        return (
            top * subs + q * subs + s, rim, upper, goal,
            (goal >= 0) & (goal < rows_n), (source >= 0) & (source < rows_n),
        )

    ring = [1, *range(3, beams), *range(2, min(3, beams))]
    by_row, direct = {0}, {2}
    singles = []

    def single(check, slot, src, k, m, **where):
        copy = remote(src, cell(k, m), corner_send.at[slot], t_recv.at[k, m], **where)
        pl.when(check)(copy.start)
        singles.append((check, copy))

    def tile(o, s):
        m, rim, upper, goal, alive, _ = spot(o, s)
        if o:
            arrived(1, m)
        far = remote(
            cell(1, m), cell(2 - 2 * c, m), out_send, t_recv.at[2 - 2 * c, m], **outer
        )
        pl.when(has_out)(far.start)
        side = remote(cell(1, m), cell(1, rim), row_send.at[upper], t_recv.at[1, rim], row=goal)
        pl.when(alive)(side.start)
        if o in direct:
            single(
                alive & has_out, o * subs + s, cell(1, m), 2 - 2 * c, rim, row=goal, **outer
            )
        remote(cell(1, m), cell(2 * c, m), near_send, t_recv.at[2 * c, m], col_1=1 - c).start()

    def corner(o, s):
        m, rim, _, goal, alive, _ = spot(o, s)
        arrived(2 * c, m, has_out)
        if o in by_row:
            single(alive & has_out, o * subs + s, cell(2 * c, m), 2 * c, rim, row=goal)

    def edge(o, s):
        _, rim, upper, _, _, alive = spot(o, s)
        arrived(1, rim, alive)
        if o not in by_row and o not in direct:
            single(alive & has_out, o * subs + s, cell(1, rim), 2 - 2 * c, rim, **outer)
        copy = remote(
            cell(1, rim), cell(2 * c, rim), rim_send.at[upper], t_recv.at[2 * c, rim], col_1=1 - c
        )
        pl.when(alive)(copy.start)

    def total_of(like, send, recv):
        return remote(like, like, send, recv, col_1=1 - c)

    for s in range(subs):
        sums = total_of(inbox.at[s, pl.ds(1, beams - 1)], sum_send.at[s], sum_recv.at[s])
        sums.wait_recv()
        phase, absorb = part[0, s, 0], part[0, s, 1]
        for o in range(1, beams):
            phase = phase + inbox[s, o, 0]
            absorb = absorb + inbox[s, o, 1]
        damping = jnp.exp(-absorb)
        mine = pl.ds(pl.multiple_of(half + (b * subs + s) * h, h), h)
        for p, value in enumerate((damping * jnp.cos(phase), damping * jnp.sin(phase))):
            t_ref[p, 1, mine, :] = value
            own_ref[p, pl.ds(s * h, h), :] = value
        m = top * subs + b * subs + s
        for o in ring:
            remote(
                cell(1, m), cell(1, m), beam_send, t_recv.at[1, m], beam=lax.rem(b + o, beams)
            ).start()
        tile(0, s)
    events = []
    for s in range(subs):
        events += [(corner, 0, s), *[(tile, o, s) for o in ring if o not in direct], (edge, 0, s)]
        events += [(tile, o, s) for o in ring if o in direct]
    events += [(edge, o, s) for s in range(subs) for o in ring]
    for event, o, s in events:
        event(o, s)
    for s in range(subs):
        for o in range(beams):
            m, rim, _, _, _, alive = spot(o, s)
            if o:
                corner(o, s)
            arrived(2 - 2 * c, m)
            arrived(2 - 2 * c, rim, alive)
            arrived(2 * c, rim, alive & has_out)
    for s in range(subs):
        total_of(part.at[pl.ds(1, beams - 1), s], sum_send.at[s], sum_recv.at[s]).wait_send()
    total_of(part.at[pl.ds(1, beams - 1)], beam_send, beam_send).wait_send()
    total_of(part, near_send, near_send).wait_send()
    pl.when(has_out)(total_of(part, out_send, out_send).wait_send)
    for upper, (goal_here, source_here) in enumerate(((above, below), (below, above))):
        like = part.at[pl.ds(0, top)]
        pl.when(goal_here)(total_of(like, row_send.at[upper], row_send.at[upper]).wait_send)
        pl.when(source_here)(total_of(like, rim_send.at[upper], rim_send.at[upper]).wait_send)
    for check, copy in singles:
        pl.when(check)(copy.wait_send)
    tall = blocks * h

    def blank(tiles, start, size):
        for k in tiles:
            t_ref[0, k, pl.ds(start, size), :] = jnp.ones((size, LANES), jnp.float32)
            t_ref[1, k, pl.ds(start, size), :] = jnp.zeros((size, LANES), jnp.float32)

    pl.when(i == 0)(lambda: blank(range(3), 0, half))
    pl.when(i == rows_n - 1)(lambda: blank(range(3), tall - half, half))
    pl.when((z == 0) & (c == 0))(lambda: blank((0,), 0, tall))
    pl.when((z == deep_n - 1) & (c == 1))(lambda: blank((2,), 0, tall))


def transmission(phase_volume, absorb_volume):
    deep, rows, lanes = phase_volume.shape
    beams = lax.axis_size("beam")
    h = rows // (beams * SUBS)
    dma = pltpu.SemaphoreType.DMA
    return pl.pallas_call(
        spread_kernel,
        out_shape=[
            jax.ShapeDtypeStruct((2, 3, 2 * rows, lanes), jnp.float32),
            jax.ShapeDtypeStruct((2, SUBS * h, lanes), jnp.float32),
        ],
        in_specs=[pl.BlockSpec(memory_space=pltpu.HBM)] * 2,
        out_specs=[pl.BlockSpec(memory_space=pltpu.VMEM)] * 2,
        scratch_shapes=[
            pltpu.VMEM((beams, 2, deep, SUBS * h, lanes), jnp.bfloat16),
            pltpu.VMEM((beams, SUBS, 2, h, lanes), jnp.float32),
            pltpu.VMEM((SUBS, beams, 2, h, lanes), jnp.float32),
            dma((beams, 2)),
            dma((SUBS,)),
            dma((SUBS,)),
            dma,
            dma,
            dma((2,)),
            dma,
            dma((2,)),
            dma((beams * SUBS,)),
            dma((3, 2 * beams * SUBS)),
        ],
        compiler_params=pltpu.CompilerParams(
            collective_id=0, has_side_effects=True, vmem_limit_bytes=VMEM_LIMIT
        ),
        name="spread",
    )(
        pltpu.with_memory_space_constraint(phase_volume, pltpu.HBM),
        pltpu.with_memory_space_constraint(absorb_volume, pltpu.HBM),
    )


def fold_kernel(
    scale, canvas_ref, own_ref, probe_ref, misfit_ref,
    grad, probe_out, sums_ref,
    sib_in, out_in, acc, corner_in, corner, row_in, q_in, p_in, p_sum, x_in, z_in, n_xy, n_zc,
    sib_send, sib_recv, out_send, out_recv, corner_send, corner_recv, row_send, row_recv,
    pair_send, pair_recv, group_send, group_recv,
):
    beams, rows_n, deep_n, cores = sizes()
    b, i, z, c = places()
    rows = grad.shape[1]
    h = rows // beams
    half = rows // 2
    tall = 2 * rows
    plane = beams * rows_n
    across = deep_n * cores
    out_z = z - 1 + 2 * c
    me_xy = b * rows_n + i
    me_zc = z * cores + c
    has_out = (out_z >= 0) & (out_z < deep_n)
    above, below = i > 0, i < rows_n - 1
    finish = []

    def go(copy, check=None):
        if check is None:
            copy.start()
        else:
            pl.when(check)(copy.start)
        finish.append((check, copy))
        return copy

    def peer_xy(o):
        return dict(beam=lax.rem(b + o // rows_n, beams), row=lax.rem(i + o % rows_n, rows_n))

    def peer_zc(o):
        return dict(col_0=lax.rem(z + o // cores, deep_n), col_1=lax.rem(c + o % cores, cores))

    def group(g, copies, like):
        for src, dst, where in copies:
            remote(src, dst, group_send.at[g], group_recv.at[g], **where).start()
        everything = remote(like, like, group_send.at[g], group_recv.at[g], col_1=1 - c)
        finish.append((None, everything))
        return everything

    barrier = pltpu.get_barrier_semaphore()
    for o in range(1, plane):
        greet(barrier, **peer_xy(o))
    for o in range(1, across):
        greet(barrier, **peer_zc(o))
    pl.semaphore_wait(barrier, plane + across - 2)

    middle = pl.ds(half, rows)
    rims = [(pl.ds(0, half), above, i - 1), (pl.ds(tall - half, half), below, i + 1)]
    outer = dict(col_0=out_z, col_1=1 - c)
    half_copy = go(remote(probe_ref.at[1 - c], p_in, pair_send.at[0], pair_recv.at[0], col_1=1 - c))
    far_rims, near_rims, corners = [], [], []
    for e, (where, alive, goal) in enumerate(rims):
        near_rims.append(
            go(
                remote(
                    canvas_ref.at[:, 2 - 2 * c, where, :], sib_in.at[:, where, :],
                    sib_send.at[e], sib_recv.at[e], col_1=1 - c,
                ),
                alive,
            )
        )
        far_rims.append(
            go(
                remote(
                    canvas_ref.at[0, 2 * c, where, :], out_in.at[0, where, :],
                    out_send.at[e], out_recv.at[e], **outer,
                ),
                has_out & alive,
            )
        )
        corners.append(
            go(
                remote(
                    canvas_ref.at[1, 2 * c, where, :], corner_in.at[e],
                    corner_send.at[e], corner_recv.at[e], row=goal,
                ),
                has_out & alive,
            )
        )
    far_first = go(
        remote(
            canvas_ref.at[0, 2 * c, middle, :], out_in.at[0, middle, :],
            out_send.at[2], out_recv.at[2], **outer,
        ),
        has_out,
    )
    near_middle = go(
        remote(
            canvas_ref.at[:, 2 - 2 * c, middle, :], sib_in.at[:, middle, :],
            sib_send.at[2], sib_recv.at[2], col_1=1 - c,
        )
    )
    half_copy.wait_recv()
    p_sum[...] = (probe_ref[c] + p_in[...]).reshape(p_sum.shape)

    edges = {}
    for p in (1, 0):
        for e, (where, alive, goal) in enumerate(rims):

            def rim(p=p, e=e, where=where):
                if p == 1:
                    near_rims[e].wait_recv()
                acc[p, where, :] = canvas_ref[p, 1, where, :] + sib_in[p, where, :]
                if p == 0:

                    @pl.when(has_out)
                    def _():
                        far_rims[e].wait_recv()
                        acc[0, where, :] += out_in[0, where, :]

            pl.when(alive)(rim)
            edges[p, e] = go(
                remote(
                    acc.at[p, where, :], row_in.at[p, e],
                    row_send.at[p, e], row_recv.at[p, e], row=goal,
                ),
                alive,
            )
    low, high = pl.ds(half, half), pl.ds(rows, half)

    def at_xy(o):
        peer = peer_xy(o)
        return peer["beam"] * rows_n + peer["row"]

    parts = group(
        0,
        [(p_sum.at[at_xy(o)], x_in.at[o], peer_xy(o)) for o in range(1, plane)],
        x_in.at[pl.ds(1, plane - 1)],
    )

    @pl.when(has_out)
    def _():
        corner[...] = canvas_ref[1, 2 * c, middle, :]

        @pl.when(below)
        def _():
            corners[0].wait_recv()
            corner[pl.ds(half, half), :] += corner_in[0]

        @pl.when(above)
        def _():
            corners[1].wait_recv()
            corner[pl.ds(0, half), :] += corner_in[1]

    far_second = go(
        remote(
            corner, out_in.at[1, middle, :], out_send.at[3], out_recv.at[3], **outer
        ),
        has_out,
    )
    near_middle.wait_recv()
    acc[:, middle, :] = canvas_ref[:, 1, middle, :] + sib_in[:, middle, :]
    @pl.when(has_out)
    def _():
        far_first.wait_recv()
        acc[0, middle, :] += out_in[0, middle, :]

    for p in (1, 0):
        for e, (alive, where) in enumerate(((below, high), (above, low))):

            def settle(p=p, e=e, where=where):
                edges[p, e].wait_recv()
                acc[p, where, :] += row_in[p, e]

            pl.when(alive)(settle)

    @pl.when(has_out)
    def _():
        far_second.wait_recv()
        acc[1, middle, :] += out_in[1, middle, :]

    quarters = group(
        2,
        [
            (
                acc.at[:, pl.ds(pl.multiple_of(half + lax.rem(b + o, beams) * h, h), h), :],
                q_in.at[o],
                dict(beam=lax.rem(b + o, beams)),
            )
            for o in [*range(2, beams), 1]
        ],
        q_in.at[pl.ds(1, beams - 1)],
    )
    parts.wait_recv()
    total = p_sum[me_xy]
    for o in range(1, plane):
        total = total + x_in[o]
    z_in[z] = total
    levels = group(
        3,
        [
            (z_in.at[z], z_in.at[z], dict(col_0=lax.rem(z + o, deep_n)))
            for o in sorted(range(1, deep_n), key=lambda o: -min(o, deep_n - o))
        ],
        z_in.at[pl.ds(0, deep_n - 1)],
    )

    mine = pl.ds(pl.multiple_of(half + b * h, h), h)
    quarters.wait_recv()
    cr, ci = acc[0, mine, :], acc[1, mine, :]
    for o in range(1, beams):
        cr = cr + q_in[o, 0]
        ci = ci + q_in[o, 1]
    tr, ti = own_ref[0], own_ref[1]
    phase = tr * ci - ti * cr
    absorb = -(tr * cr + ti * ci)
    home = pl.ds(pl.multiple_of(b * h, h), h)
    grad[0, home, :] = phase
    grad[1, home, :] = absorb
    squares = jnp.sum(phase * phase + absorb * absorb, axis=0, keepdims=True)
    misfits = jnp.sum(misfit_ref[...], axis=0, keepdims=True)
    left = lax.broadcasted_iota(jnp.int32, (1, LANES), 1) < LANES // 2
    n_xy[me_xy] = jnp.where(
        left,
        squares + pltpu.roll(squares, LANES // 2, 1),
        misfits + pltpu.roll(misfits, LANES // 2, 1),
    )
    norms = group(
        4,
        [(n_xy.at[me_xy], n_xy.at[me_xy], peer_xy(o)) for o in range(1, plane)],
        n_xy.at[pl.ds(0, plane - 1)],
    )

    levels.wait_recv()
    total = z_in[0]
    for k in range(1, deep_n):
        total = total + z_in[k]
    probe_out[c, me_xy] = total * scale
    spreads = group(
        5,
        [(probe_out.at[c, me_xy], probe_out.at[c, me_xy], peer_xy(o)) for o in range(1, plane)],
        x_in.at[pl.ds(1, plane - 1)],
    )
    grads = group(
        6,
        [
            (grad.at[:, home, :], grad.at[:, home, :], dict(beam=lax.rem(b + o, beams)))
            for o in range(1, beams)
        ],
        q_in.at[pl.ds(1, beams - 1)],
    )

    norms.wait_recv()
    pair = n_xy[0]
    for k in range(1, plane):
        pair = pair + n_xy[k]
    n_zc[me_zc] = pair
    norms = group(
        7,
        [
            (n_zc.at[me_zc], n_zc.at[me_zc], peer_zc(o))
            for o in sorted(range(1, across), key=lambda o: -min(o // cores, deep_n - o // cores))
        ],
        n_zc.at[pl.ds(0, across - 1)],
    )
    spreads.wait_recv()
    last = go(
        remote(probe_out.at[c], probe_out.at[c], pair_send.at[1], pair_recv.at[1], col_1=1 - c)
    )
    norms.wait_recv()
    pair = n_zc[0]
    for k in range(1, across):
        pair = pair + n_zc[k]
    sums_ref[...] = pair
    grads.wait_recv()
    last.wait_recv()
    for check, copy in finish:
        if check is None:
            copy.wait_send()
        else:
            pl.when(check)(copy.wait_send)


def folded(canvas, own, probe_sum, misfit, positions):
    beams, rows_n, deep_n, cores = sizes()
    _, _, tall, lanes = canvas.shape
    rows = tall // 2
    h = rows // beams
    n = probe_sum.shape[1]
    plane, across = beams * rows_n, deep_n * cores
    share = n // plane
    f32 = functools.partial(pltpu.VMEM, dtype=jnp.float32)
    sems = [(3,), (3,), (4,), (4,), (2,), (2,), (2, 2), (2, 2), (2,), (2,), (9,), (9,)]
    grad, probe_total, sums = pl.pallas_call(
        functools.partial(fold_kernel, 1.0 / positions),
        out_shape=[
            jax.ShapeDtypeStruct((2, rows, lanes), jnp.float32),
            jax.ShapeDtypeStruct((2, plane, share, n), jnp.float32),
            jax.ShapeDtypeStruct((1, LANES), jnp.float32),
        ],
        in_specs=[pl.BlockSpec(memory_space=pltpu.VMEM)] * 4,
        out_specs=[pl.BlockSpec(memory_space=pltpu.VMEM)] * 3,
        scratch_shapes=[
            f32((2, tall, lanes)),
            f32((2, tall, lanes)),
            f32((2, tall, lanes)),
            f32((2, rows // 2, lanes)),
            f32((rows, lanes)),
            f32((2, 2, rows // 2, lanes)),
            f32((beams, 2, h, lanes)),
            f32((n, n)),
            f32((plane, share, n)),
            f32((plane, share, n)),
            f32((deep_n, share, n)),
            f32((plane, 1, LANES)),
            f32((across, 1, LANES)),
            *[pltpu.SemaphoreType.DMA(count) for count in sems],
        ],
        compiler_params=pltpu.CompilerParams(
            collective_id=1, has_side_effects=True, vmem_limit_bytes=VMEM_LIMIT
        ),
        name="fold",
    )(canvas, own, probe_sum, misfit)
    return grad, probe_total.reshape(probe_sum.shape), sums


def finish_kernel(entries, terms, grad_ref, probe_ref, sums_ref, step_ref, probe_out, loss_ref):
    sums = sums_ref[...]
    left = lax.broadcasted_iota(jnp.int32, sums.shape, 1) < LANES // 2
    square = jnp.sum(jnp.where(left, sums, 0.0), axis=1, keepdims=True)
    factor = jnp.minimum(1.0, 0.5 / jnp.sqrt(square / entries + 1e-06))
    for p in range(2):
        step_ref[p] = grad_ref[p] * factor
    probe_out[...] = probe_ref[...]
    loss_ref[...] = jnp.sum(jnp.where(left, 0.0, sums), axis=1, keepdims=True) / terms


def finished(grad, probe_total, sums, entries, terms):
    vmem = pl.BlockSpec(memory_space=pltpu.VMEM)
    return pl.pallas_call(
        functools.partial(finish_kernel, entries, terms),
        out_shape=[
            jax.ShapeDtypeStruct(grad.shape, jnp.float32),
            jax.ShapeDtypeStruct(probe_total.shape, jnp.float32),
            jax.ShapeDtypeStruct((1, 1), jnp.float32),
        ],
        in_specs=[vmem] * 3,
        out_specs=[vmem] * 3,
        compiler_params=pltpu.CompilerParams(vmem_limit_bytes=VMEM_LIMIT),
        name="finish",
    )(grad, probe_total, sums)


def local(phase_volume, absorb_volume, probe, amplitudes, scan_rows, scan_cols):
    length = probe.shape[1]
    count = scan_rows.shape[2]
    beams, rows_n, deep_n, cores = sizes()
    t, own = transmission(phase_volume, absorb_volume)
    canvas, probe_term, misfit = window_terms(
        t,
        probe,
        amplitudes.reshape(count, length, length),
        scan_rows.reshape(count),
        scan_cols.reshape(count),
    )
    positions = beams * rows_n * deep_n * cores * count
    grad, probe_total, sums = folded(canvas, own, probe_term, misfit, positions)
    entries = grad.size * rows_n * deep_n * cores
    step, probe_total, loss = finished(
        grad, probe_total, sums, entries, positions * length * length
    )
    return (step, probe_total, loss[0, 0])


def solution(mesh):
    split = Mesh(
        mesh.devices.reshape(mesh.shape["beam"], mesh.shape["row"], -1, 2),
        ("beam", "row", "col_0", "col_1"),
    )
    in_specs = (
        P("beam", "row", COL),
        P("beam", "row", COL),
        P(),
        P("row", COL, "beam", None, None),
        P("row", COL, "beam"),
        P("row", COL, "beam"),
    )
    out_specs = (P(None, "row", COL), P(), P())
    return jax.shard_map(local, mesh=split, in_specs=in_specs, out_specs=out_specs, check_vma=False)
```

```python
import functools
import math

import jax
import jax.numpy as jnp
import numpy as np
from jax import lax
from jax.experimental import pallas as pl
from jax.experimental.pallas import tpu as pltpu
from jax.sharding import Mesh
from jax.sharding import PartitionSpec as P

COL = ("col_0", "col_1")
MESH = pl.DeviceIdType.MESH
LANES = 128
CHUNK = 128
BATCH = 4
SUBS = 2
VMEM_LIMIT = 20 << 20


def dft_tables(length):
    indices = np.arange(length, dtype=np.int32)
    product = indices[:, None] * indices[None, :] % length
    angles = product.astype(np.float32) * np.float32(2.0 * math.pi / length)
    factor = np.float32(1.0 / math.sqrt(length))
    return (
        jnp.asarray(np.cos(angles) * factor).astype(jnp.bfloat16),
        jnp.asarray(-np.sin(angles) * factor).astype(jnp.bfloat16),
    )


def window_kernel(
    rows_ref, cols_ref, t_ref, probe_ref, amp_ref, table_ref,
    canvas_ref, probe_sum_ref, misfit_ref,
    fwd, bwd, cut, psi, half, chi, back,
):
    step = pl.program_id(0)
    n = probe_ref.shape[1]
    batch = amp_ref.shape[0]

    @pl.when(step == 0)
    def _():
        real, imag = table_ref[0], table_ref[1]
        minus = -imag
        fwd[:n, :n] = real
        fwd[:n, n:] = minus
        fwd[n:, :n] = imag
        fwd[n:, n:] = real
        bwd[:n, :n] = real
        bwd[:n, n:] = imag
        bwd[n:, :n] = minus
        bwd[n:, n:] = real
        canvas_ref[...] = jnp.zeros_like(canvas_ref)
        probe_sum_ref[...] = jnp.zeros_like(probe_sum_ref)
        misfit_ref[...] = jnp.zeros_like(misfit_ref)

    lane = lax.broadcasted_iota(jnp.int32, (32, LANES), 1)

    def cut_windows(j):
        row, col = rows_ref[step * batch + j], cols_ref[step * batch + j]
        turn = lax.rem(LANES - col, LANES)
        near = lane < LANES - col
        for at in range(0, n, 32):
            here = pl.ds(at, 32)
            pieces = []
            for part in range(2):
                turned = [
                    pltpu.roll(t_ref[part, k, pl.ds(row + at, 32), :], turn, 1)
                    for k in range(3)
                ]
                pieces.append([jnp.where(near, turned[k], turned[k + 1]) for k in range(2)])
            for k in range(2):
                lanes = pl.ds(k * LANES, LANES)
                tr, ti = pieces[0][k], pieces[1][k]
                cut[j, 0, here, lanes] = tr
                cut[j, 1, here, lanes] = ti
                pr = probe_ref[0, here, lanes]
                pi = probe_ref[1, here, lanes]
                psi[j, here, lanes] = (pr * tr - pi * ti).astype(jnp.bfloat16)
                psi[j, pl.ds(n + at, 32), lanes] = (pr * ti + pi * tr).astype(jnp.bfloat16)

    def to_half(j):
        for part in range(2):
            half[j, :, part * n : (part + 1) * n] = jnp.dot(
                fwd[part * n : (part + 1) * n, :], psi[j], preferred_element_type=jnp.float32
            ).astype(jnp.bfloat16)

    def to_far(j):
        total = jnp.zeros((8, LANES), jnp.float32)
        for at in range(0, n, CHUNK):
            here = pl.ds(at, CHUNK)
            far = jnp.dot(half[j, here, :], bwd[...], preferred_element_type=jnp.float32)
            fr, fi = far[:, :n], far[:, n:]
            amp = amp_ref[j, here, :].astype(jnp.float32)
            power = fr * fr + fi * fi
            inverse = lax.rsqrt(power)
            modulus = jnp.where(power > 0.0, power * inverse, 0.0)
            off = modulus - amp
            square = off * off
            total = total + jnp.sum(
                (square[:, :LANES] + square[:, LANES:]).reshape(CHUNK // 8, 8, LANES), axis=0
            )
            ratio = 1.0 - amp * jnp.minimum(inverse, 2.0)
            chi[j, here, :] = (fr * ratio).astype(jnp.bfloat16)
            chi[j, pl.ds(n + at, CHUNK), :] = (fi * ratio).astype(jnp.bfloat16)
        misfit_ref[...] += total

    def to_back(j):
        for part in range(2):
            back[j, :, part * n : (part + 1) * n] = jnp.dot(
                bwd[part * n : (part + 1) * n, :], chi[j], preferred_element_type=jnp.float32
            ).astype(jnp.bfloat16)

    def add_terms(j):
        row, col = rows_ref[step * batch + j], cols_ref[step * batch + j]
        far_side = lax.broadcasted_iota(jnp.int32, (CHUNK, LANES), 1) >= col
        for at in range(0, n, CHUNK):
            here = pl.ds(at, CHUNK)
            grad = jnp.dot(back[j, here, :], fwd[...], preferred_element_type=jnp.float32)
            gr, gi = grad[:, :n], grad[:, n:]
            tr, ti = cut[j, 0, here, :], cut[j, 1, here, :]
            probe_sum_ref[0, here, :] += tr * gr + ti * gi
            probe_sum_ref[1, here, :] += tr * gi - ti * gr
            pr, pi = probe_ref[0, here, :], probe_ref[1, here, :]
            for part, value in enumerate((pr * gr + pi * gi, pr * gi - pi * gr)):
                first = pltpu.roll(value[:, :LANES], col, 1)
                second = pltpu.roll(value[:, LANES:], col, 1)
                there = pl.ds(row + at, CHUNK)
                canvas_ref[part, 0, there, :] += jnp.where(far_side, first, 0.0)
                canvas_ref[part, 1, there, :] += jnp.where(far_side, second, first)
                canvas_ref[part, 2, there, :] += jnp.where(far_side, 0.0, second)

    steps = (cut_windows, to_half, to_far, to_back, add_terms)
    for tick in range(batch + len(steps) - 1):
        for at, stage in enumerate(steps):
            if 0 <= tick - at < batch:
                stage(tick - at)


def window_terms(t, probe, amplitudes, rows, cols):
    count, n, _ = amplitudes.shape
    batch = max(size for size in (1, 2, BATCH) if count % size == 0)
    grid_spec = pltpu.PrefetchScalarGridSpec(
        num_scalar_prefetch=2,
        grid=(count // batch,),
        in_specs=[
            pl.BlockSpec(t.shape, lambda s, *_: (0, 0, 0, 0)),
            pl.BlockSpec(probe.shape, lambda s, *_: (0, 0, 0)),
            pl.BlockSpec((batch, n, n), lambda s, *_: (s, 0, 0)),
            pl.BlockSpec((2, n, n), lambda s, *_: (0, 0, 0)),
        ],
        out_specs=[
            pl.BlockSpec(t.shape, lambda s, *_: (0, 0, 0, 0)),
            pl.BlockSpec(probe.shape, lambda s, *_: (0, 0, 0)),
            pl.BlockSpec((8, LANES), lambda s, *_: (0, 0)),
        ],
        scratch_shapes=[
            pltpu.VMEM((2 * n, 2 * n), jnp.bfloat16),
            pltpu.VMEM((2 * n, 2 * n), jnp.bfloat16),
            pltpu.VMEM((batch, 2, n, n), jnp.float32),
            pltpu.VMEM((batch, 2 * n, n), jnp.bfloat16),
            pltpu.VMEM((batch, n, 2 * n), jnp.bfloat16),
            pltpu.VMEM((batch, 2 * n, n), jnp.bfloat16),
            pltpu.VMEM((batch, n, 2 * n), jnp.bfloat16),
        ],
    )
    return pl.pallas_call(
        window_kernel,
        grid_spec=grid_spec,
        out_shape=[
            jax.ShapeDtypeStruct(t.shape, jnp.float32),
            jax.ShapeDtypeStruct(probe.shape, jnp.float32),
            jax.ShapeDtypeStruct((8, LANES), jnp.float32),
        ],
        compiler_params=pltpu.CompilerParams(
            dimension_semantics=("arbitrary",), vmem_limit_bytes=VMEM_LIMIT
        ),
        name="windows",
    )(rows, cols, t, probe, amplitudes, jnp.stack(dft_tables(n)))


def places():
    return tuple(lax.axis_index(axis) for axis in ("beam", "row", "col_0", "col_1"))


def sizes():
    return tuple(lax.axis_size(axis) for axis in ("beam", "row", "col_0", "col_1"))


def remote(src, dst, send_sem, recv_sem, **where):
    return pltpu.make_async_remote_copy(
        src_ref=src,
        dst_ref=dst,
        send_sem=send_sem,
        recv_sem=recv_sem,
        device_id=where,
        device_id_type=MESH,
    )


def greet(barrier, **where):
    pl.semaphore_signal(barrier, inc=1, device_id=where, device_id_type=MESH)


def spread_kernel(
    phase_ref, absorb_ref, t_ref, own_ref,
    vol, part, inbox,
    vol_sem, sum_send, sum_recv, beam_send, near_send, rim_send, out_send, row_send, corner_send,
    t_recv,
):
    beams, rows_n, deep_n, _ = sizes()
    b, i, z, c = places()
    subs, h = part.shape[1], part.shape[3]
    quarter_rows = subs * h
    top = beams // 2
    half = top * quarter_rows
    blocks = 2 * beams * subs
    out_z = z - 1 + 2 * c
    has_out = (out_z >= 0) & (out_z < deep_n)
    above, below = i > 0, i < rows_n - 1
    outer = dict(col_0=out_z, col_1=1 - c)
    order = [*range(1, beams), 0]
    loads = {}
    for o in order:
        q = lax.rem(b + o, beams)
        rows_here = pl.ds(pl.multiple_of(q * quarter_rows, quarter_rows), quarter_rows)
        for p, ref in enumerate((phase_ref, absorb_ref)):
            loads[o, p] = pltpu.make_async_copy(
                ref.at[:, rows_here, :], vol.at[o, p], vol_sem.at[o, p]
            )
            loads[o, p].start()

    barrier = pltpu.get_barrier_semaphore()
    for o in range(1, beams):
        greet(barrier, beam=lax.rem(b + o, beams))
    greet(barrier, col_1=1 - c)

    @pl.when(has_out)
    def _():
        greet(barrier, **outer)

    for alive, row in ((above, i - 1), (below, i + 1)):

        @pl.when(alive)
        def _(row=row):
            greet(barrier, row=row)

        @pl.when(alive & has_out)
        def _(row=row):
            greet(barrier, row=row, **outer)

    for o in order:
        for p in range(2):
            loads[o, p].wait()
            total = vol[o, p, 0].astype(jnp.float32)
            for d in range(1, phase_ref.shape[0]):
                total = total + vol[o, p, d].astype(jnp.float32)
            for s in range(subs):
                part[o, s, p] = total[s * h : (s + 1) * h]
    ups, downs, outs = (flag.astype(jnp.int32) for flag in (above, below, has_out))
    pl.semaphore_wait(barrier, beams + outs + (1 + outs) * (ups + downs))
    for s in range(subs):
        for o in order[:-1]:
            remote(
                part.at[o, s], inbox.at[s, o], sum_send.at[s], sum_recv.at[s],
                beam=lax.rem(b + o, beams),
            ).start()

    def cell(k, m):
        return t_ref.at[:, k, pl.ds(pl.multiple_of(m * h, h), h), :]

    def arrived(k, m, check=None):
        wait = remote(cell(1, m), cell(k, m), near_send, t_recv.at[k, m], col_1=1 - c).wait_recv
        if check is None:
            wait()
        else:
            pl.when(check)(wait)

    def spot(o, s):
        q = lax.rem(b + o, beams)
        upper = q // top
        rim = q * subs + s - top * subs + (1 - upper) * blocks
        goal, source = i - 1 + 2 * upper, i + 1 - 2 * upper
        return (
            top * subs + q * subs + s, rim, upper, goal,
            (goal >= 0) & (goal < rows_n), (source >= 0) & (source < rows_n),
        )

    ring = [1, *range(3, beams), *range(2, min(3, beams))]
    by_row, direct = {0}, {2}
    singles = []

    def single(check, slot, src, k, m, **where):
        copy = remote(src, cell(k, m), corner_send.at[slot], t_recv.at[k, m], **where)
        pl.when(check)(copy.start)
        singles.append((check, copy))

    def tile(o, s):
        m, rim, upper, goal, alive, _ = spot(o, s)
        if o:
            arrived(1, m)
        far = remote(
            cell(1, m), cell(2 - 2 * c, m), out_send, t_recv.at[2 - 2 * c, m], **outer
        )
        pl.when(has_out)(far.start)
        side = remote(cell(1, m), cell(1, rim), row_send.at[upper], t_recv.at[1, rim], row=goal)
        pl.when(alive)(side.start)
        if o in direct:
            single(
                alive & has_out, o * subs + s, cell(1, m), 2 - 2 * c, rim, row=goal, **outer
            )
        remote(cell(1, m), cell(2 * c, m), near_send, t_recv.at[2 * c, m], col_1=1 - c).start()

    def corner(o, s):
        m, rim, _, goal, alive, _ = spot(o, s)
        arrived(2 * c, m, has_out)
        if o in by_row:
            single(alive & has_out, o * subs + s, cell(2 * c, m), 2 * c, rim, row=goal)

    def edge(o, s):
        _, rim, upper, _, _, alive = spot(o, s)
        arrived(1, rim, alive)
        if o not in by_row and o not in direct:
            single(alive & has_out, o * subs + s, cell(1, rim), 2 - 2 * c, rim, **outer)
        copy = remote(
            cell(1, rim), cell(2 * c, rim), rim_send.at[upper], t_recv.at[2 * c, rim], col_1=1 - c
        )
        pl.when(alive)(copy.start)

    def total_of(like, send, recv):
        return remote(like, like, send, recv, col_1=1 - c)

    for s in range(subs):
        sums = total_of(inbox.at[s, pl.ds(1, beams - 1)], sum_send.at[s], sum_recv.at[s])
        sums.wait_recv()
        phase, absorb = part[0, s, 0], part[0, s, 1]
        for o in range(1, beams):
            phase = phase + inbox[s, o, 0]
            absorb = absorb + inbox[s, o, 1]
        damping = jnp.exp(-absorb)
        mine = pl.ds(pl.multiple_of(half + (b * subs + s) * h, h), h)
        for p, value in enumerate((damping * jnp.cos(phase), damping * jnp.sin(phase))):
            t_ref[p, 1, mine, :] = value
            own_ref[p, pl.ds(s * h, h), :] = value
        m = top * subs + b * subs + s
        for o in ring:
            remote(
                cell(1, m), cell(1, m), beam_send, t_recv.at[1, m], beam=lax.rem(b + o, beams)
            ).start()
        tile(0, s)
    events = []
    for s in range(subs):
        events += [(corner, 0, s), *[(tile, o, s) for o in ring if o not in direct], (edge, 0, s)]
        events += [(tile, o, s) for o in ring if o in direct]
    events += [(edge, o, s) for s in range(subs) for o in ring]
    for event, o, s in events:
        event(o, s)
    for s in range(subs):
        for o in range(beams):
            m, rim, _, _, _, alive = spot(o, s)
            if o:
                corner(o, s)
            arrived(2 - 2 * c, m)
            arrived(2 - 2 * c, rim, alive)
            arrived(2 * c, rim, alive & has_out)
    for s in range(subs):
        total_of(part.at[pl.ds(1, beams - 1), s], sum_send.at[s], sum_recv.at[s]).wait_send()
    total_of(part.at[pl.ds(1, beams - 1)], beam_send, beam_send).wait_send()
    total_of(part, near_send, near_send).wait_send()
    pl.when(has_out)(total_of(part, out_send, out_send).wait_send)
    for upper, (goal_here, source_here) in enumerate(((above, below), (below, above))):
        like = part.at[pl.ds(0, top)]
        pl.when(goal_here)(total_of(like, row_send.at[upper], row_send.at[upper]).wait_send)
        pl.when(source_here)(total_of(like, rim_send.at[upper], rim_send.at[upper]).wait_send)
    for check, copy in singles:
        pl.when(check)(copy.wait_send)
    tall = blocks * h

    def blank(tiles, start, size):
        for k in tiles:
            t_ref[0, k, pl.ds(start, size), :] = jnp.ones((size, LANES), jnp.float32)
            t_ref[1, k, pl.ds(start, size), :] = jnp.zeros((size, LANES), jnp.float32)

    pl.when(i == 0)(lambda: blank(range(3), 0, half))
    pl.when(i == rows_n - 1)(lambda: blank(range(3), tall - half, half))
    pl.when((z == 0) & (c == 0))(lambda: blank((0,), 0, tall))
    pl.when((z == deep_n - 1) & (c == 1))(lambda: blank((2,), 0, tall))


def transmission(phase_volume, absorb_volume):
    deep, rows, lanes = phase_volume.shape
    beams = lax.axis_size("beam")
    h = rows // (beams * SUBS)
    dma = pltpu.SemaphoreType.DMA
    return pl.pallas_call(
        spread_kernel,
        out_shape=[
            jax.ShapeDtypeStruct((2, 3, 2 * rows, lanes), jnp.float32),
            jax.ShapeDtypeStruct((2, SUBS * h, lanes), jnp.float32),
        ],
        in_specs=[pl.BlockSpec(memory_space=pltpu.HBM)] * 2,
        out_specs=[pl.BlockSpec(memory_space=pltpu.VMEM)] * 2,
        scratch_shapes=[
            pltpu.VMEM((beams, 2, deep, SUBS * h, lanes), jnp.bfloat16),
            pltpu.VMEM((beams, SUBS, 2, h, lanes), jnp.float32),
            pltpu.VMEM((SUBS, beams, 2, h, lanes), jnp.float32),
            dma((beams, 2)),
            dma((SUBS,)),
            dma((SUBS,)),
            dma,
            dma,
            dma((2,)),
            dma,
            dma((2,)),
            dma((beams * SUBS,)),
            dma((3, 2 * beams * SUBS)),
        ],
        compiler_params=pltpu.CompilerParams(
            collective_id=0, has_side_effects=True, vmem_limit_bytes=VMEM_LIMIT
        ),
        name="spread",
    )(
        pltpu.with_memory_space_constraint(phase_volume, pltpu.HBM),
        pltpu.with_memory_space_constraint(absorb_volume, pltpu.HBM),
    )


def fold_kernel(
    scale, canvas_ref, own_ref, probe_ref, misfit_ref,
    grad, probe_out, sums_ref,
    sib_in, out_in, acc, corner_in, corner, row_in, q_in, p_in, p_sum, y_in, x_in, z_in, n_xy, n_zc,
    sib_send, sib_recv, out_send, out_recv, corner_send, corner_recv, row_send, row_recv,
    pair_send, pair_recv, group_send, group_recv,
):
    beams, rows_n, deep_n, cores = sizes()
    b, i, z, c = places()
    rows = grad.shape[1]
    h = rows // beams
    half = rows // 2
    tall = 2 * rows
    plane = beams * rows_n
    across = deep_n * cores
    out_z = z - 1 + 2 * c
    me_xy = b * rows_n + i
    me_zc = z * cores + c
    has_out = (out_z >= 0) & (out_z < deep_n)
    above, below = i > 0, i < rows_n - 1
    finish = []

    def go(copy, check=None):
        if check is None:
            copy.start()
        else:
            pl.when(check)(copy.start)
        finish.append((check, copy))
        return copy

    def peer_xy(o):
        return dict(beam=lax.rem(b + o // rows_n, beams), row=lax.rem(i + o % rows_n, rows_n))

    def peer_zc(o):
        return dict(col_0=lax.rem(z + o // cores, deep_n), col_1=lax.rem(c + o % cores, cores))

    def group(g, copies, like):
        for src, dst, where in copies:
            remote(src, dst, group_send.at[g], group_recv.at[g], **where).start()
        everything = remote(like, like, group_send.at[g], group_recv.at[g], col_1=1 - c)
        finish.append((None, everything))
        return everything

    barrier = pltpu.get_barrier_semaphore()
    for o in range(1, plane):
        greet(barrier, **peer_xy(o))
    for o in range(1, across):
        greet(barrier, **peer_zc(o))
    pl.semaphore_wait(barrier, plane + across - 2)

    middle = pl.ds(half, rows)
    subs = beams // 2
    pieces = []
    for s in range(subs):
        pieces.append((s * h, above, i - 1, below, subs + s))
        pieces.append((tall - half + s * h, below, i + 1, above, s))
    outer = dict(col_0=out_z, col_1=1 - c)
    half_copy = go(remote(probe_ref.at[1 - c], p_in, pair_send.at[0], pair_recv.at[0], col_1=1 - c))
    far_rims, near_rims, corners = [], [], []
    for e, (start, alive, goal, _, _) in enumerate(pieces):
        where = pl.ds(start, h)
        near_rims.append(
            go(
                remote(
                    canvas_ref.at[:, 2 - 2 * c, where, :], sib_in.at[:, where, :],
                    sib_send.at[e], sib_recv.at[e], col_1=1 - c,
                ),
                alive,
            )
        )
        far_rims.append(
            go(
                remote(
                    canvas_ref.at[0, 2 * c, where, :], out_in.at[0, where, :],
                    out_send.at[e], out_recv.at[e], **outer,
                ),
                has_out & alive,
            )
        )
        corners.append(
            go(
                remote(
                    canvas_ref.at[1, 2 * c, where, :], corner_in.at[e],
                    corner_send.at[e], corner_recv.at[e], row=goal,
                ),
                has_out & alive,
            )
        )
    far_first = go(
        remote(
            canvas_ref.at[0, 2 * c, middle, :], out_in.at[0, middle, :],
            out_send.at[beams], out_recv.at[beams], **outer,
        ),
        has_out,
    )
    near_middle = go(
        remote(
            canvas_ref.at[:, 2 - 2 * c, middle, :], sib_in.at[:, middle, :],
            sib_send.at[beams], sib_recv.at[beams], col_1=1 - c,
        )
    )
    half_copy.wait_recv()
    p_sum[...] = (probe_ref[c] + p_in[...]).reshape(p_sum.shape)
    parts = group(
        0,
        [
            (p_sum.at[:, lax.rem(b + o, beams)], y_in.at[o], dict(beam=lax.rem(b + o, beams)))
            for o in range(1, beams)
        ],
        y_in.at[pl.ds(1, beams - 1)],
    )

    edges, far_second = {}, {}

    def rim(p, e):
        start, alive, goal, _, _ = pieces[e]
        where = pl.ds(start, h)

        @pl.when(alive)
        def _():
            if p == 1:
                near_rims[e].wait_recv()
            acc[p, where, :] = canvas_ref[p, 1, where, :] + sib_in[p, where, :]
            if p == 0:

                @pl.when(has_out)
                def _():
                    far_rims[e].wait_recv()
                    acc[0, where, :] += out_in[0, where, :]

        edges[p, e] = go(
            remote(
                acc.at[p, where, :], row_in.at[p, e],
                row_send.at[p, e], row_recv.at[p, e], row=goal,
            ),
            alive,
        )

    def corner_piece(e):
        _, _, _, given, quarter = pieces[e]
        inside, there = pl.ds(quarter * h, h), pl.ds(half + quarter * h, h)

        @pl.when(has_out)
        def _():
            corner[inside, :] = canvas_ref[1, 2 * c, there, :]

            @pl.when(given)
            def _():
                corners[e].wait_recv()
                corner[inside, :] += corner_in[e]

        far_second[e] = go(
            remote(
                corner.at[inside, :], out_in.at[1, there, :],
                out_send.at[beams + 1 + e], out_recv.at[beams + 1 + e], **outer,
            ),
            has_out,
        )

    for e in range(beams):
        rim(1, e)
    for e in range(beams):
        rim(0, e)
        corner_piece(e)
    near_middle.wait_recv()
    acc[:, middle, :] = canvas_ref[:, 1, middle, :] + sib_in[:, middle, :]

    @pl.when(has_out)
    def _():
        far_first.wait_recv()
        acc[0, middle, :] += out_in[0, middle, :]

    quarters = remote(
        q_in.at[pl.ds(1, beams - 1)], q_in.at[pl.ds(1, beams - 1)],
        group_send.at[2], group_recv.at[2], col_1=1 - c,
    )
    finish.append((None, quarters))

    def settle(e):
        _, _, _, given, quarter = pieces[e]
        there = pl.ds(half + quarter * h, h)

        @pl.when(given)
        def _():
            for p in (1, 0):
                edges[p, e].wait_recv()
                acc[p, there, :] += row_in[p, e]

        @pl.when(has_out)
        def _():
            far_second[e].wait_recv()
            acc[1, there, :] += out_in[1, there, :]

        copy = remote(
            acc.at[:, there, :], q_in.at[b], group_send.at[2], group_recv.at[2], beam=quarter
        )
        pl.when(b != quarter)(copy.start)

    for e in range(2):
        settle(e)
    parts.wait_recv()
    block = p_sum[:, b]
    for o in range(1, beams):
        block = block + y_in[o]
    y_in[0] = block
    parts = group(
        1,
        [
            (y_in.at[0, lax.rem(i + o, rows_n)], x_in.at[o], dict(row=lax.rem(i + o, rows_n)))
            for o in range(1, rows_n)
        ],
        x_in.at[pl.ds(1, rows_n - 1)],
    )
    for e in range(2, beams):
        settle(e)
    mine = pl.ds(pl.multiple_of(half + b * h, h), h)
    q_in[b] = acc[:, mine, :]
    parts.wait_recv()
    total = y_in[0, i]
    for o in range(1, rows_n):
        total = total + x_in[o]
    z_in[z] = total
    levels = group(
        3,
        [
            (z_in.at[z], z_in.at[z], dict(col_0=lax.rem(z + o, deep_n)))
            for o in sorted(range(1, deep_n), key=lambda o: -min(o, deep_n - o))
        ],
        z_in.at[pl.ds(0, deep_n - 1)],
    )

    quarters.wait_recv()
    cr, ci = q_in[0, 0], q_in[0, 1]
    for o in range(1, beams):
        cr = cr + q_in[o, 0]
        ci = ci + q_in[o, 1]
    tr, ti = own_ref[0], own_ref[1]
    phase = tr * ci - ti * cr
    absorb = -(tr * cr + ti * ci)
    home = pl.ds(pl.multiple_of(b * h, h), h)
    grad[0, home, :] = phase
    grad[1, home, :] = absorb
    squares = jnp.sum(phase * phase + absorb * absorb, axis=0, keepdims=True)
    misfits = jnp.sum(misfit_ref[...], axis=0, keepdims=True)
    left = lax.broadcasted_iota(jnp.int32, (1, LANES), 1) < LANES // 2
    n_xy[me_xy] = jnp.where(
        left,
        squares + pltpu.roll(squares, LANES // 2, 1),
        misfits + pltpu.roll(misfits, LANES // 2, 1),
    )
    norms = group(
        4,
        [(n_xy.at[me_xy], n_xy.at[me_xy], peer_xy(o)) for o in range(1, plane)],
        n_xy.at[pl.ds(0, plane - 1)],
    )

    grads = group(
        6,
        [
            (grad.at[:, home, :], grad.at[:, home, :], dict(beam=lax.rem(b + o, beams)))
            for o in range(1, beams)
        ],
        q_in.at[pl.ds(1, beams - 1)],
    )

    levels.wait_recv()
    total = z_in[0]
    for k in range(1, deep_n):
        total = total + z_in[k]
    probe_out[c, i, b] = total * scale
    spreads = group(
        5,
        [(probe_out.at[c, i, b], probe_out.at[c, i, b], peer_xy(o)) for o in range(1, plane)],
        p_in.at[pl.ds(0, (plane - 1) * p_sum.shape[2]), :],
    )
    norms.wait_recv()
    pair = n_xy[0]
    for k in range(1, plane):
        pair = pair + n_xy[k]
    n_zc[me_zc] = pair
    norms = group(
        7,
        [
            (n_zc.at[me_zc], n_zc.at[me_zc], peer_zc(o))
            for o in sorted(range(1, across), key=lambda o: -min(o // cores, deep_n - o // cores))
        ],
        n_zc.at[pl.ds(0, across - 1)],
    )
    spreads.wait_recv()
    last = go(
        remote(probe_out.at[c], probe_out.at[c], pair_send.at[1], pair_recv.at[1], col_1=1 - c)
    )
    norms.wait_recv()
    pair = n_zc[0]
    for k in range(1, across):
        pair = pair + n_zc[k]
    sums_ref[...] = pair
    grads.wait_recv()
    last.wait_recv()
    for check, copy in finish:
        if check is None:
            copy.wait_send()
        else:
            pl.when(check)(copy.wait_send)


def folded(canvas, own, probe_sum, misfit, positions):
    beams, rows_n, deep_n, cores = sizes()
    _, _, tall, lanes = canvas.shape
    rows = tall // 2
    h = rows // beams
    n = probe_sum.shape[1]
    plane, across = beams * rows_n, deep_n * cores
    share = n // plane
    f32 = functools.partial(pltpu.VMEM, dtype=jnp.float32)
    outs, sides = 2 * beams + 1, beams + 1
    sems = [(sides,), (sides,), (outs,), (outs,), (beams,), (beams,)]
    sems += [(2, beams), (2, beams), (2,), (2,), (9,), (9,)]
    grad, probe_total, sums = pl.pallas_call(
        functools.partial(fold_kernel, 1.0 / positions),
        out_shape=[
            jax.ShapeDtypeStruct((2, rows, lanes), jnp.float32),
            jax.ShapeDtypeStruct((2, rows_n, beams, share, n), jnp.float32),
            jax.ShapeDtypeStruct((1, LANES), jnp.float32),
        ],
        in_specs=[pl.BlockSpec(memory_space=pltpu.VMEM)] * 4,
        out_specs=[pl.BlockSpec(memory_space=pltpu.VMEM)] * 3,
        scratch_shapes=[
            f32((2, tall, lanes)),
            f32((2, tall, lanes)),
            f32((2, tall, lanes)),
            f32((beams, h, lanes)),
            f32((rows, lanes)),
            f32((2, beams, h, lanes)),
            f32((beams, 2, h, lanes)),
            f32((n, n)),
            f32((rows_n, beams, share, n)),
            f32((beams, rows_n, share, n)),
            f32((rows_n, share, n)),
            f32((deep_n, share, n)),
            f32((plane, 1, LANES)),
            f32((across, 1, LANES)),
            *[pltpu.SemaphoreType.DMA(count) for count in sems],
        ],
        compiler_params=pltpu.CompilerParams(
            collective_id=1, has_side_effects=True, vmem_limit_bytes=VMEM_LIMIT
        ),
        name="fold",
    )(canvas, own, probe_sum, misfit)
    return grad, probe_total.reshape(probe_sum.shape), sums


def finish_kernel(entries, terms, grad_ref, probe_ref, sums_ref, step_ref, probe_out, loss_ref):
    sums = sums_ref[...]
    left = lax.broadcasted_iota(jnp.int32, sums.shape, 1) < LANES // 2
    square = jnp.sum(jnp.where(left, sums, 0.0), axis=1, keepdims=True)
    factor = jnp.minimum(1.0, 0.5 / jnp.sqrt(square / entries + 1e-06))
    for p in range(2):
        step_ref[p] = grad_ref[p] * factor
    probe_out[...] = probe_ref[...]
    loss_ref[...] = jnp.sum(jnp.where(left, 0.0, sums), axis=1, keepdims=True) / terms


def finished(grad, probe_total, sums, entries, terms):
    vmem = pl.BlockSpec(memory_space=pltpu.VMEM)
    return pl.pallas_call(
        functools.partial(finish_kernel, entries, terms),
        out_shape=[
            jax.ShapeDtypeStruct(grad.shape, jnp.float32),
            jax.ShapeDtypeStruct(probe_total.shape, jnp.float32),
            jax.ShapeDtypeStruct((1, 1), jnp.float32),
        ],
        in_specs=[vmem] * 3,
        out_specs=[vmem] * 3,
        compiler_params=pltpu.CompilerParams(vmem_limit_bytes=VMEM_LIMIT),
        name="finish",
    )(grad, probe_total, sums)


def local(phase_volume, absorb_volume, probe, amplitudes, scan_rows, scan_cols):
    length = probe.shape[1]
    count = scan_rows.shape[2]
    beams, rows_n, deep_n, cores = sizes()
    t, own = transmission(phase_volume, absorb_volume)
    canvas, probe_term, misfit = window_terms(
        t,
        probe,
        amplitudes.reshape(count, length, length),
        scan_rows.reshape(count),
        scan_cols.reshape(count),
    )
    positions = beams * rows_n * deep_n * cores * count
    grad, probe_total, sums = folded(canvas, own, probe_term, misfit, positions)
    entries = grad.size * rows_n * deep_n * cores
    step, probe_total, loss = finished(
        grad, probe_total, sums, entries, positions * length * length
    )
    return (step, probe_total, loss[0, 0])


def solution(mesh):
    split = Mesh(
        mesh.devices.reshape(mesh.shape["beam"], mesh.shape["row"], -1, 2),
        ("beam", "row", "col_0", "col_1"),
    )
    in_specs = (
        P("beam", "row", COL),
        P("beam", "row", COL),
        P(),
        P("row", COL, "beam", None, None),
        P("row", COL, "beam"),
        P("row", COL, "beam"),
    )
    out_specs = (P(None, "row", COL), P(), P())
    return jax.shard_map(local, mesh=split, in_specs=in_specs, out_specs=out_specs, check_vma=False)
```

```python
import functools
import math

import jax
import jax.numpy as jnp
import numpy as np
from jax import lax
from jax.experimental import pallas as pl
from jax.experimental.pallas import tpu as pltpu
from jax.sharding import Mesh
from jax.sharding import PartitionSpec as P

COL = ("col_0", "col_1")
MESH = pl.DeviceIdType.MESH
LANES = 128
CHUNK = 128
BATCH = 4
SUBS = 2
VMEM_LIMIT = 20 << 20


def dft_tables(length):
    indices = np.arange(length, dtype=np.int32)
    product = indices[:, None] * indices[None, :] % length
    angles = product.astype(np.float32) * np.float32(2.0 * math.pi / length)
    factor = np.float32(1.0 / math.sqrt(length))
    return (
        jnp.asarray(np.cos(angles) * factor).astype(jnp.bfloat16),
        jnp.asarray(-np.sin(angles) * factor).astype(jnp.bfloat16),
    )


def window_kernel(
    rows_ref, cols_ref, t_ref, probe_ref, amp_ref, table_ref,
    canvas_ref, probe_sum_ref, misfit_ref,
    fwd, bwd, cut, psi, half, chi, back,
):
    step = pl.program_id(0)
    n = probe_ref.shape[1]
    batch = amp_ref.shape[0]

    @pl.when(step == 0)
    def _():
        real, imag = table_ref[0], table_ref[1]
        minus = -imag
        fwd[:n, :n] = real
        fwd[:n, n:] = minus
        fwd[n:, :n] = imag
        fwd[n:, n:] = real
        bwd[:n, :n] = real
        bwd[:n, n:] = imag
        bwd[n:, :n] = minus
        bwd[n:, n:] = real
        canvas_ref[...] = jnp.zeros_like(canvas_ref)
        probe_sum_ref[...] = jnp.zeros_like(probe_sum_ref)
        misfit_ref[...] = jnp.zeros_like(misfit_ref)

    lane = lax.broadcasted_iota(jnp.int32, (32, LANES), 1)

    def cut_windows(j):
        row, col = rows_ref[step * batch + j], cols_ref[step * batch + j]
        turn = lax.rem(LANES - col, LANES)
        near = lane < LANES - col
        for at in range(0, n, 32):
            here = pl.ds(at, 32)
            pieces = []
            for part in range(2):
                turned = [
                    pltpu.roll(t_ref[part, k, pl.ds(row + at, 32), :], turn, 1)
                    for k in range(3)
                ]
                pieces.append([jnp.where(near, turned[k], turned[k + 1]) for k in range(2)])
            for k in range(2):
                lanes = pl.ds(k * LANES, LANES)
                tr, ti = pieces[0][k], pieces[1][k]
                cut[j, 0, here, lanes] = tr
                cut[j, 1, here, lanes] = ti
                pr = probe_ref[0, here, lanes]
                pi = probe_ref[1, here, lanes]
                psi[j, here, lanes] = (pr * tr - pi * ti).astype(jnp.bfloat16)
                psi[j, pl.ds(n + at, 32), lanes] = (pr * ti + pi * tr).astype(jnp.bfloat16)

    def to_half(j):
        for part in range(2):
            half[j, :, part * n : (part + 1) * n] = jnp.dot(
                fwd[part * n : (part + 1) * n, :], psi[j], preferred_element_type=jnp.float32
            ).astype(jnp.bfloat16)

    def to_far(j):
        total = jnp.zeros((8, LANES), jnp.float32)
        for at in range(0, n, CHUNK):
            here = pl.ds(at, CHUNK)
            far = jnp.dot(half[j, here, :], bwd[...], preferred_element_type=jnp.float32)
            fr, fi = far[:, :n], far[:, n:]
            amp = amp_ref[j, here, :].astype(jnp.float32)
            power = fr * fr + fi * fi
            inverse = lax.rsqrt(power)
            modulus = jnp.where(power > 0.0, power * inverse, 0.0)
            off = modulus - amp
            square = off * off
            total = total + jnp.sum(
                (square[:, :LANES] + square[:, LANES:]).reshape(CHUNK // 8, 8, LANES), axis=0
            )
            ratio = 1.0 - amp * jnp.minimum(inverse, 2.0)
            chi[j, here, :] = (fr * ratio).astype(jnp.bfloat16)
            chi[j, pl.ds(n + at, CHUNK), :] = (fi * ratio).astype(jnp.bfloat16)
        misfit_ref[...] += total

    def to_back(j):
        for part in range(2):
            back[j, :, part * n : (part + 1) * n] = jnp.dot(
                bwd[part * n : (part + 1) * n, :], chi[j], preferred_element_type=jnp.float32
            ).astype(jnp.bfloat16)

    def add_terms(j):
        row, col = rows_ref[step * batch + j], cols_ref[step * batch + j]
        far_side = lax.broadcasted_iota(jnp.int32, (CHUNK, LANES), 1) >= col
        for at in range(0, n, CHUNK):
            here = pl.ds(at, CHUNK)
            grad = jnp.dot(back[j, here, :], fwd[...], preferred_element_type=jnp.float32)
            gr, gi = grad[:, :n], grad[:, n:]
            tr, ti = cut[j, 0, here, :], cut[j, 1, here, :]
            probe_sum_ref[0, here, :] += tr * gr + ti * gi
            probe_sum_ref[1, here, :] += tr * gi - ti * gr
            pr, pi = probe_ref[0, here, :], probe_ref[1, here, :]
            for part, value in enumerate((pr * gr + pi * gi, pr * gi - pi * gr)):
                first = pltpu.roll(value[:, :LANES], col, 1)
                second = pltpu.roll(value[:, LANES:], col, 1)
                there = pl.ds(row + at, CHUNK)
                canvas_ref[part, 0, there, :] += jnp.where(far_side, first, 0.0)
                canvas_ref[part, 1, there, :] += jnp.where(far_side, second, first)
                canvas_ref[part, 2, there, :] += jnp.where(far_side, 0.0, second)

    steps = (cut_windows, to_half, to_far, to_back, add_terms)
    for tick in range(batch + len(steps) - 1):
        for at, stage in enumerate(steps):
            if 0 <= tick - at < batch:
                stage(tick - at)


def window_terms(t, probe, amplitudes, rows, cols):
    count, n, _ = amplitudes.shape
    batch = max(size for size in (1, 2, BATCH) if count % size == 0)
    grid_spec = pltpu.PrefetchScalarGridSpec(
        num_scalar_prefetch=2,
        grid=(count // batch,),
        in_specs=[
            pl.BlockSpec(t.shape, lambda s, *_: (0, 0, 0, 0)),
            pl.BlockSpec(probe.shape, lambda s, *_: (0, 0, 0)),
            pl.BlockSpec((batch, n, n), lambda s, *_: (s, 0, 0)),
            pl.BlockSpec((2, n, n), lambda s, *_: (0, 0, 0)),
        ],
        out_specs=[
            pl.BlockSpec(t.shape, lambda s, *_: (0, 0, 0, 0)),
            pl.BlockSpec(probe.shape, lambda s, *_: (0, 0, 0)),
            pl.BlockSpec((8, LANES), lambda s, *_: (0, 0)),
        ],
        scratch_shapes=[
            pltpu.VMEM((2 * n, 2 * n), jnp.bfloat16),
            pltpu.VMEM((2 * n, 2 * n), jnp.bfloat16),
            pltpu.VMEM((batch, 2, n, n), jnp.float32),
            pltpu.VMEM((batch, 2 * n, n), jnp.bfloat16),
            pltpu.VMEM((batch, n, 2 * n), jnp.bfloat16),
            pltpu.VMEM((batch, 2 * n, n), jnp.bfloat16),
            pltpu.VMEM((batch, n, 2 * n), jnp.bfloat16),
        ],
    )
    return pl.pallas_call(
        window_kernel,
        grid_spec=grid_spec,
        out_shape=[
            jax.ShapeDtypeStruct(t.shape, jnp.float32),
            jax.ShapeDtypeStruct(probe.shape, jnp.float32),
            jax.ShapeDtypeStruct((8, LANES), jnp.float32),
        ],
        compiler_params=pltpu.CompilerParams(
            dimension_semantics=("arbitrary",), vmem_limit_bytes=VMEM_LIMIT
        ),
        name="windows",
    )(rows, cols, t, probe, amplitudes, jnp.stack(dft_tables(n)))


def places():
    return tuple(lax.axis_index(axis) for axis in ("beam", "row", "col_0", "col_1"))


def sizes():
    return tuple(lax.axis_size(axis) for axis in ("beam", "row", "col_0", "col_1"))


def remote(src, dst, send_sem, recv_sem, **where):
    return pltpu.make_async_remote_copy(
        src_ref=src,
        dst_ref=dst,
        send_sem=send_sem,
        recv_sem=recv_sem,
        device_id=where,
        device_id_type=MESH,
    )


def greet(barrier, **where):
    pl.semaphore_signal(barrier, inc=1, device_id=where, device_id_type=MESH)


def spread_kernel(
    phase_ref, absorb_ref, t_ref, own_ref,
    vol, part, inbox,
    vol_sem, sum_send, sum_recv, beam_send, near_send, rim_send, out_send, row_send, corner_send,
    t_recv,
):
    beams, rows_n, deep_n, _ = sizes()
    b, i, z, c = places()
    subs, h = part.shape[1], part.shape[3]
    quarter_rows = subs * h
    top = beams // 2
    half = top * quarter_rows
    blocks = 2 * beams * subs
    out_z = z - 1 + 2 * c
    has_out = (out_z >= 0) & (out_z < deep_n)
    above, below = i > 0, i < rows_n - 1
    outer = dict(col_0=out_z, col_1=1 - c)
    order = [*range(1, beams), 0]
    loads = {}
    for o in order:
        q = lax.rem(b + o, beams)
        rows_here = pl.ds(pl.multiple_of(q * quarter_rows, quarter_rows), quarter_rows)
        for p, ref in enumerate((phase_ref, absorb_ref)):
            loads[o, p] = pltpu.make_async_copy(
                ref.at[:, rows_here, :], vol.at[o, p], vol_sem.at[o, p]
            )
            loads[o, p].start()

    barrier = pltpu.get_barrier_semaphore()
    for o in range(1, beams):
        greet(barrier, beam=lax.rem(b + o, beams))
    greet(barrier, col_1=1 - c)

    @pl.when(has_out)
    def _():
        greet(barrier, **outer)

    for alive, row in ((above, i - 1), (below, i + 1)):

        @pl.when(alive)
        def _(row=row):
            greet(barrier, row=row)

        @pl.when(alive & has_out)
        def _(row=row):
            greet(barrier, row=row, **outer)

    for o in order:
        for p in range(2):
            loads[o, p].wait()
            total = vol[o, p, 0].astype(jnp.float32)
            for d in range(1, phase_ref.shape[0]):
                total = total + vol[o, p, d].astype(jnp.float32)
            for s in range(subs):
                part[o, s, p] = total[s * h : (s + 1) * h]
    ups, downs, outs = (flag.astype(jnp.int32) for flag in (above, below, has_out))
    pl.semaphore_wait(barrier, beams + outs + (1 + outs) * (ups + downs))
    for s in range(subs):
        for o in order[:-1]:
            remote(
                part.at[o, s], inbox.at[s, o], sum_send.at[s], sum_recv.at[s],
                beam=lax.rem(b + o, beams),
            ).start()

    def cell(k, m):
        return t_ref.at[:, k, pl.ds(pl.multiple_of(m * h, h), h), :]

    def arrived(k, m, check=None):
        wait = remote(cell(1, m), cell(k, m), near_send, t_recv.at[k, m], col_1=1 - c).wait_recv
        if check is None:
            wait()
        else:
            pl.when(check)(wait)

    def spot(o, s):
        q = lax.rem(b + o, beams)
        upper = q // top
        rim = q * subs + s - top * subs + (1 - upper) * blocks
        goal, source = i - 1 + 2 * upper, i + 1 - 2 * upper
        return (
            top * subs + q * subs + s, rim, upper, goal,
            (goal >= 0) & (goal < rows_n), (source >= 0) & (source < rows_n),
        )

    ring = [1, *range(3, beams), *range(2, min(3, beams))]
    by_row, direct = {0}, {2}
    singles = []

    def single(check, slot, src, k, m, **where):
        copy = remote(src, cell(k, m), corner_send.at[slot], t_recv.at[k, m], **where)
        pl.when(check)(copy.start)
        singles.append((check, copy))

    def tile(o, s):
        m, rim, upper, goal, alive, _ = spot(o, s)
        if o:
            arrived(1, m)
        far = remote(
            cell(1, m), cell(2 - 2 * c, m), out_send, t_recv.at[2 - 2 * c, m], **outer
        )
        pl.when(has_out)(far.start)
        side = remote(cell(1, m), cell(1, rim), row_send.at[upper], t_recv.at[1, rim], row=goal)
        pl.when(alive)(side.start)
        if o in direct:
            single(
                alive & has_out, o * subs + s, cell(1, m), 2 - 2 * c, rim, row=goal, **outer
            )
        remote(cell(1, m), cell(2 * c, m), near_send, t_recv.at[2 * c, m], col_1=1 - c).start()

    def corner(o, s):
        m, rim, _, goal, alive, _ = spot(o, s)
        arrived(2 * c, m, has_out)
        if o in by_row:
            single(alive & has_out, o * subs + s, cell(2 * c, m), 2 * c, rim, row=goal)

    def edge(o, s):
        _, rim, upper, _, _, alive = spot(o, s)
        arrived(1, rim, alive)
        if o not in by_row and o not in direct:
            single(alive & has_out, o * subs + s, cell(1, rim), 2 - 2 * c, rim, **outer)
        copy = remote(
            cell(1, rim), cell(2 * c, rim), rim_send.at[upper], t_recv.at[2 * c, rim], col_1=1 - c
        )
        pl.when(alive)(copy.start)

    def total_of(like, send, recv):
        return remote(like, like, send, recv, col_1=1 - c)

    for s in range(subs):
        sums = total_of(inbox.at[s, pl.ds(1, beams - 1)], sum_send.at[s], sum_recv.at[s])
        sums.wait_recv()
        phase, absorb = part[0, s, 0], part[0, s, 1]
        for o in range(1, beams):
            phase = phase + inbox[s, o, 0]
            absorb = absorb + inbox[s, o, 1]
        damping = jnp.exp(-absorb)
        mine = pl.ds(pl.multiple_of(half + (b * subs + s) * h, h), h)
        for p, value in enumerate((damping * jnp.cos(phase), damping * jnp.sin(phase))):
            t_ref[p, 1, mine, :] = value
            own_ref[p, pl.ds(s * h, h), :] = value
        m = top * subs + b * subs + s
        for o in ring:
            remote(
                cell(1, m), cell(1, m), beam_send, t_recv.at[1, m], beam=lax.rem(b + o, beams)
            ).start()
        tile(0, s)
    events = []
    for s in range(subs):
        events += [(corner, 0, s), *[(tile, o, s) for o in ring if o not in direct], (edge, 0, s)]
        events += [(tile, o, s) for o in ring if o in direct]
    events += [(edge, o, s) for s in range(subs) for o in ring]
    for event, o, s in events:
        event(o, s)
    for s in range(subs):
        for o in range(beams):
            m, rim, _, _, _, alive = spot(o, s)
            if o:
                corner(o, s)
            arrived(2 - 2 * c, m)
            arrived(2 - 2 * c, rim, alive)
            arrived(2 * c, rim, alive & has_out)
    for s in range(subs):
        total_of(part.at[pl.ds(1, beams - 1), s], sum_send.at[s], sum_recv.at[s]).wait_send()
    total_of(part.at[pl.ds(1, beams - 1)], beam_send, beam_send).wait_send()
    total_of(part, near_send, near_send).wait_send()
    pl.when(has_out)(total_of(part, out_send, out_send).wait_send)
    for upper, (goal_here, source_here) in enumerate(((above, below), (below, above))):
        like = part.at[pl.ds(0, top)]
        pl.when(goal_here)(total_of(like, row_send.at[upper], row_send.at[upper]).wait_send)
        pl.when(source_here)(total_of(like, rim_send.at[upper], rim_send.at[upper]).wait_send)
    for check, copy in singles:
        pl.when(check)(copy.wait_send)
    tall = blocks * h

    def blank(tiles, start, size):
        for k in tiles:
            t_ref[0, k, pl.ds(start, size), :] = jnp.ones((size, LANES), jnp.float32)
            t_ref[1, k, pl.ds(start, size), :] = jnp.zeros((size, LANES), jnp.float32)

    pl.when(i == 0)(lambda: blank(range(3), 0, half))
    pl.when(i == rows_n - 1)(lambda: blank(range(3), tall - half, half))
    pl.when((z == 0) & (c == 0))(lambda: blank((0,), 0, tall))
    pl.when((z == deep_n - 1) & (c == 1))(lambda: blank((2,), 0, tall))


def transmission(phase_volume, absorb_volume):
    deep, rows, lanes = phase_volume.shape
    beams = lax.axis_size("beam")
    h = rows // (beams * SUBS)
    dma = pltpu.SemaphoreType.DMA
    return pl.pallas_call(
        spread_kernel,
        out_shape=[
            jax.ShapeDtypeStruct((2, 3, 2 * rows, lanes), jnp.float32),
            jax.ShapeDtypeStruct((2, SUBS * h, lanes), jnp.float32),
        ],
        in_specs=[pl.BlockSpec(memory_space=pltpu.HBM)] * 2,
        out_specs=[pl.BlockSpec(memory_space=pltpu.VMEM)] * 2,
        scratch_shapes=[
            pltpu.VMEM((beams, 2, deep, SUBS * h, lanes), jnp.bfloat16),
            pltpu.VMEM((beams, SUBS, 2, h, lanes), jnp.float32),
            pltpu.VMEM((SUBS, beams, 2, h, lanes), jnp.float32),
            dma((beams, 2)),
            dma((SUBS,)),
            dma((SUBS,)),
            dma,
            dma,
            dma((2,)),
            dma,
            dma((2,)),
            dma((beams * SUBS,)),
            dma((3, 2 * beams * SUBS)),
        ],
        compiler_params=pltpu.CompilerParams(
            collective_id=0, has_side_effects=True, vmem_limit_bytes=VMEM_LIMIT
        ),
        name="spread",
    )(
        pltpu.with_memory_space_constraint(phase_volume, pltpu.HBM),
        pltpu.with_memory_space_constraint(absorb_volume, pltpu.HBM),
    )


def fold_kernel(
    scale, canvas_ref, own_ref, probe_ref, misfit_ref,
    grad, probe_out, sums_ref,
    sib_in, out_in, acc, corner_in, corner, row_in, q_in, p_in, p_sum, y_in, x_in, z_in, n_xy, n_zc,
    sib_send, sib_recv, out_send, out_recv, corner_send, corner_recv, row_send, row_recv,
    pair_send, pair_recv, group_send, group_recv, word,
):
    beams, rows_n, deep_n, cores = sizes()
    b, i, z, c = places()
    rows = grad.shape[1]
    h = rows // beams
    half = rows // 2
    tall = 2 * rows
    plane = beams * rows_n
    across = deep_n * cores
    out_z = z - 1 + 2 * c
    me_xy = b * rows_n + i
    me_zc = z * cores + c
    has_out = (out_z >= 0) & (out_z < deep_n)
    above, below = i > 0, i < rows_n - 1
    finish = []

    def go(copy, check=None):
        if check is None:
            copy.start()
        else:
            pl.when(check)(copy.start)
        finish.append((check, copy))
        return copy

    def peer_xy(o):
        return dict(beam=lax.rem(b + o // rows_n, beams), row=lax.rem(i + o % rows_n, rows_n))

    def peer_zc(o):
        return dict(col_0=lax.rem(z + o // cores, deep_n), col_1=lax.rem(c + o % cores, cores))

    def group(g, copies, like):
        for src, dst, where in copies:
            remote(src, dst, group_send.at[g], group_recv.at[g], **where).start()
        everything = remote(like, like, group_send.at[g], group_recv.at[g], col_1=1 - c)
        finish.append((None, everything))
        return everything

    barrier = pltpu.get_barrier_semaphore()
    for o in range(1, beams):
        greet(barrier, beam=lax.rem(b + o, beams))
    for o in range(1, rows_n):
        greet(barrier, row=lax.rem(i + o, rows_n))
    greet(barrier, col_1=1 - c)
    for o in (1, deep_n - 1):
        greet(barrier, col_0=lax.rem(z + o, deep_n))

    @pl.when(has_out)
    def _():
        greet(barrier, col_0=out_z, col_1=1 - c)

    pl.semaphore_wait(barrier, beams + rows_n + 1 + has_out.astype(jnp.int32))
    for o in range(1, rows_n):
        greet(word.at[0], row=lax.rem(i + o, rows_n))
    for o in (1, deep_n - 1):
        greet(word.at[1], col_0=lax.rem(z + o, deep_n))

    middle = pl.ds(half, rows)
    subs = beams // 2
    pieces = []
    for s in range(subs):
        pieces.append((s * h, above, i - 1, below, subs + s))
        pieces.append((tall - half + s * h, below, i + 1, above, s))
    outer = dict(col_0=out_z, col_1=1 - c)
    half_copy = go(remote(probe_ref.at[1 - c], p_in, pair_send.at[0], pair_recv.at[0], col_1=1 - c))
    far_rims, near_rims, corners = [], [], []
    for e, (start, alive, goal, _, _) in enumerate(pieces):
        where = pl.ds(start, h)
        near_rims.append(
            go(
                remote(
                    canvas_ref.at[:, 2 - 2 * c, where, :], sib_in.at[:, where, :],
                    sib_send.at[e], sib_recv.at[e], col_1=1 - c,
                ),
                alive,
            )
        )
        far_rims.append(
            go(
                remote(
                    canvas_ref.at[0, 2 * c, where, :], out_in.at[0, where, :],
                    out_send.at[e], out_recv.at[e], **outer,
                ),
                has_out & alive,
            )
        )
        corners.append(
            go(
                remote(
                    canvas_ref.at[1, 2 * c, where, :], corner_in.at[e],
                    corner_send.at[e], corner_recv.at[e], row=goal,
                ),
                has_out & alive,
            )
        )
    far_first = go(
        remote(
            canvas_ref.at[0, 2 * c, middle, :], out_in.at[0, middle, :],
            out_send.at[beams], out_recv.at[beams], **outer,
        ),
        has_out,
    )
    near_middle = go(
        remote(
            canvas_ref.at[:, 2 - 2 * c, middle, :], sib_in.at[:, middle, :],
            sib_send.at[beams], sib_recv.at[beams], col_1=1 - c,
        )
    )
    half_copy.wait_recv()
    p_sum[...] = (probe_ref[c] + p_in[...]).reshape(p_sum.shape)
    parts = group(
        0,
        [
            (p_sum.at[:, lax.rem(b + o, beams)], y_in.at[o], dict(beam=lax.rem(b + o, beams)))
            for o in range(1, beams)
        ],
        y_in.at[pl.ds(1, beams - 1)],
    )

    edges, far_second = {}, {}

    def rim(p, e):
        start, alive, goal, _, _ = pieces[e]
        where = pl.ds(start, h)

        @pl.when(alive)
        def _():
            if p == 1:
                near_rims[e].wait_recv()
            acc[p, where, :] = canvas_ref[p, 1, where, :] + sib_in[p, where, :]
            if p == 0:

                @pl.when(has_out)
                def _():
                    far_rims[e].wait_recv()
                    acc[0, where, :] += out_in[0, where, :]

        edges[p, e] = go(
            remote(
                acc.at[p, where, :], row_in.at[p, e],
                row_send.at[p, e], row_recv.at[p, e], row=goal,
            ),
            alive,
        )

    def corner_piece(e):
        _, _, _, given, quarter = pieces[e]
        inside, there = pl.ds(quarter * h, h), pl.ds(half + quarter * h, h)

        @pl.when(has_out)
        def _():
            corner[inside, :] = canvas_ref[1, 2 * c, there, :]

            @pl.when(given)
            def _():
                corners[e].wait_recv()
                corner[inside, :] += corner_in[e]

        far_second[e] = go(
            remote(
                corner.at[inside, :], out_in.at[1, there, :],
                out_send.at[beams + 1 + e], out_recv.at[beams + 1 + e], **outer,
            ),
            has_out,
        )

    for e in range(beams):
        rim(1, e)
    for e in range(beams):
        rim(0, e)
        corner_piece(e)
    pl.semaphore_wait(word.at[1], 2)
    for o in (2, deep_n - 2):
        greet(word.at[2], col_0=lax.rem(z + o, deep_n))
    near_middle.wait_recv()
    acc[:, middle, :] = canvas_ref[:, 1, middle, :] + sib_in[:, middle, :]

    @pl.when(has_out)
    def _():
        far_first.wait_recv()
        acc[0, middle, :] += out_in[0, middle, :]

    quarters = remote(
        q_in.at[pl.ds(1, beams - 1)], q_in.at[pl.ds(1, beams - 1)],
        group_send.at[2], group_recv.at[2], col_1=1 - c,
    )
    finish.append((None, quarters))

    def settle(e):
        _, _, _, given, quarter = pieces[e]
        there = pl.ds(half + quarter * h, h)

        @pl.when(given)
        def _():
            for p in (1, 0):
                edges[p, e].wait_recv()
                acc[p, there, :] += row_in[p, e]

        @pl.when(has_out)
        def _():
            far_second[e].wait_recv()
            acc[1, there, :] += out_in[1, there, :]

        copy = remote(
            acc.at[:, there, :], q_in.at[b], group_send.at[2], group_recv.at[2], beam=quarter
        )
        pl.when(b != quarter)(copy.start)

    for e in range(2):
        settle(e)
    parts.wait_recv()
    block = p_sum[:, b]
    for o in range(1, beams):
        block = block + y_in[o]
    y_in[0] = block
    parts = group(
        1,
        [
            (y_in.at[0, lax.rem(i + o, rows_n)], x_in.at[o], dict(row=lax.rem(i + o, rows_n)))
            for o in range(1, rows_n)
        ],
        x_in.at[pl.ds(1, rows_n - 1)],
    )
    for e in range(2, beams):
        settle(e)
    mine = pl.ds(pl.multiple_of(half + b * h, h), h)
    q_in[b] = acc[:, mine, :]
    pl.semaphore_wait(word.at[0], rows_n - 1)
    pl.semaphore_wait(word.at[2], 2)
    parts.wait_recv()
    total = y_in[0, i]
    for o in range(1, rows_n):
        total = total + x_in[o]
    z_in[z] = total
    levels = group(
        3,
        [
            (z_in.at[z], z_in.at[z], dict(col_0=lax.rem(z + o, deep_n)))
            for o in sorted(range(1, deep_n), key=lambda o: -min(o, deep_n - o))
        ],
        z_in.at[pl.ds(0, deep_n - 1)],
    )

    quarters.wait_recv()
    cr, ci = q_in[0, 0], q_in[0, 1]
    for o in range(1, beams):
        cr = cr + q_in[o, 0]
        ci = ci + q_in[o, 1]
    tr, ti = own_ref[0], own_ref[1]
    phase = tr * ci - ti * cr
    absorb = -(tr * cr + ti * ci)
    home = pl.ds(pl.multiple_of(b * h, h), h)
    grad[0, home, :] = phase
    grad[1, home, :] = absorb
    squares = jnp.sum(phase * phase + absorb * absorb, axis=0, keepdims=True)
    misfits = jnp.sum(misfit_ref[...], axis=0, keepdims=True)
    left = lax.broadcasted_iota(jnp.int32, (1, LANES), 1) < LANES // 2
    n_xy[me_xy] = jnp.where(
        left,
        squares + pltpu.roll(squares, LANES // 2, 1),
        misfits + pltpu.roll(misfits, LANES // 2, 1),
    )
    norms = group(
        4,
        [(n_xy.at[me_xy], n_xy.at[me_xy], peer_xy(o)) for o in range(1, plane)],
        n_xy.at[pl.ds(0, plane - 1)],
    )

    grads = group(
        6,
        [
            (grad.at[:, home, :], grad.at[:, home, :], dict(beam=lax.rem(b + o, beams)))
            for o in range(1, beams)
        ],
        q_in.at[pl.ds(1, beams - 1)],
    )

    levels.wait_recv()
    total = z_in[0]
    for k in range(1, deep_n):
        total = total + z_in[k]
    probe_out[c, i, b] = total * scale
    spreads = group(
        5,
        [(probe_out.at[c, i, b], probe_out.at[c, i, b], peer_xy(o)) for o in range(1, plane)],
        p_in.at[pl.ds(0, (plane - 1) * p_sum.shape[2]), :],
    )
    norms.wait_recv()
    pair = n_xy[0]
    for k in range(1, plane):
        pair = pair + n_xy[k]
    n_zc[me_zc] = pair
    norms = group(
        7,
        [
            (n_zc.at[me_zc], n_zc.at[me_zc], peer_zc(o))
            for o in sorted(range(1, across), key=lambda o: -min(o // cores, deep_n - o // cores))
        ],
        n_zc.at[pl.ds(0, across - 1)],
    )
    spreads.wait_recv()
    last = go(
        remote(probe_out.at[c], probe_out.at[c], pair_send.at[1], pair_recv.at[1], col_1=1 - c)
    )
    norms.wait_recv()
    pair = n_zc[0]
    for k in range(1, across):
        pair = pair + n_zc[k]
    sums_ref[...] = pair
    grads.wait_recv()
    last.wait_recv()
    for check, copy in finish:
        if check is None:
            copy.wait_send()
        else:
            pl.when(check)(copy.wait_send)


def folded(canvas, own, probe_sum, misfit, positions):
    beams, rows_n, deep_n, cores = sizes()
    _, _, tall, lanes = canvas.shape
    rows = tall // 2
    h = rows // beams
    n = probe_sum.shape[1]
    plane, across = beams * rows_n, deep_n * cores
    share = n // plane
    f32 = functools.partial(pltpu.VMEM, dtype=jnp.float32)
    outs, sides = 2 * beams + 1, beams + 1
    sems = [(sides,), (sides,), (outs,), (outs,), (beams,), (beams,)]
    sems += [(2, beams), (2, beams), (2,), (2,), (9,), (9,)]
    grad, probe_total, sums = pl.pallas_call(
        functools.partial(fold_kernel, 1.0 / positions),
        out_shape=[
            jax.ShapeDtypeStruct((2, rows, lanes), jnp.float32),
            jax.ShapeDtypeStruct((2, rows_n, beams, share, n), jnp.float32),
            jax.ShapeDtypeStruct((1, LANES), jnp.float32),
        ],
        in_specs=[pl.BlockSpec(memory_space=pltpu.VMEM)] * 4,
        out_specs=[pl.BlockSpec(memory_space=pltpu.VMEM)] * 3,
        scratch_shapes=[
            f32((2, tall, lanes)),
            f32((2, tall, lanes)),
            f32((2, tall, lanes)),
            f32((beams, h, lanes)),
            f32((rows, lanes)),
            f32((2, beams, h, lanes)),
            f32((beams, 2, h, lanes)),
            f32((n, n)),
            f32((rows_n, beams, share, n)),
            f32((beams, rows_n, share, n)),
            f32((rows_n, share, n)),
            f32((deep_n, share, n)),
            f32((plane, 1, LANES)),
            f32((across, 1, LANES)),
            *[pltpu.SemaphoreType.DMA(count) for count in sems],
            pltpu.SemaphoreType.REGULAR((3,)),
        ],
        compiler_params=pltpu.CompilerParams(
            collective_id=1, has_side_effects=True, vmem_limit_bytes=VMEM_LIMIT
        ),
        name="fold",
    )(canvas, own, probe_sum, misfit)
    return grad, probe_total.reshape(probe_sum.shape), sums


def finish_kernel(entries, terms, grad_ref, probe_ref, sums_ref, step_ref, probe_out, loss_ref):
    sums = sums_ref[...]
    left = lax.broadcasted_iota(jnp.int32, sums.shape, 1) < LANES // 2
    square = jnp.sum(jnp.where(left, sums, 0.0), axis=1, keepdims=True)
    factor = jnp.minimum(1.0, 0.5 / jnp.sqrt(square / entries + 1e-06))
    for p in range(2):
        step_ref[p] = grad_ref[p] * factor
    probe_out[...] = probe_ref[...]
    loss_ref[...] = jnp.sum(jnp.where(left, 0.0, sums), axis=1, keepdims=True) / terms


def finished(grad, probe_total, sums, entries, terms):
    vmem = pl.BlockSpec(memory_space=pltpu.VMEM)
    return pl.pallas_call(
        functools.partial(finish_kernel, entries, terms),
        out_shape=[
            jax.ShapeDtypeStruct(grad.shape, jnp.float32),
            jax.ShapeDtypeStruct(probe_total.shape, jnp.float32),
            jax.ShapeDtypeStruct((1, 1), jnp.float32),
        ],
        in_specs=[vmem] * 3,
        out_specs=[vmem] * 3,
        compiler_params=pltpu.CompilerParams(vmem_limit_bytes=VMEM_LIMIT),
        name="finish",
    )(grad, probe_total, sums)


def local(phase_volume, absorb_volume, probe, amplitudes, scan_rows, scan_cols):
    length = probe.shape[1]
    count = scan_rows.shape[2]
    beams, rows_n, deep_n, cores = sizes()
    t, own = transmission(phase_volume, absorb_volume)
    canvas, probe_term, misfit = window_terms(
        t,
        probe,
        amplitudes.reshape(count, length, length),
        scan_rows.reshape(count),
        scan_cols.reshape(count),
    )
    positions = beams * rows_n * deep_n * cores * count
    grad, probe_total, sums = folded(canvas, own, probe_term, misfit, positions)
    entries = grad.size * rows_n * deep_n * cores
    step, probe_total, loss = finished(
        grad, probe_total, sums, entries, positions * length * length
    )
    return (step, probe_total, loss[0, 0])


def solution(mesh):
    split = Mesh(
        mesh.devices.reshape(mesh.shape["beam"], mesh.shape["row"], -1, 2),
        ("beam", "row", "col_0", "col_1"),
    )
    in_specs = (
        P("beam", "row", COL),
        P("beam", "row", COL),
        P(),
        P("row", COL, "beam", None, None),
        P("row", COL, "beam"),
        P("row", COL, "beam"),
    )
    out_specs = (P(None, "row", COL), P(), P())
    return jax.shard_map(local, mesh=split, in_specs=in_specs, out_specs=out_specs, check_vma=False)
```

```python
import functools
import math

import jax
import jax.numpy as jnp
import numpy as np
from jax import lax
from jax.experimental import pallas as pl
from jax.experimental.pallas import tpu as pltpu
from jax.sharding import Mesh
from jax.sharding import PartitionSpec as P

COL = ("col_0", "col_1")
MESH = pl.DeviceIdType.MESH
LANES = 128
CHUNK = 128
BATCH = 4
SUBS = 2
VMEM_LIMIT = 20 << 20


def dft_tables(length):
    indices = np.arange(length, dtype=np.int32)
    product = indices[:, None] * indices[None, :] % length
    angles = product.astype(np.float32) * np.float32(2.0 * math.pi / length)
    factor = np.float32(1.0 / math.sqrt(length))
    return (
        jnp.asarray(np.cos(angles) * factor).astype(jnp.bfloat16),
        jnp.asarray(-np.sin(angles) * factor).astype(jnp.bfloat16),
    )


def window_kernel(
    rows_ref, cols_ref, t_ref, probe_ref, amp_ref, table_ref,
    canvas_ref, probe_sum_ref, misfit_ref,
    fwd, bwd, cut, psi, half, chi, back,
):
    step = pl.program_id(0)
    n = probe_ref.shape[1]
    batch = amp_ref.shape[0]

    @pl.when(step == 0)
    def _():
        real, imag = table_ref[0], table_ref[1]
        minus = -imag
        fwd[:n, :n] = real
        fwd[:n, n:] = minus
        fwd[n:, :n] = imag
        fwd[n:, n:] = real
        bwd[:n, :n] = real
        bwd[:n, n:] = imag
        bwd[n:, :n] = minus
        bwd[n:, n:] = real
        canvas_ref[...] = jnp.zeros_like(canvas_ref)
        probe_sum_ref[...] = jnp.zeros_like(probe_sum_ref)
        misfit_ref[...] = jnp.zeros_like(misfit_ref)

    lane = lax.broadcasted_iota(jnp.int32, (32, LANES), 1)

    def cut_windows(j):
        row, col = rows_ref[step * batch + j], cols_ref[step * batch + j]
        turn = lax.rem(LANES - col, LANES)
        near = lane < LANES - col
        for at in range(0, n, 32):
            here = pl.ds(at, 32)
            pieces = []
            for part in range(2):
                turned = [
                    pltpu.roll(t_ref[part, k, pl.ds(row + at, 32), :], turn, 1)
                    for k in range(3)
                ]
                pieces.append([jnp.where(near, turned[k], turned[k + 1]) for k in range(2)])
            for k in range(2):
                lanes = pl.ds(k * LANES, LANES)
                tr, ti = pieces[0][k], pieces[1][k]
                cut[j, 0, here, lanes] = tr
                cut[j, 1, here, lanes] = ti
                pr = probe_ref[0, here, lanes]
                pi = probe_ref[1, here, lanes]
                psi[j, here, lanes] = (pr * tr - pi * ti).astype(jnp.bfloat16)
                psi[j, pl.ds(n + at, 32), lanes] = (pr * ti + pi * tr).astype(jnp.bfloat16)

    def to_half(j):
        for part in range(2):
            half[j, :, part * n : (part + 1) * n] = jnp.dot(
                fwd[part * n : (part + 1) * n, :], psi[j], preferred_element_type=jnp.float32
            ).astype(jnp.bfloat16)

    def to_far(j):
        total = jnp.zeros((8, LANES), jnp.float32)
        for at in range(0, n, CHUNK):
            here = pl.ds(at, CHUNK)
            far = jnp.dot(half[j, here, :], bwd[...], preferred_element_type=jnp.float32)
            fr, fi = far[:, :n], far[:, n:]
            amp = amp_ref[j, here, :].astype(jnp.float32)
            power = fr * fr + fi * fi
            inverse = lax.rsqrt(power)
            modulus = jnp.where(power > 0.0, power * inverse, 0.0)
            off = modulus - amp
            square = off * off
            total = total + jnp.sum(
                (square[:, :LANES] + square[:, LANES:]).reshape(CHUNK // 8, 8, LANES), axis=0
            )
            ratio = 1.0 - amp * jnp.minimum(inverse, 2.0)
            chi[j, here, :] = (fr * ratio).astype(jnp.bfloat16)
            chi[j, pl.ds(n + at, CHUNK), :] = (fi * ratio).astype(jnp.bfloat16)
        misfit_ref[...] += total

    def to_back(j):
        for part in range(2):
            back[j, :, part * n : (part + 1) * n] = jnp.dot(
                bwd[part * n : (part + 1) * n, :], chi[j], preferred_element_type=jnp.float32
            ).astype(jnp.bfloat16)

    def add_terms(j):
        row, col = rows_ref[step * batch + j], cols_ref[step * batch + j]
        far_side = lax.broadcasted_iota(jnp.int32, (CHUNK, LANES), 1) >= col
        for at in range(0, n, CHUNK):
            here = pl.ds(at, CHUNK)
            grad = jnp.dot(back[j, here, :], fwd[...], preferred_element_type=jnp.float32)
            gr, gi = grad[:, :n], grad[:, n:]
            tr, ti = cut[j, 0, here, :], cut[j, 1, here, :]
            probe_sum_ref[0, here, :] += tr * gr + ti * gi
            probe_sum_ref[1, here, :] += tr * gi - ti * gr
            pr, pi = probe_ref[0, here, :], probe_ref[1, here, :]
            for part, value in enumerate((pr * gr + pi * gi, pr * gi - pi * gr)):
                first = pltpu.roll(value[:, :LANES], col, 1)
                second = pltpu.roll(value[:, LANES:], col, 1)
                there = pl.ds(row + at, CHUNK)
                canvas_ref[part, 0, there, :] += jnp.where(far_side, first, 0.0)
                canvas_ref[part, 1, there, :] += jnp.where(far_side, second, first)
                canvas_ref[part, 2, there, :] += jnp.where(far_side, 0.0, second)

    steps = (cut_windows, to_half, to_far, to_back, add_terms)
    for tick in range(batch + len(steps) - 1):
        for at, stage in enumerate(steps):
            if 0 <= tick - at < batch:
                stage(tick - at)


def window_terms(t, probe, amplitudes, rows, cols):
    count, n, _ = amplitudes.shape
    batch = max(size for size in (1, 2, BATCH) if count % size == 0)
    grid_spec = pltpu.PrefetchScalarGridSpec(
        num_scalar_prefetch=2,
        grid=(count // batch,),
        in_specs=[
            pl.BlockSpec(t.shape, lambda s, *_: (0, 0, 0, 0)),
            pl.BlockSpec(probe.shape, lambda s, *_: (0, 0, 0)),
            pl.BlockSpec((batch, n, n), lambda s, *_: (s, 0, 0)),
            pl.BlockSpec((2, n, n), lambda s, *_: (0, 0, 0)),
        ],
        out_specs=[
            pl.BlockSpec(t.shape, lambda s, *_: (0, 0, 0, 0)),
            pl.BlockSpec(probe.shape, lambda s, *_: (0, 0, 0)),
            pl.BlockSpec((8, LANES), lambda s, *_: (0, 0)),
        ],
        scratch_shapes=[
            pltpu.VMEM((2 * n, 2 * n), jnp.bfloat16),
            pltpu.VMEM((2 * n, 2 * n), jnp.bfloat16),
            pltpu.VMEM((batch, 2, n, n), jnp.float32),
            pltpu.VMEM((batch, 2 * n, n), jnp.bfloat16),
            pltpu.VMEM((batch, n, 2 * n), jnp.bfloat16),
            pltpu.VMEM((batch, 2 * n, n), jnp.bfloat16),
            pltpu.VMEM((batch, n, 2 * n), jnp.bfloat16),
        ],
    )
    return pl.pallas_call(
        window_kernel,
        grid_spec=grid_spec,
        out_shape=[
            jax.ShapeDtypeStruct(t.shape, jnp.float32),
            jax.ShapeDtypeStruct(probe.shape, jnp.float32),
            jax.ShapeDtypeStruct((8, LANES), jnp.float32),
        ],
        compiler_params=pltpu.CompilerParams(
            dimension_semantics=("arbitrary",), vmem_limit_bytes=VMEM_LIMIT
        ),
        name="windows",
    )(rows, cols, t, probe, amplitudes, jnp.stack(dft_tables(n)))


def places():
    return tuple(lax.axis_index(axis) for axis in ("beam", "row", "col_0", "col_1"))


def sizes():
    return tuple(lax.axis_size(axis) for axis in ("beam", "row", "col_0", "col_1"))


def remote(src, dst, send_sem, recv_sem, **where):
    return pltpu.make_async_remote_copy(
        src_ref=src,
        dst_ref=dst,
        send_sem=send_sem,
        recv_sem=recv_sem,
        device_id=where,
        device_id_type=MESH,
    )


def greet(barrier, **where):
    pl.semaphore_signal(barrier, inc=1, device_id=where, device_id_type=MESH)


def spread_kernel(
    phase_ref, absorb_ref, t_ref, own_ref,
    vol, part, inbox,
    vol_sem, sum_send, sum_recv, beam_send, near_send, near_recv, rim_send, rim_recv,
    out_send, out_recv, own_recv, row_send, corner_send, corner_recv, t_recv,
):
    beams, rows_n, deep_n, _ = sizes()
    b, i, z, c = places()
    subs, h = part.shape[1], part.shape[3]
    quarter_rows = subs * h
    top = beams // 2
    half = top * quarter_rows
    blocks = 2 * beams * subs
    out_z = z - 1 + 2 * c
    has_out = (out_z >= 0) & (out_z < deep_n)
    above, below = i > 0, i < rows_n - 1
    outer = dict(col_0=out_z, col_1=1 - c)
    order = [*range(1, beams), 0]
    loads = {}
    for o in order:
        q = lax.rem(b + o, beams)
        rows_here = pl.ds(pl.multiple_of(q * quarter_rows, quarter_rows), quarter_rows)
        for p, ref in enumerate((phase_ref, absorb_ref)):
            loads[o, p] = pltpu.make_async_copy(
                ref.at[:, rows_here, :], vol.at[o, p], vol_sem.at[o, p]
            )
            loads[o, p].start()

    barrier = pltpu.get_barrier_semaphore()
    for o in range(1, beams):
        greet(barrier, beam=lax.rem(b + o, beams))
    greet(barrier, col_1=1 - c)

    @pl.when(has_out)
    def _():
        greet(barrier, **outer)

    for alive, row in ((above, i - 1), (below, i + 1)):

        @pl.when(alive)
        def _(row=row):
            greet(barrier, row=row)

        @pl.when(alive & has_out)
        def _(row=row):
            greet(barrier, row=row, **outer)

    for o in order:
        for p in range(2):
            loads[o, p].wait()
            total = vol[o, p, 0].astype(jnp.float32)
            for d in range(1, phase_ref.shape[0]):
                total = total + vol[o, p, d].astype(jnp.float32)
            for s in range(subs):
                part[o, s, p] = total[s * h : (s + 1) * h]
    ups, downs, outs = (flag.astype(jnp.int32) for flag in (above, below, has_out))
    pl.semaphore_wait(barrier, beams + outs + (1 + outs) * (ups + downs))
    for s in range(subs):
        for o in order[:-1]:
            remote(
                part.at[o, s], inbox.at[s, o], sum_send.at[s], sum_recv.at[s],
                beam=lax.rem(b + o, beams),
            ).start()

    def cell(k, m):
        return t_ref.at[:, k, pl.ds(pl.multiple_of(m * h, h), h), :]

    def arrived(m, check=None):
        wait = remote(cell(1, m), cell(1, m), near_send, t_recv.at[m], col_1=1 - c).wait_recv
        if check is None:
            wait()
        else:
            pl.when(check)(wait)

    def spot(o, s):
        q = lax.rem(b + o, beams)
        upper = q // top
        rim = q * subs + s - top * subs + (1 - upper) * blocks
        goal, source = i - 1 + 2 * upper, i + 1 - 2 * upper
        return (
            top * subs + q * subs + s, rim, upper, goal,
            (goal >= 0) & (goal < rows_n), (source >= 0) & (source < rows_n),
        )

    ring = [1, *range(3, beams), *range(2, min(3, beams))]
    by_row, direct = {0}, {2}
    singles = []

    def single(check, slot, upper, src, dst, **where):
        copy = remote(src, dst, corner_send.at[slot], corner_recv.at[upper], **where)
        pl.when(check)(copy.start)
        singles.append((check, copy))

    def tile(o, s):
        m, rim, upper, goal, alive, _ = spot(o, s)
        if o:
            arrived(m)
        landed = own_recv.at[s] if o in by_row else out_recv
        far = remote(cell(1, m), cell(2 - 2 * c, m), out_send, landed, **outer)
        pl.when(has_out)(far.start)
        side = remote(cell(1, m), cell(1, rim), row_send.at[upper], t_recv.at[rim], row=goal)
        pl.when(alive)(side.start)
        if o in direct:
            single(
                alive & has_out, o * subs + s, upper, cell(1, m), cell(2 - 2 * c, rim),
                row=goal, **outer,
            )
        remote(cell(1, m), cell(2 * c, m), near_send, near_recv, col_1=1 - c).start()

    def corner(o, s):
        m, rim, upper, goal, alive, _ = spot(o, s)
        here = cell(2 * c, m)
        pl.when(has_out)(remote(here, here, out_send, own_recv.at[s], **outer).wait_recv)
        single(alive & has_out, o * subs + s, upper, here, cell(2 * c, rim), row=goal)

    def edge(o, s):
        _, rim, upper, _, _, alive = spot(o, s)
        arrived(rim, alive)
        if o not in by_row and o not in direct:
            single(
                alive & has_out, o * subs + s, upper, cell(1, rim), cell(2 - 2 * c, rim), **outer
            )
        copy = remote(
            cell(1, rim), cell(2 * c, rim), rim_send.at[upper], rim_recv.at[upper], col_1=1 - c
        )
        pl.when(alive)(copy.start)

    def total_of(like, send, recv):
        return remote(like, like, send, recv, col_1=1 - c)

    for s in range(subs):
        sums = total_of(inbox.at[s, pl.ds(1, beams - 1)], sum_send.at[s], sum_recv.at[s])
        sums.wait_recv()
        phase, absorb = part[0, s, 0], part[0, s, 1]
        for o in range(1, beams):
            phase = phase + inbox[s, o, 0]
            absorb = absorb + inbox[s, o, 1]
        damping = jnp.exp(-absorb)
        mine = pl.ds(pl.multiple_of(half + (b * subs + s) * h, h), h)
        for p, value in enumerate((damping * jnp.cos(phase), damping * jnp.sin(phase))):
            t_ref[p, 1, mine, :] = value
            own_ref[p, pl.ds(s * h, h), :] = value
        m = top * subs + b * subs + s
        for o in ring:
            remote(
                cell(1, m), cell(1, m), beam_send, t_recv.at[m], beam=lax.rem(b + o, beams)
            ).start()
        tile(0, s)
    events = []
    for s in range(subs):
        events += [(corner, 0, s), *[(tile, o, s) for o in ring if o not in direct], (edge, 0, s)]
        events += [(tile, o, s) for o in ring if o in direct]
    events += [(edge, o, s) for s in range(subs) for o in ring]
    for event, o, s in events:
        event(o, s)
    most = part.at[pl.ds(1, beams - 1)]
    some = part.at[pl.ds(0, top)]
    total_of(part, near_send, near_recv).wait_recv()
    pl.when(has_out)(total_of(most, out_send, out_recv).wait_recv)
    for upper, source_here in enumerate((below, above)):
        pl.when(source_here)(total_of(some, rim_send.at[upper], rim_recv.at[upper]).wait_recv)
        pl.when(source_here & has_out)(
            total_of(some, rim_send.at[upper], corner_recv.at[upper]).wait_recv
        )
    for s in range(subs):
        total_of(part.at[pl.ds(1, beams - 1), s], sum_send.at[s], sum_recv.at[s]).wait_send()
    total_of(most, beam_send, beam_send).wait_send()
    total_of(part, near_send, near_send).wait_send()
    pl.when(has_out)(total_of(part, out_send, out_send).wait_send)
    for upper, (goal_here, source_here) in enumerate(((above, below), (below, above))):
        pl.when(goal_here)(total_of(some, row_send.at[upper], row_send.at[upper]).wait_send)
        pl.when(source_here)(total_of(some, rim_send.at[upper], rim_send.at[upper]).wait_send)
    for check, copy in singles:
        pl.when(check)(copy.wait_send)
    tall = blocks * h

    def blank(tiles, start, size):
        for k in tiles:
            t_ref[0, k, pl.ds(start, size), :] = jnp.ones((size, LANES), jnp.float32)
            t_ref[1, k, pl.ds(start, size), :] = jnp.zeros((size, LANES), jnp.float32)

    pl.when(i == 0)(lambda: blank(range(3), 0, half))
    pl.when(i == rows_n - 1)(lambda: blank(range(3), tall - half, half))
    pl.when((z == 0) & (c == 0))(lambda: blank((0,), 0, tall))
    pl.when((z == deep_n - 1) & (c == 1))(lambda: blank((2,), 0, tall))


def transmission(phase_volume, absorb_volume):
    deep, rows, lanes = phase_volume.shape
    beams = lax.axis_size("beam")
    h = rows // (beams * SUBS)
    dma = pltpu.SemaphoreType.DMA
    return pl.pallas_call(
        spread_kernel,
        out_shape=[
            jax.ShapeDtypeStruct((2, 3, 2 * rows, lanes), jnp.float32),
            jax.ShapeDtypeStruct((2, SUBS * h, lanes), jnp.float32),
        ],
        in_specs=[pl.BlockSpec(memory_space=pltpu.HBM)] * 2,
        out_specs=[pl.BlockSpec(memory_space=pltpu.VMEM)] * 2,
        scratch_shapes=[
            pltpu.VMEM((beams, 2, deep, SUBS * h, lanes), jnp.bfloat16),
            pltpu.VMEM((beams, SUBS, 2, h, lanes), jnp.float32),
            pltpu.VMEM((SUBS, beams, 2, h, lanes), jnp.float32),
            dma((beams, 2)),
            dma((SUBS,)),
            dma((SUBS,)),
            dma,
            dma,
            dma,
            dma((2,)),
            dma((2,)),
            dma,
            dma,
            dma((SUBS,)),
            dma((2,)),
            dma((beams * SUBS,)),
            dma((2,)),
            dma((2 * beams * SUBS,)),
        ],
        compiler_params=pltpu.CompilerParams(
            collective_id=0, has_side_effects=True, vmem_limit_bytes=VMEM_LIMIT
        ),
        name="spread",
    )(
        pltpu.with_memory_space_constraint(phase_volume, pltpu.HBM),
        pltpu.with_memory_space_constraint(absorb_volume, pltpu.HBM),
    )


def fold_kernel(
    scale, canvas_ref, own_ref, probe_ref, misfit_ref,
    grad, probe_out, sums_ref,
    sib_in, out_in, acc, corner_in, corner, row_in, q_in, p_in, p_sum, y_in, x_in, z_in, n_xy, n_zc,
    sib_send, sib_recv, out_send, out_recv, corner_send, corner_recv, row_send, row_recv,
    pair_send, pair_recv, group_send, group_recv, word,
):
    beams, rows_n, deep_n, cores = sizes()
    b, i, z, c = places()
    rows = grad.shape[1]
    h = rows // beams
    half = rows // 2
    tall = 2 * rows
    plane = beams * rows_n
    across = deep_n * cores
    out_z = z - 1 + 2 * c
    me_xy = b * rows_n + i
    me_zc = z * cores + c
    has_out = (out_z >= 0) & (out_z < deep_n)
    above, below = i > 0, i < rows_n - 1
    finish = []

    def go(copy, check=None):
        if check is None:
            copy.start()
        else:
            pl.when(check)(copy.start)
        finish.append((check, copy))
        return copy

    def peer_xy(o):
        return dict(beam=lax.rem(b + o // rows_n, beams), row=lax.rem(i + o % rows_n, rows_n))

    def peer_zc(o):
        return dict(col_0=lax.rem(z + o // cores, deep_n), col_1=lax.rem(c + o % cores, cores))

    def group(g, copies, like):
        for src, dst, where in copies:
            remote(src, dst, group_send.at[g], group_recv.at[g], **where).start()
        everything = remote(like, like, group_send.at[g], group_recv.at[g], col_1=1 - c)
        finish.append((None, everything))
        return everything

    barrier = pltpu.get_barrier_semaphore()
    for o in range(1, beams):
        greet(barrier, beam=lax.rem(b + o, beams))
    for o in range(1, rows_n):
        greet(barrier, row=lax.rem(i + o, rows_n))
    greet(barrier, col_1=1 - c)
    for o in (1, deep_n - 1):
        greet(barrier, col_0=lax.rem(z + o, deep_n))

    @pl.when(has_out)
    def _():
        greet(barrier, col_0=out_z, col_1=1 - c)

    pl.semaphore_wait(barrier, beams + rows_n + 1 + has_out.astype(jnp.int32))
    for o in range(1, rows_n):
        greet(word.at[0], row=lax.rem(i + o, rows_n))
    for o in (1, deep_n - 1):
        greet(word.at[1], col_0=lax.rem(z + o, deep_n))

    middle = pl.ds(half, rows)
    subs = beams // 2
    pieces = []
    for s in range(subs):
        pieces.append((s * h, above, i - 1, below, subs + s))
        pieces.append((tall - half + s * h, below, i + 1, above, s))
    outer = dict(col_0=out_z, col_1=1 - c)
    half_copy = go(remote(probe_ref.at[1 - c], p_in, pair_send.at[0], pair_recv.at[0], col_1=1 - c))
    far_rims, near_rims, corners = [], [], []
    for e, (start, alive, goal, _, _) in enumerate(pieces):
        where = pl.ds(start, h)
        near_rims.append(
            go(
                remote(
                    canvas_ref.at[:, 2 - 2 * c, where, :], sib_in.at[:, where, :],
                    sib_send.at[e], sib_recv.at[e], col_1=1 - c,
                ),
                alive,
            )
        )
        far_rims.append(
            go(
                remote(
                    canvas_ref.at[0, 2 * c, where, :], out_in.at[0, where, :],
                    out_send.at[e], out_recv.at[e], **outer,
                ),
                has_out & alive,
            )
        )
        corners.append(
            go(
                remote(
                    canvas_ref.at[1, 2 * c, where, :], corner_in.at[e],
                    corner_send.at[e], corner_recv.at[e], row=goal,
                ),
                has_out & alive,
            )
        )
    far_first = go(
        remote(
            canvas_ref.at[0, 2 * c, middle, :], out_in.at[0, middle, :],
            out_send.at[beams], out_recv.at[beams], **outer,
        ),
        has_out,
    )
    near_middle = go(
        remote(
            canvas_ref.at[:, 2 - 2 * c, middle, :], sib_in.at[:, middle, :],
            sib_send.at[beams], sib_recv.at[beams], col_1=1 - c,
        )
    )
    half_copy.wait_recv()
    p_sum[...] = (probe_ref[c] + p_in[...]).reshape(p_sum.shape)
    parts = group(
        0,
        [
            (p_sum.at[:, lax.rem(b + o, beams)], y_in.at[o], dict(beam=lax.rem(b + o, beams)))
            for o in range(1, beams)
        ],
        y_in.at[pl.ds(1, beams - 1)],
    )

    edges, far_second = {}, {}

    def rim(p, e):
        start, alive, goal, _, _ = pieces[e]
        where = pl.ds(start, h)

        @pl.when(alive)
        def _():
            if p == 1:
                near_rims[e].wait_recv()
            acc[p, where, :] = canvas_ref[p, 1, where, :] + sib_in[p, where, :]
            if p == 0:

                @pl.when(has_out)
                def _():
                    far_rims[e].wait_recv()
                    acc[0, where, :] += out_in[0, where, :]

        edges[p, e] = go(
            remote(
                acc.at[p, where, :], row_in.at[p, e],
                row_send.at[p, e], row_recv.at[p, e], row=goal,
            ),
            alive,
        )

    def corner_piece(e):
        _, _, _, given, quarter = pieces[e]
        inside, there = pl.ds(quarter * h, h), pl.ds(half + quarter * h, h)

        @pl.when(has_out)
        def _():
            corner[inside, :] = canvas_ref[1, 2 * c, there, :]

            @pl.when(given)
            def _():
                corners[e].wait_recv()
                corner[inside, :] += corner_in[e]

        far_second[e] = go(
            remote(
                corner.at[inside, :], out_in.at[1, there, :],
                out_send.at[beams + 1 + e], out_recv.at[beams + 1 + e], **outer,
            ),
            has_out,
        )

    for e in range(beams):
        rim(1, e)
    for e in range(beams):
        rim(0, e)
        corner_piece(e)
    pl.semaphore_wait(word.at[1], 2)
    for o in (2, deep_n - 2):
        greet(word.at[2], col_0=lax.rem(z + o, deep_n))
    near_middle.wait_recv()
    acc[:, middle, :] = canvas_ref[:, 1, middle, :] + sib_in[:, middle, :]

    @pl.when(has_out)
    def _():
        far_first.wait_recv()
        acc[0, middle, :] += out_in[0, middle, :]

    quarters = remote(
        q_in.at[pl.ds(1, beams - 1)], q_in.at[pl.ds(1, beams - 1)],
        group_send.at[2], group_recv.at[2], col_1=1 - c,
    )
    finish.append((None, quarters))

    def settle(e):
        _, _, _, given, quarter = pieces[e]
        there = pl.ds(half + quarter * h, h)

        @pl.when(given)
        def _():
            for p in (1, 0):
                edges[p, e].wait_recv()
                acc[p, there, :] += row_in[p, e]

        @pl.when(has_out)
        def _():
            far_second[e].wait_recv()
            acc[1, there, :] += out_in[1, there, :]

        copy = remote(
            acc.at[:, there, :], q_in.at[b], group_send.at[2], group_recv.at[2], beam=quarter
        )
        pl.when(b != quarter)(copy.start)

    for e in range(2):
        settle(e)
    parts.wait_recv()
    block = p_sum[:, b]
    for o in range(1, beams):
        block = block + y_in[o]
    y_in[0] = block
    parts = group(
        1,
        [
            (y_in.at[0, lax.rem(i + o, rows_n)], x_in.at[o], dict(row=lax.rem(i + o, rows_n)))
            for o in range(1, rows_n)
        ],
        x_in.at[pl.ds(1, rows_n - 1)],
    )
    for e in range(2, beams):
        settle(e)
    mine = pl.ds(pl.multiple_of(half + b * h, h), h)
    q_in[b] = acc[:, mine, :]
    pl.semaphore_wait(word.at[0], rows_n - 1)
    pl.semaphore_wait(word.at[2], 2)
    parts.wait_recv()
    total = y_in[0, i]
    for o in range(1, rows_n):
        total = total + x_in[o]
    z_in[z] = total
    levels = group(
        3,
        [
            (z_in.at[z], z_in.at[z], dict(col_0=lax.rem(z + o, deep_n)))
            for o in sorted(range(1, deep_n), key=lambda o: -min(o, deep_n - o))
        ],
        z_in.at[pl.ds(0, deep_n - 1)],
    )

    quarters.wait_recv()
    cr, ci = q_in[0, 0], q_in[0, 1]
    for o in range(1, beams):
        cr = cr + q_in[o, 0]
        ci = ci + q_in[o, 1]
    tr, ti = own_ref[0], own_ref[1]
    phase = tr * ci - ti * cr
    absorb = -(tr * cr + ti * ci)
    home = pl.ds(pl.multiple_of(b * h, h), h)
    grad[0, home, :] = phase
    grad[1, home, :] = absorb
    squares = jnp.sum(phase * phase + absorb * absorb, axis=0, keepdims=True)
    misfits = jnp.sum(misfit_ref[...], axis=0, keepdims=True)
    left = lax.broadcasted_iota(jnp.int32, (1, LANES), 1) < LANES // 2
    n_xy[me_xy] = jnp.where(
        left,
        squares + pltpu.roll(squares, LANES // 2, 1),
        misfits + pltpu.roll(misfits, LANES // 2, 1),
    )
    norms = group(
        4,
        [(n_xy.at[me_xy], n_xy.at[me_xy], peer_xy(o)) for o in range(1, plane)],
        n_xy.at[pl.ds(0, plane - 1)],
    )

    grads = group(
        6,
        [
            (grad.at[:, home, :], grad.at[:, home, :], dict(beam=lax.rem(b + o, beams)))
            for o in range(1, beams)
        ],
        q_in.at[pl.ds(1, beams - 1)],
    )

    levels.wait_recv()
    total = z_in[0]
    for k in range(1, deep_n):
        total = total + z_in[k]
    probe_out[c, i, b] = total * scale
    share = p_sum.shape[2]
    own_piece = probe_out.at[c, i, b]
    near_by = [o for o in range(1, plane) if o % rows_n != rows_n // 2]
    far_off = [o for o in range(1, plane) if o % rows_n == rows_n // 2]
    spreads = group(
        5,
        [(own_piece, own_piece, peer_xy(o)) for o in near_by],
        p_in.at[pl.ds(0, len(near_by) * share), :],
    )
    far_pieces = group(
        8,
        [
            (own_piece, own_piece, dict(peer_xy(o), col_1=core))
            for core in (c, 1 - c)
            for o in far_off
        ],
        p_in.at[pl.ds(0, 2 * len(far_off) * share), :],
    )
    norms.wait_recv()
    pair = n_xy[0]
    for k in range(1, plane):
        pair = pair + n_xy[k]
    n_zc[me_zc] = pair
    norms = group(
        7,
        [
            (n_zc.at[me_zc], n_zc.at[me_zc], peer_zc(o))
            for o in sorted(range(1, across), key=lambda o: -min(o // cores, deep_n - o // cores))
        ],
        n_zc.at[pl.ds(0, across - 1)],
    )
    spreads.wait_recv()
    last = group(
        9,
        [
            (
                probe_out.at[c, lax.rem(i + o, rows_n)],
                probe_out.at[c, lax.rem(i + o, rows_n)],
                dict(col_1=1 - c),
            )
            for o in range(rows_n)
            if o != rows_n // 2
        ],
        probe_out.at[0, pl.ds(0, rows_n - 1)],
    )
    norms.wait_recv()
    pair = n_zc[0]
    for k in range(1, across):
        pair = pair + n_zc[k]
    sums_ref[...] = pair
    grads.wait_recv()
    far_pieces.wait_recv()
    last.wait_recv()
    for check, copy in finish:
        if check is None:
            copy.wait_send()
        else:
            pl.when(check)(copy.wait_send)


def folded(canvas, own, probe_sum, misfit, positions):
    beams, rows_n, deep_n, cores = sizes()
    _, _, tall, lanes = canvas.shape
    rows = tall // 2
    h = rows // beams
    n = probe_sum.shape[1]
    plane, across = beams * rows_n, deep_n * cores
    share = n // plane
    f32 = functools.partial(pltpu.VMEM, dtype=jnp.float32)
    outs, sides = 2 * beams + 1, beams + 1
    sems = [(sides,), (sides,), (outs,), (outs,), (beams,), (beams,)]
    sems += [(2, beams), (2, beams), (1,), (1,), (10,), (10,)]
    grad, probe_total, sums = pl.pallas_call(
        functools.partial(fold_kernel, 1.0 / positions),
        out_shape=[
            jax.ShapeDtypeStruct((2, rows, lanes), jnp.float32),
            jax.ShapeDtypeStruct((2, rows_n, beams, share, n), jnp.float32),
            jax.ShapeDtypeStruct((1, LANES), jnp.float32),
        ],
        in_specs=[pl.BlockSpec(memory_space=pltpu.VMEM)] * 4,
        out_specs=[pl.BlockSpec(memory_space=pltpu.VMEM)] * 3,
        scratch_shapes=[
            f32((2, tall, lanes)),
            f32((2, tall, lanes)),
            f32((2, tall, lanes)),
            f32((beams, h, lanes)),
            f32((rows, lanes)),
            f32((2, beams, h, lanes)),
            f32((beams, 2, h, lanes)),
            f32((n, n)),
            f32((rows_n, beams, share, n)),
            f32((beams, rows_n, share, n)),
            f32((rows_n, share, n)),
            f32((deep_n, share, n)),
            f32((plane, 1, LANES)),
            f32((across, 1, LANES)),
            *[pltpu.SemaphoreType.DMA(count) for count in sems],
            pltpu.SemaphoreType.REGULAR((3,)),
        ],
        compiler_params=pltpu.CompilerParams(
            collective_id=1, has_side_effects=True, vmem_limit_bytes=VMEM_LIMIT
        ),
        name="fold",
    )(canvas, own, probe_sum, misfit)
    return grad, probe_total.reshape(probe_sum.shape), sums


def finish_kernel(entries, terms, grad_ref, probe_ref, sums_ref, step_ref, probe_out, loss_ref):
    sums = sums_ref[...]
    left = lax.broadcasted_iota(jnp.int32, sums.shape, 1) < LANES // 2
    square = jnp.sum(jnp.where(left, sums, 0.0), axis=1, keepdims=True)
    factor = jnp.minimum(1.0, 0.5 / jnp.sqrt(square / entries + 1e-06))
    for p in range(2):
        step_ref[p] = grad_ref[p] * factor
    probe_out[...] = probe_ref[...]
    loss_ref[...] = jnp.sum(jnp.where(left, 0.0, sums), axis=1, keepdims=True) / terms


def finished(grad, probe_total, sums, entries, terms):
    vmem = pl.BlockSpec(memory_space=pltpu.VMEM)
    return pl.pallas_call(
        functools.partial(finish_kernel, entries, terms),
        out_shape=[
            jax.ShapeDtypeStruct(grad.shape, jnp.float32),
            jax.ShapeDtypeStruct(probe_total.shape, jnp.float32),
            jax.ShapeDtypeStruct((1, 1), jnp.float32),
        ],
        in_specs=[vmem] * 3,
        out_specs=[vmem] * 3,
        compiler_params=pltpu.CompilerParams(vmem_limit_bytes=VMEM_LIMIT),
        name="finish",
    )(grad, probe_total, sums)


def local(phase_volume, absorb_volume, probe, amplitudes, scan_rows, scan_cols):
    length = probe.shape[1]
    count = scan_rows.shape[2]
    beams, rows_n, deep_n, cores = sizes()
    t, own = transmission(phase_volume, absorb_volume)
    canvas, probe_term, misfit = window_terms(
        t,
        probe,
        amplitudes.reshape(count, length, length),
        scan_rows.reshape(count),
        scan_cols.reshape(count),
    )
    positions = beams * rows_n * deep_n * cores * count
    grad, probe_total, sums = folded(canvas, own, probe_term, misfit, positions)
    entries = grad.size * rows_n * deep_n * cores
    step, probe_total, loss = finished(
        grad, probe_total, sums, entries, positions * length * length
    )
    return (step, probe_total, loss[0, 0])


def solution(mesh):
    split = Mesh(
        mesh.devices.reshape(mesh.shape["beam"], mesh.shape["row"], -1, 2),
        ("beam", "row", "col_0", "col_1"),
    )
    in_specs = (
        P("beam", "row", COL),
        P("beam", "row", COL),
        P(),
        P("row", COL, "beam", None, None),
        P("row", COL, "beam"),
        P("row", COL, "beam"),
    )
    out_specs = (P(None, "row", COL), P(), P())
    return jax.shard_map(local, mesh=split, in_specs=in_specs, out_specs=out_specs, check_vma=False)
```

```python
import functools
import math

import jax
import jax.numpy as jnp
import numpy as np
from jax import lax
from jax.experimental import pallas as pl
from jax.experimental.pallas import tpu as pltpu
from jax.sharding import Mesh
from jax.sharding import PartitionSpec as P

COL = ("col_0", "col_1")
MESH = pl.DeviceIdType.MESH
LANES = 128
CHUNK = 128
BATCH = 8
SUBS = 4
VMEM_LIMIT = 20 << 20


def dft_tables(length):
    indices = np.arange(length, dtype=np.int32)
    product = indices[:, None] * indices[None, :] % length
    angles = product.astype(np.float32) * np.float32(2.0 * math.pi / length)
    factor = np.float32(1.0 / math.sqrt(length))
    return (
        jnp.asarray(np.cos(angles) * factor).astype(jnp.bfloat16),
        jnp.asarray(-np.sin(angles) * factor).astype(jnp.bfloat16),
    )


def window_kernel(
    rows_ref, cols_ref, t_ref, probe_ref, amp_ref, table_ref,
    canvas_ref, probe_sum_ref, misfit_ref,
    fwd, bwd, cut, psi, half, chi, back,
):
    step = pl.program_id(0)
    n = probe_ref.shape[1]
    batch = amp_ref.shape[0]

    @pl.when(step == 0)
    def _():
        real, imag = table_ref[0], table_ref[1]
        minus = -imag
        fwd[:n, :n] = real
        fwd[:n, n:] = minus
        fwd[n:, :n] = imag
        fwd[n:, n:] = real
        bwd[:n, :n] = real
        bwd[:n, n:] = imag
        bwd[n:, :n] = minus
        bwd[n:, n:] = real
        canvas_ref[...] = jnp.zeros_like(canvas_ref)
        probe_sum_ref[...] = jnp.zeros_like(probe_sum_ref)
        misfit_ref[...] = jnp.zeros_like(misfit_ref)

    lane = lax.broadcasted_iota(jnp.int32, (32, LANES), 1)

    def cut_windows(j):
        row, col = rows_ref[step * batch + j], cols_ref[step * batch + j]
        turn = lax.rem(LANES - col, LANES)
        near = lane < LANES - col
        for at in range(0, n, 32):
            here = pl.ds(at, 32)
            pieces = []
            for part in range(2):
                turned = [
                    pltpu.roll(t_ref[part, k, pl.ds(row + at, 32), :], turn, 1)
                    for k in range(3)
                ]
                pieces.append([jnp.where(near, turned[k], turned[k + 1]) for k in range(2)])
            for k in range(2):
                lanes = pl.ds(k * LANES, LANES)
                tr, ti = pieces[0][k], pieces[1][k]
                cut[j, 0, here, lanes] = tr
                cut[j, 1, here, lanes] = ti
                pr = probe_ref[0, here, lanes]
                pi = probe_ref[1, here, lanes]
                psi[j, here, lanes] = (pr * tr - pi * ti).astype(jnp.bfloat16)
                psi[j, pl.ds(n + at, 32), lanes] = (pr * ti + pi * tr).astype(jnp.bfloat16)

    def to_half(j):
        for part in range(2):
            half[j, :, part * n : (part + 1) * n] = jnp.dot(
                fwd[part * n : (part + 1) * n, :], psi[j], preferred_element_type=jnp.float32
            ).astype(jnp.bfloat16)

    def to_far(j):
        total = jnp.zeros((8, LANES), jnp.float32)
        for at in range(0, n, CHUNK):
            here = pl.ds(at, CHUNK)
            far = jnp.dot(half[j, here, :], bwd[...], preferred_element_type=jnp.float32)
            fr, fi = far[:, :n], far[:, n:]
            amp = amp_ref[j, here, :].astype(jnp.float32)
            power = fr * fr + fi * fi
            inverse = lax.rsqrt(power)
            modulus = jnp.where(power > 0.0, power * inverse, 0.0)
            off = modulus - amp
            square = off * off
            total = total + jnp.sum(
                (square[:, :LANES] + square[:, LANES:]).reshape(CHUNK // 8, 8, LANES), axis=0
            )
            ratio = 1.0 - amp * jnp.minimum(inverse, 2.0)
            chi[j, here, :] = (fr * ratio).astype(jnp.bfloat16)
            chi[j, pl.ds(n + at, CHUNK), :] = (fi * ratio).astype(jnp.bfloat16)
        misfit_ref[...] += total

    def to_back(j):
        for part in range(2):
            back[j, :, part * n : (part + 1) * n] = jnp.dot(
                bwd[part * n : (part + 1) * n, :], chi[j], preferred_element_type=jnp.float32
            ).astype(jnp.bfloat16)

    def add_terms(j):
        row, col = rows_ref[step * batch + j], cols_ref[step * batch + j]
        far_side = lax.broadcasted_iota(jnp.int32, (CHUNK, LANES), 1) >= col
        for at in range(0, n, CHUNK):
            here = pl.ds(at, CHUNK)
            grad = jnp.dot(back[j, here, :], fwd[...], preferred_element_type=jnp.float32)
            gr, gi = grad[:, :n], grad[:, n:]
            tr, ti = cut[j, 0, here, :], cut[j, 1, here, :]
            probe_sum_ref[0, here, :] += tr * gr + ti * gi
            probe_sum_ref[1, here, :] += tr * gi - ti * gr
            pr, pi = probe_ref[0, here, :], probe_ref[1, here, :]
            for part, value in enumerate((pr * gr + pi * gi, pr * gi - pi * gr)):
                first = pltpu.roll(value[:, :LANES], col, 1)
                second = pltpu.roll(value[:, LANES:], col, 1)
                there = pl.ds(row + at, CHUNK)
                canvas_ref[part, 0, there, :] += jnp.where(far_side, first, 0.0)
                canvas_ref[part, 1, there, :] += jnp.where(far_side, second, first)
                canvas_ref[part, 2, there, :] += jnp.where(far_side, 0.0, second)

    steps = (cut_windows, to_half, to_far, to_back, add_terms)
    for tick in range(batch + len(steps) - 1):
        for at, stage in enumerate(steps):
            if 0 <= tick - at < batch:
                stage(tick - at)


def window_terms(t, probe, amplitudes, rows, cols):
    count, n, _ = amplitudes.shape
    batch = max(size for size in (1, 2, BATCH) if count % size == 0)
    grid_spec = pltpu.PrefetchScalarGridSpec(
        num_scalar_prefetch=2,
        grid=(count // batch,),
        in_specs=[
            pl.BlockSpec(t.shape, lambda s, *_: (0, 0, 0, 0)),
            pl.BlockSpec(probe.shape, lambda s, *_: (0, 0, 0)),
            pl.BlockSpec((batch, n, n), lambda s, *_: (s, 0, 0)),
            pl.BlockSpec((2, n, n), lambda s, *_: (0, 0, 0)),
        ],
        out_specs=[
            pl.BlockSpec(t.shape, lambda s, *_: (0, 0, 0, 0)),
            pl.BlockSpec(probe.shape, lambda s, *_: (0, 0, 0)),
            pl.BlockSpec((8, LANES), lambda s, *_: (0, 0)),
        ],
        scratch_shapes=[
            pltpu.VMEM((2 * n, 2 * n), jnp.bfloat16),
            pltpu.VMEM((2 * n, 2 * n), jnp.bfloat16),
            pltpu.VMEM((batch, 2, n, n), jnp.float32),
            pltpu.VMEM((batch, 2 * n, n), jnp.bfloat16),
            pltpu.VMEM((batch, n, 2 * n), jnp.bfloat16),
            pltpu.VMEM((batch, 2 * n, n), jnp.bfloat16),
            pltpu.VMEM((batch, n, 2 * n), jnp.bfloat16),
        ],
    )
    return pl.pallas_call(
        window_kernel,
        grid_spec=grid_spec,
        out_shape=[
            jax.ShapeDtypeStruct(t.shape, jnp.float32),
            jax.ShapeDtypeStruct(probe.shape, jnp.float32),
            jax.ShapeDtypeStruct((8, LANES), jnp.float32),
        ],
        compiler_params=pltpu.CompilerParams(
            dimension_semantics=("arbitrary",), vmem_limit_bytes=VMEM_LIMIT
        ),
        name="windows",
    )(rows, cols, t, probe, amplitudes, jnp.stack(dft_tables(n)))


def places():
    return tuple(lax.axis_index(axis) for axis in ("beam", "row", "col_0", "col_1"))


def sizes():
    return tuple(lax.axis_size(axis) for axis in ("beam", "row", "col_0", "col_1"))


def remote(src, dst, send_sem, recv_sem, **where):
    return pltpu.make_async_remote_copy(
        src_ref=src,
        dst_ref=dst,
        send_sem=send_sem,
        recv_sem=recv_sem,
        device_id=where,
        device_id_type=MESH,
    )


def greet(barrier, **where):
    pl.semaphore_signal(barrier, inc=1, device_id=where, device_id_type=MESH)


def spread_kernel(
    phase_ref, absorb_ref, t_ref, own_ref,
    vol, part, inbox,
    vol_sem, sum_send, sum_recv, beam_send, near_send, near_recv, rim_send, rim_recv,
    out_send, out_recv, own_recv, row_send, corner_send, corner_recv, t_recv,
):
    beams, rows_n, deep_n, _ = sizes()
    b, i, z, c = places()
    subs, h = part.shape[1], part.shape[3]
    quarter_rows = subs * h
    top = beams // 2
    half = top * quarter_rows
    blocks = 2 * beams * subs
    out_z = z - 1 + 2 * c
    has_out = (out_z >= 0) & (out_z < deep_n)
    above, below = i > 0, i < rows_n - 1
    outer = dict(col_0=out_z, col_1=1 - c)
    order = [*range(1, beams), 0]
    loads = {}
    for o in order:
        q = lax.rem(b + o, beams)
        rows_here = pl.ds(pl.multiple_of(q * quarter_rows, quarter_rows), quarter_rows)
        for p, ref in enumerate((phase_ref, absorb_ref)):
            loads[o, p] = pltpu.make_async_copy(
                ref.at[:, rows_here, :], vol.at[o, p], vol_sem.at[o, p]
            )
            loads[o, p].start()

    barrier = pltpu.get_barrier_semaphore()
    for o in range(1, beams):
        greet(barrier, beam=lax.rem(b + o, beams))
    greet(barrier, col_1=1 - c)

    @pl.when(has_out)
    def _():
        greet(barrier, **outer)

    for alive, row in ((above, i - 1), (below, i + 1)):

        @pl.when(alive)
        def _(row=row):
            greet(barrier, row=row)

        @pl.when(alive & has_out)
        def _(row=row):
            greet(barrier, row=row, **outer)

    for o in order:
        for p in range(2):
            loads[o, p].wait()
            total = vol[o, p, 0].astype(jnp.float32)
            for d in range(1, phase_ref.shape[0]):
                total = total + vol[o, p, d].astype(jnp.float32)
            for s in range(subs):
                part[o, s, p] = total[s * h : (s + 1) * h]
    ups, downs, outs = (flag.astype(jnp.int32) for flag in (above, below, has_out))
    pl.semaphore_wait(barrier, beams + outs + (1 + outs) * (ups + downs))
    for s in range(subs):
        for o in order[:-1]:
            remote(
                part.at[o, s], inbox.at[s, o], sum_send.at[s], sum_recv.at[s],
                beam=lax.rem(b + o, beams),
            ).start()

    def cell(k, m):
        return t_ref.at[:, k, pl.ds(pl.multiple_of(m * h, h), h), :]

    def arrived(m, check=None):
        wait = remote(cell(1, m), cell(1, m), near_send, t_recv.at[m], col_1=1 - c).wait_recv
        if check is None:
            wait()
        else:
            pl.when(check)(wait)

    def spot(o, s):
        q = lax.rem(b + o, beams)
        upper = q // top
        rim = q * subs + s - top * subs + (1 - upper) * blocks
        goal, source = i - 1 + 2 * upper, i + 1 - 2 * upper
        return (
            top * subs + q * subs + s, rim, upper, goal,
            (goal >= 0) & (goal < rows_n), (source >= 0) & (source < rows_n),
        )

    ring = [1, *range(3, beams), *range(2, min(3, beams))]
    by_row, direct = {0}, {2}
    singles = []

    def single(check, slot, upper, src, dst, **where):
        copy = remote(src, dst, corner_send.at[slot], corner_recv.at[upper], **where)
        pl.when(check)(copy.start)
        singles.append((check, copy))

    def tile(o, s):
        m, rim, upper, goal, alive, _ = spot(o, s)
        if o:
            arrived(m)
        landed = own_recv.at[s] if o in by_row else out_recv
        far = remote(cell(1, m), cell(2 - 2 * c, m), out_send, landed, **outer)
        pl.when(has_out)(far.start)
        side = remote(cell(1, m), cell(1, rim), row_send.at[upper], t_recv.at[rim], row=goal)
        pl.when(alive)(side.start)
        if o in direct:
            single(
                alive & has_out, o * subs + s, upper, cell(1, m), cell(2 - 2 * c, rim),
                row=goal, **outer,
            )
        remote(cell(1, m), cell(2 * c, m), near_send, near_recv, col_1=1 - c).start()

    def corner(o, s):
        m, rim, upper, goal, alive, _ = spot(o, s)
        here = cell(2 * c, m)
        pl.when(has_out)(remote(here, here, out_send, own_recv.at[s], **outer).wait_recv)
        single(alive & has_out, o * subs + s, upper, here, cell(2 * c, rim), row=goal)

    def edge(o, s):
        _, rim, upper, _, _, alive = spot(o, s)
        arrived(rim, alive)
        if o not in by_row and o not in direct:
            single(
                alive & has_out, o * subs + s, upper, cell(1, rim), cell(2 - 2 * c, rim), **outer
            )
        copy = remote(
            cell(1, rim), cell(2 * c, rim), rim_send.at[upper], rim_recv.at[upper], col_1=1 - c
        )
        pl.when(alive)(copy.start)

    def total_of(like, send, recv):
        return remote(like, like, send, recv, col_1=1 - c)

    for s in range(subs):
        sums = total_of(inbox.at[s, pl.ds(1, beams - 1)], sum_send.at[s], sum_recv.at[s])
        sums.wait_recv()
        phase, absorb = part[0, s, 0], part[0, s, 1]
        for o in range(1, beams):
            phase = phase + inbox[s, o, 0]
            absorb = absorb + inbox[s, o, 1]
        damping = jnp.exp(-absorb)
        mine = pl.ds(pl.multiple_of(half + (b * subs + s) * h, h), h)
        for p, value in enumerate((damping * jnp.cos(phase), damping * jnp.sin(phase))):
            t_ref[p, 1, mine, :] = value
            own_ref[p, pl.ds(s * h, h), :] = value
        m = top * subs + b * subs + s
        for o in ring:
            remote(
                cell(1, m), cell(1, m), beam_send, t_recv.at[m], beam=lax.rem(b + o, beams)
            ).start()
        tile(0, s)
    events = []
    for s in range(subs):
        events += [(corner, 0, s), *[(tile, o, s) for o in ring if o not in direct], (edge, 0, s)]
        events += [(tile, o, s) for o in ring if o in direct]
    events += [(edge, o, s) for s in range(subs) for o in ring]
    for event, o, s in events:
        event(o, s)
    most = part.at[pl.ds(1, beams - 1)]
    some = part.at[pl.ds(0, top)]
    total_of(part, near_send, near_recv).wait_recv()
    pl.when(has_out)(total_of(most, out_send, out_recv).wait_recv)
    for upper, source_here in enumerate((below, above)):
        pl.when(source_here)(total_of(some, rim_send.at[upper], rim_recv.at[upper]).wait_recv)
        pl.when(source_here & has_out)(
            total_of(some, rim_send.at[upper], corner_recv.at[upper]).wait_recv
        )
    for s in range(subs):
        total_of(part.at[pl.ds(1, beams - 1), s], sum_send.at[s], sum_recv.at[s]).wait_send()
    total_of(most, beam_send, beam_send).wait_send()
    total_of(part, near_send, near_send).wait_send()
    pl.when(has_out)(total_of(part, out_send, out_send).wait_send)
    for upper, (goal_here, source_here) in enumerate(((above, below), (below, above))):
        pl.when(goal_here)(total_of(some, row_send.at[upper], row_send.at[upper]).wait_send)
        pl.when(source_here)(total_of(some, rim_send.at[upper], rim_send.at[upper]).wait_send)
    for check, copy in singles:
        pl.when(check)(copy.wait_send)
    tall = blocks * h

    def blank(tiles, start, size):
        for k in tiles:
            t_ref[0, k, pl.ds(start, size), :] = jnp.ones((size, LANES), jnp.float32)
            t_ref[1, k, pl.ds(start, size), :] = jnp.zeros((size, LANES), jnp.float32)

    pl.when(i == 0)(lambda: blank(range(3), 0, half))
    pl.when(i == rows_n - 1)(lambda: blank(range(3), tall - half, half))
    pl.when((z == 0) & (c == 0))(lambda: blank((0,), 0, tall))
    pl.when((z == deep_n - 1) & (c == 1))(lambda: blank((2,), 0, tall))


def transmission(phase_volume, absorb_volume):
    deep, rows, lanes = phase_volume.shape
    beams = lax.axis_size("beam")
    h = rows // (beams * SUBS)
    dma = pltpu.SemaphoreType.DMA
    return pl.pallas_call(
        spread_kernel,
        out_shape=[
            jax.ShapeDtypeStruct((2, 3, 2 * rows, lanes), jnp.float32),
            jax.ShapeDtypeStruct((2, SUBS * h, lanes), jnp.float32),
        ],
        in_specs=[pl.BlockSpec(memory_space=pltpu.HBM)] * 2,
        out_specs=[pl.BlockSpec(memory_space=pltpu.VMEM)] * 2,
        scratch_shapes=[
            pltpu.VMEM((beams, 2, deep, SUBS * h, lanes), jnp.bfloat16),
            pltpu.VMEM((beams, SUBS, 2, h, lanes), jnp.float32),
            pltpu.VMEM((SUBS, beams, 2, h, lanes), jnp.float32),
            dma((beams, 2)),
            dma((SUBS,)),
            dma((SUBS,)),
            dma,
            dma,
            dma,
            dma((2,)),
            dma((2,)),
            dma,
            dma,
            dma((SUBS,)),
            dma((2,)),
            dma((beams * SUBS,)),
            dma((2,)),
            dma((2 * beams * SUBS,)),
        ],
        compiler_params=pltpu.CompilerParams(
            collective_id=0, has_side_effects=True, vmem_limit_bytes=VMEM_LIMIT
        ),
        name="spread",
    )(
        pltpu.with_memory_space_constraint(phase_volume, pltpu.HBM),
        pltpu.with_memory_space_constraint(absorb_volume, pltpu.HBM),
    )


def fold_kernel(
    scale, canvas_ref, own_ref, probe_ref, misfit_ref,
    grad, probe_out, sums_ref,
    sib_in, out_in, acc, corner_in, corner, row_in, q_in, p_in, p_sum, y_in, x_in, z_in, n_xy, n_zc,
    sib_send, sib_recv, out_send, out_recv, corner_send, corner_recv, row_send, row_recv,
    pair_send, pair_recv, group_send, group_recv, word,
):
    beams, rows_n, deep_n, cores = sizes()
    b, i, z, c = places()
    rows = grad.shape[1]
    h = rows // beams
    half = rows // 2
    tall = 2 * rows
    plane = beams * rows_n
    across = deep_n * cores
    out_z = z - 1 + 2 * c
    me_xy = b * rows_n + i
    me_zc = z * cores + c
    has_out = (out_z >= 0) & (out_z < deep_n)
    above, below = i > 0, i < rows_n - 1
    finish = []

    def go(copy, check=None):
        if check is None:
            copy.start()
        else:
            pl.when(check)(copy.start)
        finish.append((check, copy))
        return copy

    def peer_xy(o):
        return dict(beam=lax.rem(b + o // rows_n, beams), row=lax.rem(i + o % rows_n, rows_n))

    def reach(o):
        ob, oi = o // rows_n, o % rows_n
        return -min(ob, beams - ob) - min(oi, rows_n - oi)

    def peer_zc(o):
        return dict(col_0=lax.rem(z + o // cores, deep_n), col_1=lax.rem(c + o % cores, cores))

    def group(g, copies, like):
        for src, dst, where in copies:
            remote(src, dst, group_send.at[g], group_recv.at[g], **where).start()
        everything = remote(like, like, group_send.at[g], group_recv.at[g], col_1=1 - c)
        finish.append((None, everything))
        return everything

    barrier = pltpu.get_barrier_semaphore()
    for o in range(1, beams):
        greet(barrier, beam=lax.rem(b + o, beams))
    for o in range(1, rows_n):
        greet(barrier, row=lax.rem(i + o, rows_n))
    greet(barrier, col_1=1 - c)
    for o in (1, deep_n - 1):
        greet(barrier, col_0=lax.rem(z + o, deep_n))

    @pl.when(has_out)
    def _():
        greet(barrier, col_0=out_z, col_1=1 - c)

    pl.semaphore_wait(barrier, beams + rows_n + 1 + has_out.astype(jnp.int32))
    for o in range(1, rows_n):
        greet(word.at[0], row=lax.rem(i + o, rows_n))
    for o in (1, deep_n - 1):
        greet(word.at[1], col_0=lax.rem(z + o, deep_n))

    middle = pl.ds(half, rows)
    subs = beams // 2
    pieces = []
    for s in range(subs):
        pieces.append((s * h, above, i - 1, below, subs + s))
        pieces.append((tall - half + s * h, below, i + 1, above, s))
    outer = dict(col_0=out_z, col_1=1 - c)
    half_copy = go(remote(probe_ref.at[1 - c], p_in, pair_send.at[0], pair_recv.at[0], col_1=1 - c))
    far_rims, near_rims, corners = [], [], []
    for e, (start, alive, goal, _, _) in enumerate(pieces):
        where = pl.ds(start, h)
        near_rims.append(
            go(
                remote(
                    canvas_ref.at[:, 2 - 2 * c, where, :], sib_in.at[:, where, :],
                    sib_send.at[e], sib_recv.at[e], col_1=1 - c,
                ),
                alive,
            )
        )
        far_rims.append(
            go(
                remote(
                    canvas_ref.at[0, 2 * c, where, :], out_in.at[0, where, :],
                    out_send.at[e], out_recv.at[e], **outer,
                ),
                has_out & alive,
            )
        )
        corners.append(
            go(
                remote(
                    canvas_ref.at[1, 2 * c, where, :], corner_in.at[e],
                    corner_send.at[e], corner_recv.at[e], row=goal,
                ),
                has_out & alive,
            )
        )
    far_first = go(
        remote(
            canvas_ref.at[0, 2 * c, middle, :], out_in.at[0, middle, :],
            out_send.at[beams], out_recv.at[beams], **outer,
        ),
        has_out,
    )
    near_middle = go(
        remote(
            canvas_ref.at[:, 2 - 2 * c, middle, :], sib_in.at[:, middle, :],
            sib_send.at[beams], sib_recv.at[beams], col_1=1 - c,
        )
    )
    half_copy.wait_recv()
    p_sum[...] = (probe_ref[c] + p_in[...]).reshape(p_sum.shape)
    parts = group(
        0,
        [
            (p_sum.at[:, lax.rem(b + o, beams)], y_in.at[o], dict(beam=lax.rem(b + o, beams)))
            for o in range(1, beams)
        ],
        y_in.at[pl.ds(1, beams - 1)],
    )

    edges, far_second = {}, {}

    def rim(p, e):
        start, alive, goal, _, _ = pieces[e]
        where = pl.ds(start, h)

        @pl.when(alive)
        def _():
            if p == 1:
                near_rims[e].wait_recv()
            acc[p, where, :] = canvas_ref[p, 1, where, :] + sib_in[p, where, :]
            if p == 0:

                @pl.when(has_out)
                def _():
                    far_rims[e].wait_recv()
                    acc[0, where, :] += out_in[0, where, :]

        edges[p, e] = go(
            remote(
                acc.at[p, where, :], row_in.at[p, e],
                row_send.at[p, e], row_recv.at[p, e], row=goal,
            ),
            alive,
        )

    def corner_piece(e):
        _, _, _, given, quarter = pieces[e]
        inside, there = pl.ds(quarter * h, h), pl.ds(half + quarter * h, h)

        @pl.when(has_out)
        def _():
            corner[inside, :] = canvas_ref[1, 2 * c, there, :]

            @pl.when(given)
            def _():
                corners[e].wait_recv()
                corner[inside, :] += corner_in[e]

        far_second[e] = go(
            remote(
                corner.at[inside, :], out_in.at[1, there, :],
                out_send.at[beams + 1 + e], out_recv.at[beams + 1 + e], **outer,
            ),
            has_out,
        )

    for e in range(beams):
        rim(1, e)
    for e in range(beams):
        rim(0, e)
        corner_piece(e)
    pl.semaphore_wait(word.at[1], 2)
    for o in (2, deep_n - 2):
        greet(word.at[2], col_0=lax.rem(z + o, deep_n))
    near_middle.wait_recv()
    acc[:, middle, :] = canvas_ref[:, 1, middle, :] + sib_in[:, middle, :]

    @pl.when(has_out)
    def _():
        far_first.wait_recv()
        acc[0, middle, :] += out_in[0, middle, :]

    quarters = remote(
        q_in.at[pl.ds(1, beams - 1)], q_in.at[pl.ds(1, beams - 1)],
        group_send.at[2], group_recv.at[2], col_1=1 - c,
    )
    finish.append((None, quarters))

    def settle(e):
        _, _, _, given, quarter = pieces[e]
        there = pl.ds(half + quarter * h, h)

        @pl.when(given)
        def _():
            for p in (1, 0):
                edges[p, e].wait_recv()
                acc[p, there, :] += row_in[p, e]

        @pl.when(has_out)
        def _():
            far_second[e].wait_recv()
            acc[1, there, :] += out_in[1, there, :]

        copy = remote(
            acc.at[:, there, :], q_in.at[b], group_send.at[2], group_recv.at[2], beam=quarter
        )
        pl.when(b != quarter)(copy.start)

    for e in range(2):
        settle(e)
    parts.wait_recv()
    block = p_sum[:, b]
    for o in range(1, beams):
        block = block + y_in[o]
    y_in[0] = block
    parts = group(
        1,
        [
            (y_in.at[0, lax.rem(i + o, rows_n)], x_in.at[o], dict(row=lax.rem(i + o, rows_n)))
            for o in range(1, rows_n)
        ],
        x_in.at[pl.ds(1, rows_n - 1)],
    )
    for e in range(2, beams):
        settle(e)
    mine = pl.ds(pl.multiple_of(half + b * h, h), h)
    q_in[b] = acc[:, mine, :]
    pl.semaphore_wait(word.at[0], rows_n - 1)
    pl.semaphore_wait(word.at[2], 2)
    parts.wait_recv()
    total = y_in[0, i]
    for o in range(1, rows_n):
        total = total + x_in[o]
    z_in[z] = total
    levels = group(
        3,
        [
            (z_in.at[z], z_in.at[z], dict(col_0=lax.rem(z + o, deep_n)))
            for o in sorted(range(1, deep_n), key=lambda o: -min(o, deep_n - o))
        ],
        z_in.at[pl.ds(0, deep_n - 1)],
    )

    quarters.wait_recv()
    cr, ci = q_in[0, 0], q_in[0, 1]
    for o in range(1, beams):
        cr = cr + q_in[o, 0]
        ci = ci + q_in[o, 1]
    tr, ti = own_ref[0], own_ref[1]
    phase = tr * ci - ti * cr
    absorb = -(tr * cr + ti * ci)
    home = pl.ds(pl.multiple_of(b * h, h), h)
    grad[0, home, :] = phase
    grad[1, home, :] = absorb
    squares = jnp.sum(phase * phase + absorb * absorb, axis=0, keepdims=True)
    misfits = jnp.sum(misfit_ref[...], axis=0, keepdims=True)
    left = lax.broadcasted_iota(jnp.int32, (1, LANES), 1) < LANES // 2
    n_xy[me_xy] = jnp.where(
        left,
        squares + pltpu.roll(squares, LANES // 2, 1),
        misfits + pltpu.roll(misfits, LANES // 2, 1),
    )
    norms = group(
        4,
        [(n_xy.at[me_xy], n_xy.at[me_xy], peer_xy(o)) for o in sorted(range(1, plane), key=reach)],
        n_xy.at[pl.ds(0, plane - 1)],
    )

    grads = group(
        6,
        [
            (grad.at[:, home, :], grad.at[:, home, :], dict(beam=lax.rem(b + o, beams)))
            for o in range(1, beams)
        ],
        q_in.at[pl.ds(1, beams - 1)],
    )

    levels.wait_recv()
    total = z_in[0]
    for k in range(1, deep_n):
        total = total + z_in[k]
    probe_out[c, i, b] = total * scale
    share = p_sum.shape[2]
    own_piece = probe_out.at[c, i, b]
    near_by = [o for o in range(1, plane) if o % rows_n != rows_n // 2]
    far_off = [o for o in range(1, plane) if o % rows_n == rows_n // 2]
    spreads = group(
        5,
        [(own_piece, own_piece, peer_xy(o)) for o in near_by],
        p_in.at[pl.ds(0, len(near_by) * share), :],
    )
    far_pieces = group(
        8,
        [
            (own_piece, own_piece, dict(peer_xy(o), col_1=core))
            for core in (c, 1 - c)
            for o in far_off
        ],
        p_in.at[pl.ds(0, 2 * len(far_off) * share), :],
    )
    norms.wait_recv()
    pair = n_xy[0]
    for k in range(1, plane):
        pair = pair + n_xy[k]
    n_zc[me_zc] = pair
    norms = group(
        7,
        [
            (n_zc.at[me_zc], n_zc.at[me_zc], peer_zc(o))
            for o in sorted(range(1, across), key=lambda o: -min(o // cores, deep_n - o // cores))
        ],
        n_zc.at[pl.ds(0, across - 1)],
    )
    spreads.wait_recv()
    last = group(
        9,
        [
            (
                probe_out.at[c, lax.rem(i + o, rows_n)],
                probe_out.at[c, lax.rem(i + o, rows_n)],
                dict(col_1=1 - c),
            )
            for o in range(rows_n)
            if o != rows_n // 2
        ],
        probe_out.at[0, pl.ds(0, rows_n - 1)],
    )
    norms.wait_recv()
    pair = n_zc[0]
    for k in range(1, across):
        pair = pair + n_zc[k]
    sums_ref[...] = pair
    grads.wait_recv()
    far_pieces.wait_recv()
    last.wait_recv()
    for check, copy in finish:
        if check is None:
            copy.wait_send()
        else:
            pl.when(check)(copy.wait_send)


def folded(canvas, own, probe_sum, misfit, positions):
    beams, rows_n, deep_n, cores = sizes()
    _, _, tall, lanes = canvas.shape
    rows = tall // 2
    h = rows // beams
    n = probe_sum.shape[1]
    plane, across = beams * rows_n, deep_n * cores
    share = n // plane
    f32 = functools.partial(pltpu.VMEM, dtype=jnp.float32)
    outs, sides = 2 * beams + 1, beams + 1
    sems = [(sides,), (sides,), (outs,), (outs,), (beams,), (beams,)]
    sems += [(2, beams), (2, beams), (1,), (1,), (10,), (10,)]
    grad, probe_total, sums = pl.pallas_call(
        functools.partial(fold_kernel, 1.0 / positions),
        out_shape=[
            jax.ShapeDtypeStruct((2, rows, lanes), jnp.float32),
            jax.ShapeDtypeStruct((2, rows_n, beams, share, n), jnp.float32),
            jax.ShapeDtypeStruct((1, LANES), jnp.float32),
        ],
        in_specs=[pl.BlockSpec(memory_space=pltpu.VMEM)] * 4,
        out_specs=[pl.BlockSpec(memory_space=pltpu.VMEM)] * 3,
        scratch_shapes=[
            f32((2, tall, lanes)),
            f32((2, tall, lanes)),
            f32((2, tall, lanes)),
            f32((beams, h, lanes)),
            f32((rows, lanes)),
            f32((2, beams, h, lanes)),
            f32((beams, 2, h, lanes)),
            f32((n, n)),
            f32((rows_n, beams, share, n)),
            f32((beams, rows_n, share, n)),
            f32((rows_n, share, n)),
            f32((deep_n, share, n)),
            f32((plane, 1, LANES)),
            f32((across, 1, LANES)),
            *[pltpu.SemaphoreType.DMA(count) for count in sems],
            pltpu.SemaphoreType.REGULAR((3,)),
        ],
        compiler_params=pltpu.CompilerParams(
            collective_id=1, has_side_effects=True, vmem_limit_bytes=VMEM_LIMIT
        ),
        name="fold",
    )(canvas, own, probe_sum, misfit)
    return grad, probe_total.reshape(probe_sum.shape), sums


def finish_kernel(entries, terms, grad_ref, probe_ref, sums_ref, step_ref, probe_out, loss_ref):
    sums = sums_ref[...]
    left = lax.broadcasted_iota(jnp.int32, sums.shape, 1) < LANES // 2
    square = jnp.sum(jnp.where(left, sums, 0.0), axis=1, keepdims=True)
    factor = jnp.minimum(1.0, 0.5 / jnp.sqrt(square / entries + 1e-06))
    for p in range(2):
        step_ref[p] = grad_ref[p] * factor
    probe_out[...] = probe_ref[...]
    loss_ref[...] = jnp.sum(jnp.where(left, 0.0, sums), axis=1, keepdims=True) / terms


def finished(grad, probe_total, sums, entries, terms):
    vmem = pl.BlockSpec(memory_space=pltpu.VMEM)
    return pl.pallas_call(
        functools.partial(finish_kernel, entries, terms),
        out_shape=[
            jax.ShapeDtypeStruct(grad.shape, jnp.float32),
            jax.ShapeDtypeStruct(probe_total.shape, jnp.float32),
            jax.ShapeDtypeStruct((1, 1), jnp.float32),
        ],
        in_specs=[vmem] * 3,
        out_specs=[vmem] * 3,
        compiler_params=pltpu.CompilerParams(vmem_limit_bytes=VMEM_LIMIT),
        name="finish",
    )(grad, probe_total, sums)


def local(phase_volume, absorb_volume, probe, amplitudes, scan_rows, scan_cols):
    length = probe.shape[1]
    count = scan_rows.shape[2]
    beams, rows_n, deep_n, cores = sizes()
    t, own = transmission(phase_volume, absorb_volume)
    canvas, probe_term, misfit = window_terms(
        t,
        probe,
        amplitudes.reshape(count, length, length),
        scan_rows.reshape(count),
        scan_cols.reshape(count),
    )
    positions = beams * rows_n * deep_n * cores * count
    grad, probe_total, sums = folded(canvas, own, probe_term, misfit, positions)
    entries = grad.size * rows_n * deep_n * cores
    step, probe_total, loss = finished(
        grad, probe_total, sums, entries, positions * length * length
    )
    return (step, probe_total, loss[0, 0])


def solution(mesh):
    split = Mesh(
        mesh.devices.reshape(mesh.shape["beam"], mesh.shape["row"], -1, 2),
        ("beam", "row", "col_0", "col_1"),
    )
    in_specs = (
        P("beam", "row", COL),
        P("beam", "row", COL),
        P(),
        P("row", COL, "beam", None, None),
        P("row", COL, "beam"),
        P("row", COL, "beam"),
    )
    out_specs = (P(None, "row", COL), P(), P())
    return jax.shard_map(local, mesh=split, in_specs=in_specs, out_specs=out_specs, check_vma=False)
```
